512 devices in a mesh: section: 8 (over z), expert: 16 (over y, core), dp: 4 (over x).
Axes of the slice: x: 4, y: 8, z: 8, core: 2. Of those that a mesh axis runs over, the one named last changes fastest.
Arguments:
- arrivals: bfloat16 [8, 4096, 2048], P('section', ('expert', 'dp')), may hold values from -6 to 6
- fresh: bfloat16 [1, 4096, 2048], P(None, ('expert', 'dp')), may hold values from -6 to 6
- routes: int32 [8, 2, 4096, 6], P('section', None, ('expert', 'dp')), may hold values from 0 to 63, as said below
- gates: bfloat16 [8, 2, 4096, 6], P('section', None, ('expert', 'dp')), may hold values from 0.099609375 to 1
- cotangent: bfloat16 [8, 2, 4096, 2048], P('section', None, ('expert', 'dp')), may hold values from -0.3125 to 0.3125
- norm_gain: float32 [8, 2048], P('section'), may hold values from 0.5 to 1.5
- w_gate: bfloat16 [8, 5632, 2048], P('section', 'expert', 'dp'), may hold values from -0.125 to 0.125
- w_up: bfloat16 [8, 5632, 2048], P('section', 'expert', 'dp'), may hold values from -0.125 to 0.125
- w_down: bfloat16 [8, 5632, 2048], P('section', 'expert', 'dp'), may hold values from -0.15625 to 0.15625
Outputs:
- layer_out: bfloat16 [8, 2, 4096, 2048], P('section', None, ('expert', 'dp'))
- grad_down: float32 [8, 5632, 2048], P('section', 'expert', 'dp')
The draws below stay inside these ranges and needn't reach their ends.
Inputs may be any that keep to these rules, and one draw needn't show every extreme that they name: `routes`: each token's 6 entries are different expert numbers.
All inputs are finite; a program needn't handle non-finite values.
Results may differ from the reference program's by a relative error of at most 0.0085.
Values may be sent and summed in bfloat16 or wider, within the bound.
A program may use at most 64 MiB of HBM per device.

```python
import jax
import jax.numpy as jnp
from jax import lax

D = 2048
EXPERTS = 64
TOPK = 6
EXP_HID = 1408
SPLIT = 4
CAP = 12
STEPS = 2
TOK_MB = 64
FLIGHT = 4
HID_DEV = 352
LAYERS = 8
FRESH = 1
TOKENS = 4096


def draw_routes(key, part):
    total_rows = LAYERS * STEPS * TOKENS
    groups = LAYERS * STEPS
    blocks = total_rows // TOK_MB
    key_noise, key_hot, key_rank, key_pick, key_boost = jax.random.split(jax.random.fold_in(key, 7), 5)
    column = jnp.arange(EXPERTS, dtype=jnp.int32)
    noise = jax.random.randint(key_noise, (total_rows, EXPERTS), 0, 1 << 20, dtype=jnp.int32)
    scores = noise * EXPERTS + column[None, :]
    hottest = jax.random.randint(key_hot, (groups,), 0, FLIGHT, dtype=jnp.int32)
    hot_rows = jnp.repeat(hottest, TOKENS)
    ranking = jax.random.randint(key_rank, (blocks, TOK_MB), 0, 1 << 20, dtype=jnp.int32) * TOK_MB + jnp.arange(TOK_MB, dtype=jnp.int32)[None, :]
    ordering = jnp.argsort(jnp.argsort(ranking, axis=1), axis=1).reshape(total_rows)
    forced = (ordering < CAP).astype(jnp.int32)
    scores = scores + forced[:, None] * (column[None, :] == hot_rows[:, None]).astype(jnp.int32) * (1 << 28)
    picked = jax.random.randint(key_pick, (total_rows,), 0, FLIGHT, dtype=jnp.int32)
    boosted = (jax.random.randint(key_boost, (total_rows,), 0, 4, dtype=jnp.int32) == 0).astype(jnp.int32)
    scores = scores + boosted[:, None] * (column[None, :] == picked[:, None]).astype(jnp.int32) * (1 << 27)
    top_values, chosen = lax.top_k(scores, TOPK)
    return chosen.astype(jnp.int32).reshape(LAYERS, STEPS, TOKENS, TOPK)


def level_of(own_key, dims, shards, low, largest):
    level = 1.0
    for dim, blocks in shards:
        draws = jax.random.uniform(jax.random.fold_in(jax.random.fold_in(own_key, 6), dim), (blocks,), jnp.float32, low / len(shards), largest / len(shards))
        level = level * jnp.repeat(jnp.exp(draws), dims[dim] // blocks).reshape((-1,) + (1,) * (len(dims) - 1 - dim))
    return level


def gaussian(rng, extent, width, bound, cuts=(), kind=jnp.bfloat16):
    level = level_of(rng, extent, cuts, -0.22, 0.18) if cuts else 1.0
    values = jax.random.normal(rng, extent, jnp.float32) * width * level
    return jnp.minimum(jnp.maximum(values, -bound), bound).astype(kind)


def setup_inputs(seed: int = 0) -> dict:
    seeds = jax.random.split(jax.random.key(seed), 10)
    return {
        "arrivals": gaussian(seeds[0], (LAYERS, TOKENS, D), 1.0, 6.0, ((0, 8), (1, 64))),
        "fresh": gaussian(seeds[1], (FRESH, TOKENS, D), 1.0, 6.0, ((1, 64),)),
        "routes": draw_routes(jax.random.fold_in(seeds[9], 71), 0),
        "gates": jnp.clip(0.099609375 + 0.9003906 * jax.random.uniform(seeds[3], (LAYERS, STEPS, TOKENS, TOPK), jnp.float32) ** level_of(seeds[3], (LAYERS, STEPS, TOKENS, TOPK), ((0, 8), (2, 64)), -0.2, 0.2), 0.099609375, 1.0).astype(jnp.bfloat16),
        "cotangent": gaussian(seeds[4], (LAYERS, STEPS, TOKENS, D), 0.05, 0.3125, ((0, 8), (2, 64))),
        "norm_gain": jnp.clip(1.0 + 0.1 * jax.random.normal(seeds[5], (LAYERS, D), jnp.float32), 0.5, 1.5),
        "w_gate": gaussian(seeds[6], (LAYERS, FLIGHT * EXP_HID, D), D ** -0.5, 0.125, ((0, 8), (1, 16), (2, 4))),
        "w_up": gaussian(seeds[7], (LAYERS, FLIGHT * EXP_HID, D), D ** -0.5, 0.125, ((0, 8), (1, 16), (2, 4))),
        "w_down": gaussian(seeds[8], (LAYERS, FLIGHT * EXP_HID, D), EXP_HID ** -0.5, 0.15625, ((0, 8), (1, 16), (2, 4))),
    }


def rms_normed(values, gains):
    floats = values.astype(jnp.float32)
    scale = lax.rsqrt(lax.optimization_barrier(jnp.mean(floats * floats, axis=-1, keepdims=True)) + 0.5)
    return (floats * scale * gains[None, :]).astype(jnp.bfloat16)

def layer(inputs, routing, weights, cot, gains, gate_rows, up_rows, down_rows):
    highest = lax.Precision.HIGHEST
    blocks = TOKENS // TOK_MB
    normed = rms_normed(inputs, gains).astype(jnp.float32).reshape(blocks, TOK_MB, D)
    cot_blocks = cot.astype(jnp.float32).reshape(blocks, TOK_MB, D)
    route_blocks = routing.reshape(blocks, TOK_MB, TOPK)
    weight_blocks = weights.astype(jnp.float32).reshape(blocks, TOK_MB, TOPK)
    slot_ids = jnp.arange(CAP, dtype=jnp.int32)
    mixture = jnp.zeros((blocks, TOK_MB, D), jnp.float32)
    grads = []
    for expert in range(FLIGHT):
        matches = route_blocks == expert
        naming = jnp.any(matches, axis=-1).astype(jnp.int32)
        shares = lax.optimization_barrier(jnp.sum(jnp.where(matches, weight_blocks, 0.0), axis=-1))
        places = jnp.cumsum(naming, axis=1) - naming
        select = ((naming[:, None, :] == 1) & (places[:, None, :] == slot_ids[None, :, None])).astype(jnp.float32)
        rows_tok = jnp.einsum('bpt,btd->bpd', select, normed, precision=highest).reshape(blocks * CAP, D)
        rows_cot = jnp.einsum('bpt,btd->bpd', select, cot_blocks, precision=highest).reshape(blocks * CAP, D)
        rows_gate = jnp.einsum('bpt,bt->bp', select, shares, precision=highest)
        first_row = expert * EXP_HID
        gate_w = gate_rows[first_row:first_row + EXP_HID].astype(jnp.float32)
        up_w = up_rows[first_row:first_row + EXP_HID].astype(jnp.float32)
        down_w = down_rows[first_row:first_row + EXP_HID].astype(jnp.float32)
        gate_act = jnp.dot(rows_tok, gate_w.T, precision=highest)
        up_act = jnp.dot(rows_tok, up_w.T, precision=highest)
        hidden = lax.optimization_barrier((jax.nn.silu(gate_act) * up_act).astype(jnp.bfloat16)).astype(jnp.float32)
        pieces = jnp.einsum('rmf,mfd->rmd', hidden.reshape(blocks * CAP, SPLIT, HID_DEV), down_w.reshape(SPLIT, HID_DEV, D), precision=highest)
        pieces = lax.optimization_barrier(pieces.astype(jnp.bfloat16)).astype(jnp.float32)
        expert_out = lax.optimization_barrier(jnp.sum(pieces, axis=1)).reshape(blocks, CAP, D)
        mixture = mixture + jnp.einsum('bpt,bp,bpd->btd', select, rows_gate, expert_out, precision=highest)
        gate_flat = rows_gate.reshape(blocks * CAP)
        weighted = lax.optimization_barrier((hidden * gate_flat[:, None]).astype(jnp.bfloat16)).astype(jnp.float32)
        grads.append(jnp.dot(weighted.T, rows_cot, precision=highest))
    result = (inputs.astype(jnp.float32) + mixture.reshape(TOKENS, D)).astype(jnp.bfloat16)
    return (result, jnp.concatenate(grads, axis=0))

def reference(arrivals, fresh, routes, gates, cotangent, norm_gain, w_gate, w_up, w_down):
    results = []
    grads = []
    for layer_num in range(LAYERS):
        row_out = []
        total = jnp.zeros((FLIGHT * EXP_HID, D), jnp.float32)
        for turn_num in range(STEPS):
            if turn_num == 0:
                inputs = arrivals[layer_num]
            elif layer_num == 0:
                inputs = fresh[turn_num - 1]
            else:
                inputs = results[layer_num - 1][turn_num - 1]
            output, grad_part = layer(inputs, routes[layer_num, turn_num], gates[layer_num, turn_num], cotangent[layer_num, turn_num], norm_gain[layer_num], w_gate[layer_num], w_up[layer_num], w_down[layer_num])
            row_out.append(output)
            total = total + grad_part
        results.append(row_out)
        grads.append(total)
    layer_out = jnp.stack([jnp.stack(row_out) for row_out in results])
    grad_down = jnp.stack(grads)
    return (layer_out, grad_down)
```

```python
import functools

import jax
import jax.numpy as jnp
from jax import lax
from jax.experimental import pallas as pl
from jax.experimental.pallas import tpu as pltpu
from jax.sharding import PartitionSpec as P

SPLIT = 4
CAP = 12
SLOTS = 16
MESH = pl.DeviceIdType.MESH
NT = (((1,), (1,)), ((), ()))
TN = (((0,), (0,)), ((), ()))
F32 = jnp.float32
BF16 = jnp.bfloat16


def kernel_body(
    nsec, nexp, ndp,
    arr, fresh, routes, gates, cot, gain, wg, wu, wd,
    out, grad_out,
    xin, cin, wbuf, tsend, trecv, csend, crecv, cotx, hid, dsend, drecv, rsend, rrecv,
    mix, obuf, gacc,
    lsem, wss, wrs, fss, frs, tss, trs, tds, tdr, css, crs, cxs, cxr, cds, cdr,
    hss, hrs, dss, drs, rss, rrs, zss, zrs,
):
    s = lax.axis_index("section")
    i = lax.axis_index("expert")
    d = lax.axis_index("dp")
    ny = nexp // 2
    y = lax.div(i, 2)
    c = lax.rem(i, 2)
    tok, width = arr.shape
    hidn, cols = wg.shape
    half = hidn // 2
    flight = nexp // SPLIT
    rows = flight * SLOTS

    def at_x(k):
        return (s, i, lax.rem(d + k, ndp))

    def at_y(k):
        return (s, lax.rem(y + k, ny) * 2 + c, d)

    def ysrc(k):
        return lax.rem(y + ny - k, ny)

    partner = (s, y * 2 + 1 - c, d)

    def colsl(x):
        return pl.ds(pl.multiple_of(x * cols, cols), cols)

    def rc(src, dst, ss, rs, dev):
        return pltpu.make_async_remote_copy(
            src_ref=src, dst_ref=dst, send_sem=ss, recv_sem=rs, device_id=dev, device_id_type=MESH
        )

    sends = []

    def go(cp):
        cp.start()
        sends.append(cp)
        return cp

    l_arr = pltpu.make_async_copy(arr, xin.at[0], lsem.at[0])
    l_cot = pltpu.make_async_copy(cot, cin, lsem.at[1])
    l_w = [
        pltpu.make_async_copy(w, wbuf.at[m, :, colsl(d)], lsem.at[2 + m])
        for m, w in enumerate((wg, wu, wd))
    ]
    l_fresh = pltpu.make_async_copy(fresh, xin.at[1], lsem.at[5])
    l_arr.start()
    for l in l_w:
        l.start()
    l_cot.start()

    @pl.when(s == 0)
    def _():
        l_fresh.start()

    bar = pltpu.get_barrier_semaphore()
    peers = [at_x(k) for k in range(1, ndp)] + [at_y(k) for k in range(1, ny)] + [partner]
    for p in peers:
        pl.semaphore_signal(bar, inc=1, device_id=p, device_id_type=MESH)

    @pl.when(s > 0)
    def _():
        pl.semaphore_signal(bar, inc=1, device_id=(s - 1, i, d), device_id_type=MESH)

    @pl.when(s < nsec - 1)
    def _():
        pl.semaphore_signal(bar, inc=1, device_id=(s + 1, i, d), device_id_type=MESH)

    slot = lax.rem(lax.broadcasted_iota(jnp.int32, (rows, tok), 0), SLOTS)
    ia = lax.broadcasted_iota(jnp.int32, (tok, tok), 0)
    ib = lax.broadcasted_iota(jnp.int32, (tok, tok), 1)
    before = (ia < ib).astype(F32).astype(BF16)
    eye = (ia == ib).astype(F32).astype(BF16)
    sels, selgs = [], []
    for k in range(2):
        r = routes[k]
        g = gates[k]
        names, shares = [], []
        for e in range(flight):
            m = r == e
            nm = jnp.max(jnp.where(m, 1.0, 0.0), axis=0, keepdims=True)
            sh = jnp.sum(jnp.where(m, g, 0.0), axis=0, keepdims=True)
            names.append(jnp.broadcast_to(nm, (SLOTS, tok)))
            shares.append(jnp.broadcast_to(sh, (SLOTS, tok)))
        naming = jnp.concatenate(names, axis=0)
        share = jnp.concatenate(shares, axis=0)
        places = jnp.dot(naming.astype(BF16), before, preferred_element_type=F32)
        chosen = (naming > 0.5) & (jnp.abs(places - slot.astype(F32)) < 0.5) & (slot < CAP)
        sel = jnp.where(chosen, 1.0, 0.0).astype(BF16)
        selg = jnp.where(chosen, share, 0.0).astype(BF16)
        sels.append(sel)
        selgs.append(selg)
        g3 = selg.reshape(flight, 1, SLOTS, tok)
        g3 = jnp.concatenate([g3, g3], axis=1).reshape(2 * rows, tok)
        mix[k] = lax.dot_general(eye, g3, NT, preferred_element_type=F32).astype(BF16)

    pl.semaphore_wait(
        bar,
        len(peers) + jnp.where(s > 0, 1, 0) + jnp.where(s < nsec - 1, 1, 0),
    )

    def send_w(m, w):
        for j, k in enumerate((1, ndp - 1)):
            go(rc(w, wbuf.at[m, :, colsl(d)], wss.at[m, j], wrs.at[m, j], at_x(k)))

    def forward_w(m, w):
        for j, k in enumerate((1, ndp - 1)):
            owner = lax.rem(d + ndp - k, ndp)
            rc(w, wbuf.at[m, :, colsl(owner)], wss.at[m, j], wrs.at[m, j], at_x(k)).wait_recv()
            part = wbuf.at[m, pl.ds(j * half, half), colsl(owner)]
            go(rc(part, part, fss.at[m, j], frs.at[m, j], at_x(k)))

    def wait_far(m):
        owner = lax.rem(d + 2, ndp)
        for j, k in enumerate((1, ndp - 1)):
            part = wbuf.at[m, pl.ds(j * half, half), colsl(owner)]
            rc(part, part, fss.at[m, j], frs.at[m, j], at_x(k)).wait_recv()

    send_w(0, wg)
    send_w(1, wu)

    gains = gain[...]

    def dispatch(k):
        x = xin[k].astype(F32)
        scale = lax.rsqrt(jnp.mean(x * x, axis=1, keepdims=True) + 0.5)
        normed = (x * scale * gains).astype(BF16)
        picked = jnp.dot(sels[k], normed, preferred_element_type=F32).astype(BF16)
        tsend[k] = picked.reshape(flight, SLOTS, width)
        own = tsend.at[k, lax.div(y, 2)]
        for n in range(1, ny):
            dest = lax.rem(y + n, ny)
            go(rc(tsend.at[k, lax.div(dest, 2)], trecv.at[k, 0, y], tss.at[k, n], trs.at[k, n], at_y(n)))
        go(rc(own, trecv.at[k, 1, y], tds.at[k, 0], tdr.at[k, 0], partner))
        trecv[k, 0, y] = tsend[k, lax.div(y, 2)]

    def spread(k):
        for n in range(1, ny):
            blk = trecv.at[k, 0, ysrc(n)]
            rc(blk, blk, tss.at[k, n], trs.at[k, n], at_y(n)).wait_recv()
            go(rc(blk, trecv.at[k, 1, ysrc(n)], tds.at[k, n], tdr.at[k, n], partner))
    def wait_spread(k):
        for n in range(ny):
            blk = trecv.at[k, 1, ysrc(n)]
            rc(blk, blk, tds.at[k, n], tdr.at[k, n], partner).wait_recv()

    l_arr.wait()
    dispatch(0)

    l_cot.wait()
    for k in range(2):
        picked = jnp.dot(selgs[k], cin[k], preferred_element_type=F32).astype(BF16)
        csend[:, pl.ds(k * SLOTS, SLOTS), :] = picked.reshape(flight, SLOTS, width)
    for n in range(1, ny):
        dest = lax.rem(y + n, ny)
        go(rc(csend.at[lax.div(dest, 2)], crecv.at[y], css.at[n], crs.at[n], at_y(n)))
    crecv[y] = csend[lax.div(y, 2)]

    forward_w(0, wg)
    spread(0)
    forward_w(1, wu)
    send_w(2, wd)
    wait_spread(0)

    def gate_up(k):
        x = trecv[k].reshape(nexp * SLOTS, width)
        ga = lax.dot_general(wbuf[0], x, NT, preferred_element_type=F32)
        ua = lax.dot_general(wbuf[1], x, NT, preferred_element_type=F32)
        h = (ga / (1.0 + jnp.exp(-ga)) * ua).astype(BF16)
        hid[k, d] = h
        for n in range(1, ndp):
            go(rc(hid.at[k, d], hid.at[k, d], hss.at[k, n], hrs.at[k, n], at_x(n)))
        return h

    def down(k, h):
        hrows = nexp * SLOTS // 2

        def finish(r):
            rc(dsend.at[k, r], drecv.at[k, r], dss.at[k, r], drs.at[k, r], partner).wait_recv()
            total = (rsend[k, r].reshape(hrows, cols).astype(F32) + drecv[k, r].astype(F32)).astype(BF16)
            rsend[k, r] = total.reshape(ny, SLOTS, cols)
            for n in range(1, ny):
                go(rc(rsend.at[k, r, lax.rem(y + n, ny)], rrecv.at[k, r, y], rss.at[k, r, n], rrs.at[k, r, n], at_y(n)))
            rrecv[k, r, y] = rsend[k, r, y]

        for r in range(ndp):
            if k == 0 and r == 1:
                forward_w(2, wd)
            if k == 0 and r == 3:
                wait_far(2)
            off = (0, 1, 3, 2)[r]
            x = lax.rem(d + off, ndp)
            part = lax.dot_general(h, wbuf[2, :, colsl(x)], TN, preferred_element_type=F32).astype(BF16)
            dsend[k, r] = part[hrows:]
            go(rc(dsend.at[k, r], drecv.at[k, r], dss.at[k, r], drs.at[k, r], partner))
            rsend[k, r] = part[:hrows].reshape(ny, SLOTS, cols)
            if r > 0:
                finish(r - 1)
        finish(ndp - 1)

    def combine(k):
        for r in range(ndp):
            off = (0, 1, 3, 2)[r]
            cs = colsl(lax.rem(d + off, ndp))
            for n in range(1, ny):
                blk = rrecv.at[k, r, ysrc(n)]
                rc(blk, blk, rss.at[k, r, n], rrs.at[k, r, n], at_y(n)).wait_recv()
            got = rrecv[k, r].reshape(ny * SLOTS, cols)
            res = xin[k, :, cs].astype(F32) + jnp.dot(mix[k], got, preferred_element_type=F32)
            obuf[k, :, cs] = res.astype(BF16)
            if k == 0:
                @pl.when(s < nsec - 1)
                def _():
                    rc(obuf.at[0, :, cs], xin.at[1, :, cs], zss.at[r], zrs.at[r], (s + 1, i, d)).start()

    l_w[0].wait()
    l_w[1].wait()
    wait_far(0)
    wait_far(1)
    h0 = gate_up(0)
    l_w[2].wait()
    down(0, h0)

    for n in range(1, ny):
        blk = crecv.at[ysrc(n)]
        rc(blk, blk, css.at[n], crs.at[n], at_y(n)).wait_recv()
    for n in range(1, ndp):
        dest = lax.rem(d + n, ndp)
        go(rc(crecv.at[:, :, colsl(dest)], cotx.at[0, d], cxs.at[n], cxr.at[n], at_x(n)))
    cotx[0, d] = crecv[:, :, colsl(d)]
    go(rc(cotx.at[0, d], cotx.at[1, d], cds.at[0], cdr.at[0], partner))

    combine(0)
    out0 = pltpu.make_async_copy(obuf.at[0], out.at[0], lsem.at[6])
    out0.start()

    @pl.when(s > 0)
    def _():
        for r in range(ndp):
            cs = colsl(lax.rem(d + (0, 1, 3, 2)[r], ndp))
            rc(xin.at[1, :, cs], xin.at[1, :, cs], zss.at[r], zrs.at[r], (s - 1, i, d)).wait_recv()

    @pl.when(s == 0)
    def _():
        l_fresh.wait()

    dispatch(1)

    for n in range(1, ndp):
        x = lax.rem(d + ndp - n, ndp)
        rc(cotx.at[0, x], cotx.at[0, x], cxs.at[n], cxr.at[n], at_x(n)).wait_recv()
        go(rc(cotx.at[0, x], cotx.at[1, x], cds.at[n], cdr.at[n], partner))
    spread(1)

    def grad(k):
        for n in range(ndp):
            x = lax.rem(d + ndp - n, ndp)
            if k == 0:
                rc(cotx.at[1, x], cotx.at[1, x], cds.at[n], cdr.at[n], partner).wait_recv()
            if n > 0:
                rc(hid.at[k, x], hid.at[k, x], hss.at[k, n], hrs.at[k, n], at_x(n)).wait_recv()
            cr = cotx[:, x, :, pl.ds(k * SLOTS, SLOTS), :].reshape(nexp * SLOTS, cols)
            add = jnp.dot(hid[k, x], cr, preferred_element_type=F32)
            if k == 0 and n == 0:
                gacc[...] = add
            else:
                gacc[...] += add

    wait_spread(1)
    h1 = gate_up(1)
    down(1, h1)
    grad(0)
    grad(1)
    gout = pltpu.make_async_copy(gacc, grad_out, lsem.at[7])
    gout.start()
    combine(1)
    out1 = pltpu.make_async_copy(obuf.at[1], out.at[1], lsem.at[8])
    out1.start()
    for cp in sends:
        cp.wait_send()

    @pl.when(s < nsec - 1)
    def _():
        for r in range(ndp):
            cs = colsl(lax.rem(d + (0, 1, 3, 2)[r], ndp))
            rc(obuf.at[0, :, cs], xin.at[1, :, cs], zss.at[r], zrs.at[r], (s + 1, i, d)).wait_send()

    out0.wait()
    gout.wait()
    out1.wait()


def local(nsec, nexp, ndp, arrivals, fresh, routes, gates, cotangent, norm_gain, w_gate, w_up, w_down):
    tok, width = arrivals.shape[1:]
    hidn, cols = w_gate.shape[1:]
    flight = nexp // SPLIT
    ny = nexp // 2
    steps = routes.shape[1]
    rows = nexp * SLOTS
    routes_t = jnp.transpose(routes[0], (0, 2, 1))
    gates_t = jnp.transpose(gates[0], (0, 2, 1)).astype(F32)
    any_spec = pl.BlockSpec(memory_space=pl.ANY)
    vm_spec = pl.BlockSpec(memory_space=pltpu.VMEM)
    dma = pltpu.SemaphoreType.DMA
    out, grad = pl.pallas_call(
        functools.partial(kernel_body, nsec, nexp, ndp),
        name="moe_relay",
        out_shape=(
            jax.ShapeDtypeStruct((steps, tok, width), BF16),
            jax.ShapeDtypeStruct((hidn, cols), F32),
        ),
        in_specs=[any_spec, any_spec, vm_spec, vm_spec, any_spec, vm_spec, any_spec, any_spec, any_spec],
        out_specs=(any_spec, any_spec),
        scratch_shapes=[
            pltpu.VMEM((2, tok, width), BF16),
            pltpu.VMEM((2, tok, width), BF16),
            pltpu.VMEM((3, hidn, width), BF16),
            pltpu.VMEM((2, flight, SLOTS, width), BF16),
            pltpu.VMEM((2, 2, ny, SLOTS, width), BF16),
            pltpu.VMEM((flight, 2 * SLOTS, width), BF16),
            pltpu.VMEM((ny, 2 * SLOTS, width), BF16),
            pltpu.VMEM((2, ndp, ny, 2 * SLOTS, cols), BF16),
            pltpu.VMEM((2, ndp, hidn, rows), BF16),
            pltpu.VMEM((2, ndp, rows // 2, cols), BF16),
            pltpu.VMEM((2, ndp, rows // 2, cols), BF16),
            pltpu.VMEM((2, ndp, ny, SLOTS, cols), BF16),
            pltpu.VMEM((2, ndp, ny, SLOTS, cols), BF16),
            pltpu.VMEM((2, tok, ny * SLOTS), BF16),
            pltpu.VMEM((2, tok, width), BF16),
            pltpu.VMEM((hidn, cols), F32),
            dma((9,)),
            dma((3, 2)), dma((3, 2)), dma((3, 2)), dma((3, 2)),
            dma((2, ny)), dma((2, ny)), dma((2, ny)), dma((2, ny)),
            dma((ny,)), dma((ny,)), dma((ndp,)), dma((ndp,)), dma((ndp,)), dma((ndp,)),
            dma((2, ndp)), dma((2, ndp)), dma((2, ndp)), dma((2, ndp)),
            dma((2, ndp, ny)), dma((2, ndp, ny)), dma((ndp,)), dma((ndp,)),
        ],
        compiler_params=pltpu.CompilerParams(
            collective_id=0, has_side_effects=True, vmem_limit_bytes=60 * 1024 * 1024
        ),
    )(
        arrivals[0], fresh[0], routes_t, gates_t, cotangent[0], norm_gain, w_gate[0], w_up[0], w_down[0]
    )
    return out[None], grad[None]


def solution(mesh):
    placed = (
        P("section", ("expert", "dp"), None),
        P(None, ("expert", "dp"), None),
        P("section", None, ("expert", "dp"), None),
        P("section", None, ("expert", "dp"), None),
        P("section", None, ("expert", "dp"), None),
        P("section", None),
        P("section", "expert", "dp"),
        P("section", "expert", "dp"),
        P("section", "expert", "dp"),
    )
    return jax.shard_map(
        functools.partial(local, mesh.shape["section"], mesh.shape["expert"], mesh.shape["dp"]),
        mesh=mesh,
        in_specs=placed,
        out_specs=(P("section", None, ("expert", "dp"), None), P("section", "expert", "dp")),
        check_vma=False,
    )
```

```python
import functools

import jax
import jax.numpy as jnp
from jax import lax
from jax.experimental import pallas as pl
from jax.experimental.pallas import tpu as pltpu
from jax.sharding import PartitionSpec as P

SPLIT = 4
CAP = 12
SLOTS = 16
NEAR = (3, 5, 2, 6, 1, 7)
MESH = pl.DeviceIdType.MESH
NT = (((1,), (1,)), ((), ()))
TN = (((0,), (0,)), ((), ()))
F32 = jnp.float32
BF16 = jnp.bfloat16


def kernel_body(
    nsec, nexp, ndp,
    arr, fresh, routes, gates, cot, gain, wg, wu, wd,
    out, grad_out,
    xin, cin, wbuf, tsend, trecv, csend, crecv, cotx, hid, dsend, drecv, psum, rsend, mrecv, rrecv,
    rts, gts, selb, selg, mix, mixs, obuf, gacc,
    lsem, wss, wrs, fss, frs, tss, trs, tds, tdr, css, crs, cxs, cxr, cds, cdr,
    hss, hrs, dss, drs, mss, mrs, rss, rrs, zss, zrs,
):
    s = lax.axis_index("section")
    i = lax.axis_index("expert")
    d = lax.axis_index("dp")
    ny = nexp // 2
    y = lax.div(i, 2)
    c = lax.rem(i, 2)
    tok, width = arr.shape
    hidn, cols = wg.shape
    half = hidn // 2
    wide = tsend.shape[3]
    step = wide // 3
    rwide = rsend.shape[4]
    rstep = rwide // 3
    far = ny // 2
    near = [n for n in NEAR if 0 < n < ny and n != far]
    odd = lax.rem(y, 2)
    mate = y + 1 - 2 * odd
    mate_far = lax.rem(mate + far, ny)
    relay_n = far - 1 + 2 * odd
    mate_dev = (s, mate * 2 + c, d)
    flight = nexp // SPLIT
    rows = flight * SLOTS

    def at_x(k):
        return (s, i, lax.rem(d + k, ndp))

    def at_y(k):
        return (s, lax.rem(y + k, ny) * 2 + c, d)

    def ysrc(k):
        return lax.rem(y + ny - k, ny)

    partner = (s, y * 2 + 1 - c, d)

    def colsl(x):
        return pl.ds(pl.multiple_of(x * cols, cols), cols)

    def rc(src, dst, ss, rs, dev):
        return pltpu.make_async_remote_copy(
            src_ref=src, dst_ref=dst, send_sem=ss, recv_sem=rs, device_id=dev, device_id_type=MESH
        )

    sends = []

    def go(cp):
        cp.start()
        sends.append(cp)
        return cp

    l_arr = pltpu.make_async_copy(arr, xin.at[0], lsem.at[0])
    l_cot = pltpu.make_async_copy(cot, cin, lsem.at[1])
    l_w = [
        pltpu.make_async_copy(w, wbuf.at[m, :, colsl(d)], lsem.at[2 + m])
        for m, w in enumerate((wg, wu, wd))
    ]
    l_fresh = pltpu.make_async_copy(fresh, xin.at[1], lsem.at[5])
    l_rt = pltpu.make_async_copy(routes, rts, lsem.at[9])
    l_gt = pltpu.make_async_copy(gates, gts, lsem.at[10])
    l_rt.start()
    l_gt.start()
    l_arr.start()
    for l in l_w:
        l.start()
    l_cot.start()

    @pl.when(s == 0)
    def _():
        l_fresh.start()

    bar = pltpu.get_barrier_semaphore()
    peers = [at_x(k) for k in range(1, ndp)] + [at_y(n) for n in near] + [partner]
    for p in peers:
        pl.semaphore_signal(bar, inc=1, device_id=p, device_id_type=MESH)

    @pl.when(s > 0)
    def _():
        pl.semaphore_signal(bar, inc=1, device_id=(s - 1, i, d), device_id_type=MESH)

    @pl.when(s < nsec - 1)
    def _():
        pl.semaphore_signal(bar, inc=1, device_id=(s + 1, i, d), device_id_type=MESH)

    pos = lax.rem(lax.broadcasted_iota(jnp.int32, (rows, tok), 0), SLOTS)
    tail = SLOTS - CAP
    maps = [jnp.where(pos < CAP, pos, -5).astype(F32)]
    for q in range(3):
        maps.append(jnp.where(pos >= CAP, pos - CAP + tail * q, -5).astype(F32))
    ia = lax.broadcasted_iota(jnp.int32, (tok, tok), 0)
    ib = lax.broadcasted_iota(jnp.int32, (tok, tok), 1)
    before = (ia < ib).astype(F32).astype(BF16)
    eye = (ia == ib).astype(F32).astype(BF16)
    l_rt.wait()
    l_gt.wait()
    rt = rts[...]
    gt = gts[...].astype(F32)
    for k in range(2):
        r = rt[:, k, :]
        g = gt[:, k, :]
        names, shares = [], []
        for e in range(flight):
            m = r == e
            nm = jnp.max(jnp.where(m, 1.0, 0.0), axis=0, keepdims=True)
            sh = jnp.sum(jnp.where(m, g, 0.0), axis=0, keepdims=True)
            names.append(jnp.broadcast_to(nm, (SLOTS, tok)))
            shares.append(jnp.broadcast_to(sh, (SLOTS, tok)))
        naming = jnp.concatenate(names, axis=0)
        share = jnp.concatenate(shares, axis=0)
        places = jnp.dot(naming.astype(BF16), before, preferred_element_type=F32)
        picks, mixes = [], []
        for slot in maps:
            chosen = (naming > 0.5) & (jnp.abs(places - slot) < 0.5)
            picks.append(jnp.where(chosen, 1.0, 0.0).astype(BF16))
            g3 = jnp.where(chosen, share, 0.0).astype(BF16)
            if not mixes:
                selg[k] = g3
            g3 = g3.reshape(flight, 1, SLOTS, tok)
            g3 = jnp.concatenate([g3, g3], axis=1).reshape(2 * rows, tok)
            mixes.append(lax.dot_general(eye, g3, NT, preferred_element_type=F32).astype(BF16))
        mix[k] = mixes[0]
        mixs[k] = jnp.concatenate(mixes[1:], axis=1)
        for q in range(3):
            selb[k, q] = jnp.concatenate([picks[0], picks[q + 1]], axis=1)
        for r in range(ndp):
            rrecv[k, r, lax.rem(y + far, ny)] = jnp.zeros((SLOTS, rwide), BF16)

    pl.semaphore_wait(
        bar,
        len(peers) + jnp.where(s > 0, 1, 0) + jnp.where(s < nsec - 1, 1, 0),
    )

    def part_of(w, j, own):
        return w.at[pl.ds(j * half, half), colsl(own)] if own is not None else w.at[pl.ds(j * half, half)]

    def send_w(m, w):
        for q in range(2):
            for j, k in enumerate((1, ndp - 1)):
                p = j if q == 0 else 1 - j
                go(rc(part_of(w, p, None), part_of(wbuf.at[m], p, d), wss.at[m, j, q], wrs.at[m, j, q], at_x(k)))

    def forward_w(m):
        for j, k in enumerate((1, ndp - 1)):
            part = part_of(wbuf.at[m], j, lax.rem(d + ndp - k, ndp))
            rc(part, part, wss.at[m, j, 0], wrs.at[m, j, 0], at_x(k)).wait_recv()
            go(rc(part, part, fss.at[m, j], frs.at[m, j], at_x(k)))

    def wait_near(m):
        for j, k in enumerate((1, ndp - 1)):
            part = part_of(wbuf.at[m], 1 - j, lax.rem(d + ndp - k, ndp))
            rc(part, part, wss.at[m, j, 1], wrs.at[m, j, 1], at_x(k)).wait_recv()

    def wait_far(m):
        owner = lax.rem(d + 2, ndp)
        for j, k in enumerate((1, ndp - 1)):
            part = wbuf.at[m, pl.ds(j * half, half), colsl(owner)]
            rc(part, part, fss.at[m, j], frs.at[m, j], at_x(k)).wait_recv()

    send_w(0, wg)
    send_w(1, wu)

    gains = gain[...]

    def dispatch(k):
        x = xin[k].astype(F32)
        scale = lax.rsqrt(jnp.mean(x * x, axis=1, keepdims=True) + 0.5)
        normed = (x * scale * gains).astype(BF16)
        last = normed[:, wide:]
        for q in range(3):
            both = jnp.concatenate([normed[:, q * step : (q + 1) * step], last], axis=0)
            picked = jnp.dot(selb[k, q], both, preferred_element_type=F32).astype(BF16)
            tsend[k, :, :, q * step : (q + 1) * step] = picked.reshape(flight, SLOTS, step)
        own = tsend.at[k, lax.div(y, 2)]
        for n in near:
            dest = lax.rem(y + n, ny)
            go(rc(tsend.at[k, lax.div(dest, 2)], trecv.at[k, 0, y], tss.at[k, n], trs.at[k, n], at_y(n)))
        go(rc(own, trecv.at[k, 1, y], tds.at[k, 0], tdr.at[k, 0], partner))
        trecv[k, 0, y] = tsend[k, lax.div(y, 2)]

    def spread(k):
        blk = trecv.at[k, 0, mate_far]
        rc(blk, blk, tss.at[k, relay_n], trs.at[k, relay_n], mate_dev).wait_recv()
        go(rc(blk, blk, tss.at[k, far], trs.at[k, far], mate_dev))
        go(rc(blk, trecv.at[k, 1, mate_far], tds.at[k, relay_n], tdr.at[k, relay_n], partner))
        for n in near[::-1]:
            blk = trecv.at[k, 0, ysrc(n)]
            if n in (far - 1, far + 1):
                @pl.when(relay_n != n)
                def _(n=n, blk=blk):
                    rc(blk, blk, tss.at[k, n], trs.at[k, n], at_y(n)).wait_recv()
                    rc(blk, trecv.at[k, 1, ysrc(n)], tds.at[k, n], tdr.at[k, n], partner).start()
            else:
                rc(blk, blk, tss.at[k, n], trs.at[k, n], at_y(n)).wait_recv()
                go(rc(blk, trecv.at[k, 1, ysrc(n)], tds.at[k, n], tdr.at[k, n], partner))
        blk = trecv.at[k, 0, ysrc(far)]
        rc(blk, blk, tss.at[k, far], trs.at[k, far], mate_dev).wait_recv()
        go(rc(blk, trecv.at[k, 1, ysrc(far)], tds.at[k, far], tdr.at[k, far], partner))

    late = []

    def wait_spread(k):
        for n in range(ny):
            blk = trecv.at[k, 1, ysrc(n)]
            rc(blk, blk, tds.at[k, n], tdr.at[k, n], partner).wait_recv()
        other = 2 * far - relay_n
        blk = trecv.at[k, 0, ysrc(other)]
        late.append(rc(blk, blk, tds.at[k, other], tdr.at[k, other], partner))

    l_arr.wait()
    dispatch(0)

    l_cot.wait()
    for k in range(2):
        picked = jnp.dot(selg[k], cin[k], preferred_element_type=F32).astype(BF16)
        csend[:, pl.ds(k * SLOTS, SLOTS), :] = picked.reshape(flight, SLOTS, width)
    for n in near:
        dest = lax.rem(y + n, ny)
        go(rc(csend.at[lax.div(dest, 2)], crecv.at[y], css.at[n], crs.at[n], at_y(n)))
    crecv[y] = csend[lax.div(y, 2)]

    spread(0)
    forward_w(0)
    forward_w(1)
    send_w(2, wd)
    blk = crecv.at[mate_far]
    rc(blk, blk, css.at[relay_n], crs.at[relay_n], mate_dev).wait_recv()
    go(rc(blk, blk, css.at[far], crs.at[far], mate_dev))
    wait_spread(0)

    def gate_up(k):
        count = nexp * SLOTS
        pieces = [trecv[k, :, :, :, q * step : (q + 1) * step].reshape(count, step) for q in range(3)]
        tails = [trecv[k, :, :, 8:, q * step : (q + 1) * step].astype(F32).reshape(count // 2, step) for q in range(3)]
        low = lax.rem(lax.broadcasted_iota(jnp.int32, (count // 2, step), 0), 8) < 4
        first = jnp.where(low, turned(tails[0]), tails[1])
        second = turned(tails[2])
        merged = jnp.concatenate(
            [first.reshape(nexp, 1, 8, step), second.reshape(nexp, 1, 8, step)], axis=1
        ).reshape(count, step)
        x = jnp.concatenate(pieces + [merged.astype(BF16)], axis=1)
        ga = lax.dot_general(wbuf[0], x, NT, preferred_element_type=F32)
        ua = lax.dot_general(wbuf[1], x, NT, preferred_element_type=F32)
        h = (ga / (1.0 + jnp.exp(-ga)) * ua).astype(BF16)
        hid[k, d] = h
        return h

    def turned(v):
        n, w = v.shape
        return pltpu.roll(v.reshape(n // 8, 8, w), 4, 1).reshape(n, w)

    def share_hidden(k):
        for n in range(1, ndp):
            go(rc(hid.at[k, d], hid.at[k, d], hss.at[k, n], hrs.at[k, n], at_x(n)))

    def down(k, h):
        hrows = nexp * SLOTS // 2

        def direct(r, n, dest):
            return rc(rsend.at[k, r, dest], rrecv.at[k, r, y], rss.at[k, r, n], rrs.at[k, r, n], at_y(n))

        def finish(r):
            rc(dsend.at[k, r], drecv.at[k, r], dss.at[k, r], drs.at[k, r], partner).wait_recv()
            total = psum[r] + drecv[k, r].astype(F32)
            t4 = total.reshape(ny, 2, 8, cols)
            lo, hi = t4[:, 0].reshape(ny * 8, cols), t4[:, 1].reshape(ny * 8, cols)
            lo3, hi3 = lo[:, rwide:], hi[:, rwide:]
            fill = jnp.concatenate([turned(lo3), lo3, turned(hi3)], axis=1)
            low = lax.rem(lax.broadcasted_iota(jnp.int32, (ny * 8, rwide), 0), 8) < 4
            hi = jnp.where(low, hi[:, :rwide], fill)
            packed = jnp.concatenate(
                [lo[:, :rwide].reshape(ny, 1, 8, rwide), hi.reshape(ny, 1, 8, rwide)], axis=1
            )
            rsend[k, r] = packed.reshape(ny, SLOTS, rwide).astype(BF16)
            go(rc(rsend.at[k, r, lax.rem(y + far, ny)], mrecv.at[k, r], mss.at[k, r], mrs.at[k, r], mate_dev))
            for n in near:
                if n in (far - 1, far + 1):
                    @pl.when(2 * far - relay_n != n)
                    def _(n=n):
                        direct(r, n, lax.rem(y + n, ny)).start()
                else:
                    go(direct(r, n, lax.rem(y + n, ny)))
            rrecv[k, r, y] = rsend[k, r, y]

        def finish_far(r):
            rc(mrecv.at[k, r], mrecv.at[k, r], mss.at[k, r], mrs.at[k, r], mate_dev).wait_recv()
            both = rsend[k, r, mate_far].astype(F32) + mrecv[k, r].astype(F32)
            rsend[k, r, mate_far] = both.astype(BF16)
            n = 2 * far - relay_n
            dest = (s, mate_far * 2 + c, d)
            rc(rsend.at[k, r, mate_far], rrecv.at[k, r, y], rss.at[k, r, n], rrs.at[k, r, n], dest).start()
            for n in (far - 1, far + 1):
                late.append(direct(r, n, lax.rem(y + n, ny)))

        for r in range(ndp):
            if k == 0 and r == 1:
                forward_w(2)
                share_hidden(0)
                wait_near(2)
            if k == 0 and r == 3:
                wait_far(2)
            off = (0, 1, 3, 2)[r]
            x = lax.rem(d + off, ndp)
            part = lax.dot_general(h, wbuf[2, :, colsl(x)], TN, preferred_element_type=F32)
            dsend[k, r] = part[hrows:].astype(BF16)
            go(rc(dsend.at[k, r], drecv.at[k, r], dss.at[k, r], drs.at[k, r], partner))
            psum[r] = part[:hrows]
            if r > 0:
                finish(r - 1)
            if r > 1:
                finish_far(r - 2)
        finish(ndp - 1)
        finish_far(ndp - 2)
        finish_far(ndp - 1)

    def combine(k):
        for r in range(ndp):
            off = (0, 1, 3, 2)[r]
            cs = colsl(lax.rem(d + off, ndp))
            for n in near[::-1]:
                blk = rrecv.at[k, r, ysrc(n)]
                rc(blk, blk, rss.at[k, r, n], rrs.at[k, r, n], at_y(n)).wait_recv()
            got = rrecv[k, r].reshape(ny * SLOTS, rwide)
            folded = jnp.concatenate([got[:, q * rstep : (q + 1) * rstep] for q in range(3)], axis=0)
            res = xin[k, :, cs].astype(F32) + jnp.concatenate(
                [
                    jnp.dot(mix[k], got, preferred_element_type=F32),
                    jnp.dot(mixs[k], folded, preferred_element_type=F32),
                ],
                axis=1,
            )
            obuf[k, :, cs] = res.astype(BF16)
            if k == 0:
                @pl.when(s < nsec - 1)
                def _():
                    rc(obuf.at[0, :, cs], xin.at[1, :, cs], zss.at[r], zrs.at[r], (s + 1, i, d)).start()

    l_w[0].wait()
    l_w[1].wait()
    wait_near(0)
    wait_near(1)
    wait_far(0)
    wait_far(1)
    h0 = gate_up(0)
    l_w[2].wait()
    down(0, h0)

    for n in near:
        if n in (far - 1, far + 1):
            @pl.when(relay_n != n)
            def _(n=n):
                blk = crecv.at[ysrc(n)]
                rc(blk, blk, css.at[n], crs.at[n], at_y(n)).wait_recv()
        else:
            blk = crecv.at[ysrc(n)]
            rc(blk, blk, css.at[n], crs.at[n], at_y(n)).wait_recv()
    blk = crecv.at[ysrc(far)]
    rc(blk, blk, css.at[far], crs.at[far], mate_dev).wait_recv()
    for n in range(1, ndp):
        dest = lax.rem(d + n, ndp)
        go(rc(crecv.at[:, :, colsl(dest)], cotx.at[0, d], cxs.at[n], cxr.at[n], at_x(n)))
    cotx[0, d] = crecv[:, :, colsl(d)]
    go(rc(cotx.at[0, d], cotx.at[1, d], cds.at[0], cdr.at[0], partner))

    combine(0)
    out0 = pltpu.make_async_copy(obuf.at[0], out.at[0], lsem.at[6])
    out0.start()

    @pl.when(s > 0)
    def _():
        for r in range(ndp):
            cs = colsl(lax.rem(d + (0, 1, 3, 2)[r], ndp))
            rc(xin.at[1, :, cs], xin.at[1, :, cs], zss.at[r], zrs.at[r], (s - 1, i, d)).wait_recv()

    @pl.when(s == 0)
    def _():
        l_fresh.wait()

    dispatch(1)

    for n in range(1, ndp):
        x = lax.rem(d + ndp - n, ndp)
        rc(cotx.at[0, x], cotx.at[0, x], cxs.at[n], cxr.at[n], at_x(n)).wait_recv()
        go(rc(cotx.at[0, x], cotx.at[1, x], cds.at[n], cdr.at[n], partner))
    spread(1)

    def grad(k):
        for n in range(ndp):
            x = lax.rem(d + ndp - n, ndp)
            if k == 0:
                rc(cotx.at[1, x], cotx.at[1, x], cds.at[n], cdr.at[n], partner).wait_recv()
            if n > 0:
                rc(hid.at[k, x], hid.at[k, x], hss.at[k, n], hrs.at[k, n], at_x(n)).wait_recv()
            cr = cotx[:, x, :, pl.ds(k * SLOTS, SLOTS), :].reshape(nexp * SLOTS, cols)
            add = jnp.dot(hid[k, x], cr, preferred_element_type=F32)
            if k == 0 and n == 0:
                gacc[...] = add
            else:
                gacc[...] += add

    wait_spread(1)
    h1 = gate_up(1)
    share_hidden(1)
    down(1, h1)
    grad(0)
    grad(1)
    gout = pltpu.make_async_copy(gacc, grad_out, lsem.at[7])
    gout.start()
    combine(1)
    out1 = pltpu.make_async_copy(obuf.at[1], out.at[1], lsem.at[8])
    out1.start()
    for cp in sends + late:
        cp.wait_send()

    @pl.when(s < nsec - 1)
    def _():
        for r in range(ndp):
            cs = colsl(lax.rem(d + (0, 1, 3, 2)[r], ndp))
            rc(obuf.at[0, :, cs], xin.at[1, :, cs], zss.at[r], zrs.at[r], (s + 1, i, d)).wait_send()

    out0.wait()
    gout.wait()
    out1.wait()


def local(nsec, nexp, ndp, arrivals, fresh, routes, gates, cotangent, norm_gain, w_gate, w_up, w_down):
    tok, width = arrivals.shape[1:]
    hidn, cols = w_gate.shape[1:]
    flight = nexp // SPLIT
    ny = nexp // 2
    steps = routes.shape[1]
    rows = nexp * SLOTS
    routes_t = jnp.transpose(routes[0], (2, 0, 1))
    gates_t = jnp.transpose(gates[0], (2, 0, 1))
    wide = width // 4 * 3
    rwide = cols // 4 * 3
    any_spec = pl.BlockSpec(memory_space=pl.ANY)
    vm_spec = pl.BlockSpec(memory_space=pltpu.VMEM)
    dma = pltpu.SemaphoreType.DMA
    out, grad = pl.pallas_call(
        functools.partial(kernel_body, nsec, nexp, ndp),
        name="moe_relay",
        out_shape=(
            jax.ShapeDtypeStruct((steps, tok, width), BF16),
            jax.ShapeDtypeStruct((hidn, cols), F32),
        ),
        in_specs=[any_spec, any_spec, any_spec, any_spec, any_spec, vm_spec, any_spec, any_spec, any_spec],
        out_specs=(any_spec, any_spec),
        scratch_shapes=[
            pltpu.VMEM((2, tok, width), BF16),
            pltpu.VMEM((2, tok, width), BF16),
            pltpu.VMEM((3, hidn, width), BF16),
            pltpu.VMEM((2, flight, SLOTS, wide), BF16),
            pltpu.VMEM((2, 2, ny, SLOTS, wide), BF16),
            pltpu.VMEM((flight, 2 * SLOTS, width), BF16),
            pltpu.VMEM((ny, 2 * SLOTS, width), BF16),
            pltpu.VMEM((2, ndp, ny, 2 * SLOTS, cols), BF16),
            pltpu.VMEM((2, ndp, hidn, rows), BF16),
            pltpu.VMEM((2, ndp, rows // 2, cols), BF16),
            pltpu.VMEM((2, ndp, rows // 2, cols), BF16),
            pltpu.VMEM((ndp, rows // 2, cols), F32),
            pltpu.VMEM((2, ndp, ny, SLOTS, rwide), BF16),
            pltpu.VMEM((2, ndp, SLOTS, rwide), BF16),
            pltpu.VMEM((2, ndp, ny, SLOTS, rwide), BF16),
            pltpu.VMEM(routes_t.shape, jnp.int32),
            pltpu.VMEM(gates_t.shape, BF16),
            pltpu.VMEM((2, 3, flight * SLOTS, 2 * tok), BF16),
            pltpu.VMEM((2, flight * SLOTS, tok), BF16),
            pltpu.VMEM((2, tok, ny * SLOTS), BF16),
            pltpu.VMEM((2, tok, 3 * ny * SLOTS), BF16),
            pltpu.VMEM((2, tok, width), BF16),
            pltpu.VMEM((hidn, cols), F32),
            dma((11,)),
            dma((3, 2, 2)), dma((3, 2, 2)), dma((3, 2)), dma((3, 2)),
            dma((2, ny)), dma((2, ny)), dma((2, ny)), dma((2, ny)),
            dma((ny,)), dma((ny,)), dma((ndp,)), dma((ndp,)), dma((ndp,)), dma((ndp,)),
            dma((2, ndp)), dma((2, ndp)), dma((2, ndp)), dma((2, ndp)), dma((2, ndp)), dma((2, ndp)),
            dma((2, ndp, ny)), dma((2, ndp, ny)), dma((ndp,)), dma((ndp,)),
        ],
        compiler_params=pltpu.CompilerParams(
            collective_id=0, has_side_effects=True, vmem_limit_bytes=60 * 1024 * 1024
        ),
    )(
        arrivals[0], fresh[0], routes_t, gates_t, cotangent[0], norm_gain, w_gate[0], w_up[0], w_down[0]
    )
    return out[None], grad[None]


def solution(mesh):
    placed = (
        P("section", ("expert", "dp"), None),
        P(None, ("expert", "dp"), None),
        P("section", None, ("expert", "dp"), None),
        P("section", None, ("expert", "dp"), None),
        P("section", None, ("expert", "dp"), None),
        P("section", None),
        P("section", "expert", "dp"),
        P("section", "expert", "dp"),
        P("section", "expert", "dp"),
    )
    return jax.shard_map(
        functools.partial(local, mesh.shape["section"], mesh.shape["expert"], mesh.shape["dp"]),
        mesh=mesh,
        in_specs=placed,
        out_specs=(P("section", None, ("expert", "dp"), None), P("section", "expert", "dp")),
        check_vma=False,
    )
```

```python
import functools

import jax
import jax.numpy as jnp
from jax import lax
from jax.experimental import pallas as pl
from jax.experimental.pallas import tpu as pltpu
from jax.sharding import PartitionSpec as P

SPLIT = 4
CAP = 12
SLOTS = 16
NEAR = (3, 5, 2, 6, 1, 7)
ORDER = (0, 1, 3, 2)
MESH = pl.DeviceIdType.MESH
NT = (((1,), (1,)), ((), ()))
TN = (((0,), (0,)), ((), ()))
F32 = jnp.float32
BF16 = jnp.bfloat16


def kernel_body(
    nsec, nexp, ndp,
    arr, fresh, routes, gates, cot, gain, wg, wu, wd,
    out, grad_out,
    xin, cin, wbuf, tsend, trecv, xraw, csend, crecv, cstage, cotx, hid, dsend, drecv, psum, rsend, mrecv, rrecv,
    rts, gts, gns, selb, selgb, mix, mixs, obuf, gacc,
    lsem, sends, wrs, wns, frs, trs, tdr, crs, cxr, cgr, cfr, cdr, hrs, hns, hfr, drs, mrs, rrs, zrs,
):
    s = lax.axis_index("section")
    i = lax.axis_index("expert")
    d = lax.axis_index("dp")
    ny = nexp // 2
    y = lax.div(i, 2)
    c = lax.rem(i, 2)
    tok, width = arr.shape
    hidn, cols = wg.shape
    half = hidn // 2
    rwide = rsend.shape[4]
    rstep = rwide // 3
    far = ny // 2
    near = [n for n in NEAR if 0 < n < ny and n != far]
    odd = lax.rem(y, 2)
    mate = y + 1 - 2 * odd
    mate_far = lax.rem(mate + far, ny)
    relay_n = far - 1 + 2 * odd
    mate_dev = (s, mate * 2 + c, d)
    flight = nexp // SPLIT
    rows = flight * SLOTS

    def at_x(k):
        return (s, i, lax.rem(d + k, ndp))

    def at_y(k):
        return (s, lax.rem(y + k, ny) * 2 + c, d)

    def ysrc(k):
        return lax.rem(y + ny - k, ny)

    partner = (s, y * 2 + 1 - c, d)

    def colsl(x):
        return pl.ds(pl.multiple_of(x * cols, cols), cols)

    def rc(src, dst, ss, rs, dev):
        return pltpu.make_async_remote_copy(
            src_ref=src, dst_ref=dst, send_sem=ss, recv_sem=rs, device_id=dev, device_id_type=MESH
        )

    s_w, s_t, s_c, s_x, s_h, s_d, s_m, s_r, s_z = (sends.at[n] for n in range(9))

    def drain(sem, ref):
        rc(ref, ref, sem, sem, partner).wait_send()

    def arrived(sem, ref):
        rc(ref, ref, sem, sem, partner).wait_recv()

    l_arr = pltpu.make_async_copy(arr, xin.at[0], lsem.at[0])
    l_cot = pltpu.make_async_copy(cot, cin, lsem.at[1])
    l_w = [
        pltpu.make_async_copy(w, wbuf.at[m, :, colsl(d)], lsem.at[2 + m])
        for m, w in enumerate((wg, wu, wd))
    ]
    l_fresh = pltpu.make_async_copy(fresh, xin.at[1], lsem.at[5])
    l_rt = pltpu.make_async_copy(routes, rts, lsem.at[9])
    l_gt = pltpu.make_async_copy(gates, gts, lsem.at[10])
    l_gn = pltpu.make_async_copy(gain, gns, lsem.at[11])
    l_gn.start()
    l_rt.start()
    l_gt.start()
    l_arr.start()
    for l in l_w:
        l.start()
    l_cot.start()

    @pl.when(s == 0)
    def _():
        l_fresh.start()

    bar = pltpu.get_barrier_semaphore()
    peers = [at_x(k) for k in range(1, ndp)] + [at_y(n) for n in near] + [partner]
    for p in peers:
        pl.semaphore_signal(bar, inc=1, device_id=p, device_id_type=MESH)

    @pl.when(s > 0)
    def _():
        pl.semaphore_signal(bar, inc=1, device_id=(s - 1, i, d), device_id_type=MESH)

    @pl.when(s < nsec - 1)
    def _():
        pl.semaphore_signal(bar, inc=1, device_id=(s + 1, i, d), device_id_type=MESH)

    with jax.named_scope("bar"):
        pl.semaphore_wait(
            bar,
            len(peers) + jnp.where(s > 0, 1, 0) + jnp.where(s < nsec - 1, 1, 0),
        )

    def part_of(w, j, own):
        return w.at[pl.ds(j * half, half), colsl(own)] if own is not None else w.at[pl.ds(j * half, half)]

    def send_w(m, w):
        for q in range(2):
            for j, k in enumerate((1, ndp - 1)):
                p = j if q == 0 else 1 - j
                rs = wrs.at[m, j] if q == 0 else wns.at[m]
                rc(part_of(w, p, None), part_of(wbuf.at[m], p, d), s_w, rs, at_x(k)).start()

    def forward_w(m):
        for j, k in enumerate((1, ndp - 1)):
            part = part_of(wbuf.at[m], j, lax.rem(d + ndp - k, ndp))
            arrived(wrs.at[m, j], part)
            rc(part, part, s_w, frs.at[m], at_x(k)).start()

    def wait_near(m):
        arrived(wns.at[m], wbuf.at[m, :, pl.ds(0, cols)])

    def wait_far(m):
        arrived(frs.at[m], wbuf.at[m, :, pl.ds(0, cols)])

    send_w(0, wg)
    send_w(1, wu)

    pos = lax.rem(lax.broadcasted_iota(jnp.int32, (rows, tok), 0), SLOTS)
    tail = SLOTS - CAP
    maps = [jnp.where(pos < CAP, pos, -5).astype(F32)]
    for q in range(3):
        maps.append(jnp.where(pos >= CAP, pos - CAP + tail * q, -5).astype(F32))
    ia = lax.broadcasted_iota(jnp.int32, (tok, tok), 0)
    ib = lax.broadcasted_iota(jnp.int32, (tok, tok), 1)
    before = (ia < ib).astype(F32).astype(BF16)
    eye = (ia == ib).astype(F32).astype(BF16)
    l_rt.wait()
    l_gt.wait()
    rt = rts[...]
    gt = gts[...].astype(F32)

    def select(k):
        r = rt[:, k, :]
        g = gt[:, k, :]
        names, shares = [], []
        for e in range(flight):
            m = r == e
            nm = jnp.max(jnp.where(m, 1.0, 0.0), axis=0, keepdims=True)
            sh = jnp.sum(jnp.where(m, g, 0.0), axis=0, keepdims=True)
            names.append(jnp.broadcast_to(nm, (SLOTS, tok)))
            shares.append(jnp.broadcast_to(sh, (SLOTS, tok)))
        naming = jnp.concatenate(names, axis=0)
        share = jnp.concatenate(shares, axis=0)
        places = jnp.dot(naming.astype(BF16), before, preferred_element_type=F32)
        picks, gated, mixes = [], [], []
        for slot in maps:
            chosen = (naming > 0.5) & (jnp.abs(places - slot) < 0.5)
            picks.append(jnp.where(chosen, 1.0, 0.0).astype(BF16))
            g3 = jnp.where(chosen, share, 0.0).astype(BF16)
            gated.append(g3)
            g3 = g3.reshape(flight, 1, SLOTS, tok)
            g3 = jnp.concatenate([g3, g3], axis=1).reshape(2 * rows, tok)
            mixes.append(lax.dot_general(eye, g3, NT, preferred_element_type=F32).astype(BF16))
        mix[k] = mixes[0]
        mixs[k] = jnp.concatenate(mixes[1:], axis=1)
        for q in range(3):
            selb[k, q] = jnp.concatenate([picks[0], picks[q + 1]], axis=1)
            selgb[k, q] = jnp.concatenate([gated[0], gated[q + 1]], axis=1)

    def view(ref, m, *at):
        return ref.at[(0,) + at] if m == 0 else ref.at[(1,) + at + (m - 1,)]

    def block(r):
        return colsl(lax.rem(d + ORDER[r], ndp))

    def pick(sel, k, x, put):
        last = x[:, rwide:]
        for q in range(3):
            both = jnp.concatenate([x[:, q * rstep : (q + 1) * rstep], last], axis=0)
            got = jnp.dot(sel[k, q], both, preferred_element_type=F32).astype(BF16)
            put(pl.ds(q * rstep, rstep), got.reshape(flight, SLOTS, rstep))

    def dispatch(m):
        k = 0 if m == 0 else 1
        for r in range(ndp) if m == 0 else (m - 1,):

            def put(cs, v, r=r):
                tsend[k, :, r, :, cs] = v

            pick(selb, k, xin[k, :, block(r)], put)
        for n in near:
            dest = lax.rem(y + n, ny)
            src = view(tsend, m, lax.div(dest, 2))
            rc(src, view(trecv, m, 0, y), s_t, trs.at[m, n - 1], at_y(n)).start()
        own = view(tsend, m, lax.div(y, 2))
        rc(own, view(trecv, m, 1, y), s_t, tdr.at[m], partner).start()
        if m == 0:
            trecv[0, 0, y] = tsend[0, lax.div(y, 2)]
        else:
            trecv[1, 0, y, m - 1] = tsend[1, lax.div(y, 2), m - 1]

    def onward(m, src, n):
        blk = view(trecv, m, 0, src)
        arrived(trs.at[m, n - 1], blk)
        rc(blk, view(trecv, m, 1, src), s_t, tdr.at[m], partner).start()

    def relay(m):
        onward(m, mate_far, relay_n)
        blk = view(trecv, m, 0, mate_far)
        rc(blk, blk, s_t, trs.at[m, far - 1], mate_dev).start()

    def spread(m):
        for n in near[::-1]:
            if n in (far - 1, far + 1):

                @pl.when(relay_n != n)
                def _(n=n):
                    onward(m, ysrc(n), n)
            else:
                onward(m, ysrc(n), n)
        onward(m, ysrc(far), far)

    def wait_spread(m):
        arrived(tdr.at[m], trecv.at[0, 1] if m == 0 else trecv.at[1, 1, :, m - 1])

    count = nexp * SLOTS

    def turned(v):
        n, w = v.shape
        return pltpu.roll(v.reshape(n // 8, 8, w), 4, 1).reshape(n, w)

    low = lax.rem(lax.broadcasted_iota(jnp.int32, (count // 2, rstep), 0), 8) < 4

    def merge(get):
        tails = [
            get(pl.ds(8, 8), pl.ds(q * rstep, rstep)).astype(F32).reshape(count // 2, rstep) for q in range(3)
        ]
        first = jnp.where(low, turned(tails[0]), tails[1])
        second = turned(tails[2])
        return jnp.concatenate(
            [first.reshape(nexp, 1, 8, rstep), second.reshape(nexp, 1, 8, rstep)], axis=1
        ).reshape(count, rstep)

    def unpack(k, r):
        merged = merge(lambda rs, cs: trecv[k, :, :, r, rs, cs])
        main = trecv[k, :, :, r, :, :].reshape(count, rwide)
        xraw[:, block(r)] = jnp.concatenate([main, merged.astype(BF16)], axis=1)
        mf = main.astype(F32)
        return sum(
            (mf[:, q * rstep : (q + 1) * rstep] * mf[:, q * rstep : (q + 1) * rstep] for q in range(3)),
            merged * merged,
        )

    def gate_up(k, squares):
        total = jnp.sum(squares[0] + squares[1] + (squares[2] + squares[3]), axis=1, keepdims=True)
        scale = lax.rsqrt(total * (1.0 / width) + 0.5)
        x = (xraw[...].astype(F32) * scale * gns[...]).astype(BF16)
        ga = lax.dot_general(wbuf[0], x, NT, preferred_element_type=F32)
        ua = lax.dot_general(wbuf[1], x, NT, preferred_element_type=F32)
        kept = lax.rem(lax.broadcasted_iota(jnp.int32, ga.shape, 1), SLOTS) < CAP
        h = jnp.where(kept, ga / (1.0 + jnp.exp(-ga)) * ua, 0.0).astype(BF16)
        hid[k, d] = h
        return h

    def hid_half(k, x, p):
        return hid.at[k, x, pl.ds(p * half, half)]

    def share_hidden(k):
        for q in range(2):
            for j, n in enumerate((1, ndp - 1)):
                part = hid_half(k, d, j if q == 0 else 1 - j)
                rs = hrs.at[k, j] if q == 0 else hns.at[k]
                rc(part, part, s_h, rs, at_x(n)).start()

    def forward_hidden(k):
        for j, n in enumerate((1, ndp - 1)):
            part = hid_half(k, lax.rem(d + ndp - n, ndp), j)
            arrived(hrs.at[k, j], part)
            rc(part, part, s_h, hfr.at[k], at_x(n)).start()

    def wait_hidden(k):
        arrived(hns.at[k], hid.at[k, 0])
        arrived(hfr.at[k], hid.at[k, 0])

    hy = ny // 2

    def share_cot():
        across = lax.rem(d + 2, ndp)
        for j, n in enumerate((1, ndp - 1)):
            src = crecv.at[pl.ds(j * hy, hy), :, across]
            rc(src, cstage.at[j], s_x, cgr.at[j], at_x(n)).start()
        for j, n in enumerate((1, ndp - 1)):
            src = crecv.at[:, :, lax.rem(d + n, ndp)]
            rc(src, cotx.at[0, d], s_x, cxr.at[j], at_x(n)).start()
        cotx[0, d] = crecv[:, :, d]
        rc(cotx.at[0, d], cotx.at[1, d], s_x, cdr, partner).start()

    def forward_cot():
        for j, n in enumerate((1, ndp - 1)):
            arrived(cgr.at[j], cstage.at[j])
            dst = cotx.at[0, lax.rem(d + ndp - n, ndp), pl.ds(j * hy, hy)]
            rc(cstage.at[j], dst, s_x, cfr, at_x(n)).start()

    def spread_cot():
        for j, n in enumerate((1, ndp - 1)):
            x = lax.rem(d + ndp - n, ndp)
            arrived(cxr.at[j], cotx.at[0, x])
            rc(cotx.at[0, x], cotx.at[1, x], s_x, cdr, partner).start()
        x = lax.rem(d + 2, ndp)
        arrived(cfr, cotx.at[0, x])
        rc(cotx.at[0, x], cotx.at[1, x], s_x, cdr, partner).start()

    hrows = count // 2

    def direct(k, r, n, dest):
        return rc(rsend.at[k, r, dest], rrecv.at[k, r, y], s_r, rrs.at[k, r], at_y(n))

    def multiply(k, r, h):
        part = lax.dot_general(h, wbuf[2, :, block(r)], TN, preferred_element_type=F32)
        dsend[k, r] = part[hrows:].astype(BF16)
        rc(dsend.at[k, r], drecv.at[k, r], s_d, drs.at[k, r], partner).start()
        psum[r] = part[:hrows]

    def pack(k, r):
        with jax.named_scope(f"dw{k}{r}"):
            arrived(drs.at[k, r], drecv.at[k, r])
        total = psum[r] + drecv[k, r].astype(F32)
        t4 = total.reshape(ny, 2, 8, cols)
        lo, hi = t4[:, 0].reshape(ny * 8, cols), t4[:, 1].reshape(ny * 8, cols)
        lo3, hi3 = lo[:, rwide:], hi[:, rwide:]
        fill = jnp.concatenate([turned(lo3), lo3, turned(hi3)], axis=1)
        low = lax.rem(lax.broadcasted_iota(jnp.int32, (ny * 8, rwide), 0), 8) < 4
        hi = jnp.where(low, hi[:, :rwide], fill)
        packed = jnp.concatenate(
            [lo[:, :rwide].reshape(ny, 1, 8, rwide), hi.reshape(ny, 1, 8, rwide)], axis=1
        )
        rsend[k, r] = packed.reshape(ny, SLOTS, rwide).astype(BF16)
        rc(rsend.at[k, r, lax.rem(y + far, ny)], mrecv.at[k, r], s_m, mrs.at[k, r], mate_dev).start()

    def straight(k, r):
        for n in near:
            if n in (far - 1, far + 1):

                @pl.when(2 * far - relay_n != n)
                def _(n=n):
                    direct(k, r, n, lax.rem(y + n, ny)).start()
            else:
                direct(k, r, n, lax.rem(y + n, ny)).start()
        rrecv[k, r, y] = rsend[k, r, y]

    def finish_far(k, r):
        with jax.named_scope(f"mw{k}{r}"):
            arrived(mrs.at[k, r], mrecv.at[k, r])
        both = rsend[k, r, mate_far].astype(F32) + mrecv[k, r].astype(F32)
        rsend[k, r, mate_far] = both.astype(BF16)
        dest = (s, mate_far * 2 + c, d)
        rc(rsend.at[k, r, mate_far], rrecv.at[k, r, y], s_r, rrs.at[k, r], dest).start()

    def zcopy(r, sec):
        cs = block(r)
        return rc(obuf.at[0, :, cs], xin.at[1, :, cs], s_z, zrs.at[r], (sec, i, d))

    def combine(k, r):
        cs = block(r)
        with jax.named_scope(f"rw{k}{r}"):
            arrived(rrs.at[k, r], rrecv.at[k, r, pl.ds(0, len(near))])
        got = rrecv[k, r].reshape(ny * SLOTS, rwide)
        folded = jnp.concatenate([got[:, q * rstep : (q + 1) * rstep] for q in range(3)], axis=0)
        res = xin[k, :, cs].astype(F32) + jnp.concatenate(
            [
                jnp.dot(mix[k], got, preferred_element_type=F32),
                jnp.dot(mixs[k], folded, preferred_element_type=F32),
            ],
            axis=1,
        )
        obuf[k, :, cs] = res.astype(BF16)
        if k == 0:

            @pl.when(s < nsec - 1)
            def _():
                zcopy(r, s + 1).start()

    def zwait(r):
        with jax.named_scope(f"zw{r}"):

            @pl.when(s > 0)
            def _():
                zcopy(r, s - 1).wait_recv()

            if r == 0:

                @pl.when(s == 0)
                def _():
                    l_fresh.wait()

    def cot_arrive(n):
        arrived(crs.at[n - 1], crecv.at[ysrc(n)])

    select(0)
    l_arr.wait()
    with jax.named_scope("disp0"):
        dispatch(0)
    select(1)
    for k in range(2):
        for r in range(ndp):
            rrecv[k, r, lax.rem(y + far, ny)] = jnp.zeros((SLOTS, rwide), BF16)
    l_cot.wait()
    for k in range(2):
        for b in range(ndp):

            def put(cs, v, k=k, b=b):
                csend[:, k, b, :, cs] = v

            pick(selgb, k, cin[k, :, b * cols : (b + 1) * cols], put)
    with jax.named_scope("rel0"):
        relay(0)
    with jax.named_scope("spr0"):
        spread(0)
    for n in near:
        dest = lax.rem(y + n, ny)
        rc(csend.at[lax.div(dest, 2)], crecv.at[y], s_c, crs.at[n - 1], at_y(n)).start()
    crecv[y] = csend[lax.div(y, 2)]
    with jax.named_scope("fw0"):
        forward_w(0)
    with jax.named_scope("fw1"):
        forward_w(1)
    send_w(2, wd)
    with jax.named_scope("wspr0"):
        wait_spread(0)
    l_gn.wait()
    squares = [unpack(0, r) for r in range(ndp)]
    with jax.named_scope("cotm"):
        blk = crecv.at[mate_far]
        arrived(crs.at[relay_n - 1], blk)
        rc(blk, blk, s_c, crs.at[far - 1], mate_dev).start()
    l_w[0].wait()
    l_w[1].wait()
    with jax.named_scope("near01"):
        wait_near(0)
        wait_near(1)
    with jax.named_scope("far01"):
        wait_far(0)
        wait_far(1)
    with jax.named_scope("gu0"):
        h = gate_up(0, squares)
    l_w[2].wait()
    multiply(0, 0, h)
    with jax.named_scope("fw2"):
        forward_w(2)
    share_hidden(0)
    pack(0, 0)
    straight(0, 0)
    with jax.named_scope("cotw"):
        for n in near:
            if n in (far - 1, far + 1):

                @pl.when(relay_n != n)
                def _(n=n):
                    cot_arrive(n)
            else:
                cot_arrive(n)
        cot_arrive(far)
    share_cot()
    finish_far(0, 0)
    with jax.named_scope("near2"):
        wait_near(2)
    for r in (1, 2):
        multiply(0, r, h)
    for r in (1, 2):
        pack(0, r)
        straight(0, r)
    combine(0, 0)
    with jax.named_scope("far2"):
        wait_far(2)
    multiply(0, 3, h)
    pack(0, 3)
    straight(0, 3)
    for r in (1, 2, 3):
        finish_far(0, r)
    combine(0, 1)
    combine(0, 2)

    zwait(0)
    dispatch(1)
    combine(0, 3)
    out0 = pltpu.make_async_copy(obuf.at[0], out.at[0], lsem.at[6])
    out0.start()
    with jax.named_scope("fh0"):
        forward_hidden(0)
    for r in (1, 2):
        zwait(r)
        dispatch(r + 1)
    with jax.named_scope("rel1"):
        relay(1)
    with jax.named_scope("fc"):
        forward_cot()
    zwait(3)
    dispatch(4)
    with jax.named_scope("rel23"):
        relay(2)
        relay(3)
    with jax.named_scope("spr12"):
        spread(1)
        spread(2)
    with jax.named_scope("rel4"):
        relay(4)
    with jax.named_scope("spr3"):
        spread(3)
    squares = []
    for r in range(3):
        wait_spread(r + 1)
        squares.append(unpack(1, r))
    with jax.named_scope("spr4"):
        spread(4)
    with jax.named_scope("wspr4"):
        wait_spread(4)
    squares.append(unpack(1, 3))
    with jax.named_scope("gu1"):
        h = gate_up(1, squares)
    share_hidden(1)
    for r in range(ndp):
        multiply(1, r, h)
    for r in range(ndp):
        pack(1, r)
    for r in range(ndp):
        straight(1, r)
    finish_far(1, 0)
    with jax.named_scope("fh1"):
        forward_hidden(1)
    for r in range(1, ndp):
        finish_far(1, r)

    with jax.named_scope("sc"):
        spread_cot()
    with jax.named_scope("wsc"):
        arrived(cdr, cotx.at[1])
    for k in range(2):
        with jax.named_scope(f"wh{k}"):
            wait_hidden(k)
        with jax.named_scope(f"grad{k}"):
            for x in range(ndp):
                merged = merge(lambda rs, cs, x=x, k=k: cotx[:, x, :, k, rs, cs]).astype(BF16)
                main = cotx[:, x, :, k].reshape(count, rwide)
                cr = jnp.concatenate([main, merged], axis=1)
                add = jnp.dot(hid[k, x], cr, preferred_element_type=F32)
                if k == 0 and x == 0:
                    gacc[...] = add
                else:
                    gacc[...] += add
    gout = pltpu.make_async_copy(gacc, grad_out, lsem.at[7])
    gout.start()
    for r in range(ndp):
        combine(1, r)
    out1 = pltpu.make_async_copy(obuf.at[1], out.at[1], lsem.at[8])
    out1.start()
    with jax.named_scope("tail"):
        drain(s_w, wbuf.at[:, :, pl.ds(0, 3 * cols)])
        drain(s_t, trecv.at[0])
        drain(s_t, trecv.at[1, :, pl.ds(0, ny - 1)])
        drain(s_c, crecv.at[pl.ds(0, ny - 1)])
        drain(s_x, cotx.at[1])
        drain(s_x, cotx.at[0, pl.ds(0, 3)])
        drain(s_x, cstage)
        drain(s_h, hid.at[:, pl.ds(0, 3)])
        drain(s_d, drecv)
        drain(s_m, mrecv)
        drain(s_r, rrecv.at[:, :, pl.ds(0, len(near))])
    with jax.named_scope("zs"):

        @pl.when(s < nsec - 1)
        def _():
            drain(s_z, obuf.at[0])

    with jax.named_scope("outw"):
        out0.wait()
        gout.wait()
        out1.wait()


def local(nsec, nexp, ndp, arrivals, fresh, routes, gates, cotangent, norm_gain, w_gate, w_up, w_down):
    tok, width = arrivals.shape[1:]
    hidn, cols = w_gate.shape[1:]
    flight = nexp // SPLIT
    ny = nexp // 2
    steps = routes.shape[1]
    rows = nexp * SLOTS
    routes_t = jnp.transpose(routes[0], (2, 0, 1))
    gates_t = jnp.transpose(gates[0], (2, 0, 1))
    rwide = cols // 4 * 3
    any_spec = pl.BlockSpec(memory_space=pl.ANY)
    hbm_spec = pl.BlockSpec(memory_space=pltpu.HBM)
    dma = pltpu.SemaphoreType.DMA
    out, grad = pl.pallas_call(
        functools.partial(kernel_body, nsec, nexp, ndp),
        name="moe_relay",
        out_shape=(
            jax.ShapeDtypeStruct((steps, tok, width), BF16),
            jax.ShapeDtypeStruct((hidn, cols), F32),
        ),
        in_specs=[hbm_spec] * 9,
        out_specs=(any_spec, any_spec),
        scratch_shapes=[
            pltpu.VMEM((2, tok, width), BF16),
            pltpu.VMEM((2, tok, width), BF16),
            pltpu.VMEM((3, hidn, width), BF16),
            pltpu.VMEM((2, flight, ndp, SLOTS, rwide), BF16),
            pltpu.VMEM((2, 2, ny, ndp, SLOTS, rwide), BF16),
            pltpu.VMEM((rows, width), BF16),
            pltpu.VMEM((flight, 2, ndp, SLOTS, rwide), BF16),
            pltpu.VMEM((ny, 2, ndp, SLOTS, rwide), BF16),
            pltpu.VMEM((2, ny // 2, 2, SLOTS, rwide), BF16),
            pltpu.VMEM((2, ndp, ny, 2, SLOTS, rwide), BF16),
            pltpu.VMEM((2, ndp, hidn, rows), BF16),
            pltpu.VMEM((2, ndp, rows // 2, cols), BF16),
            pltpu.VMEM((2, ndp, rows // 2, cols), BF16),
            pltpu.VMEM((ndp, rows // 2, cols), F32),
            pltpu.VMEM((2, ndp, ny, SLOTS, rwide), BF16),
            pltpu.VMEM((2, ndp, SLOTS, rwide), BF16),
            pltpu.VMEM((2, ndp, ny, SLOTS, rwide), BF16),
            pltpu.VMEM(routes_t.shape, jnp.int32),
            pltpu.VMEM(gates_t.shape, BF16),
            pltpu.VMEM((1, width), F32),
            pltpu.VMEM((2, 3, flight * SLOTS, 2 * tok), BF16),
            pltpu.VMEM((2, 3, flight * SLOTS, 2 * tok), BF16),
            pltpu.VMEM((2, tok, ny * SLOTS), BF16),
            pltpu.VMEM((2, tok, 3 * ny * SLOTS), BF16),
            pltpu.VMEM((2, tok, width), BF16),
            pltpu.VMEM((hidn, cols), F32),
            dma((12,)), dma((9,)),
            dma((3, 2)), dma((3,)), dma((3,)),
            dma((1 + ndp, ny - 1)), dma((1 + ndp,)),
            dma((ny - 1,)), dma((2,)), dma((2,)), dma(()), dma(()),
            dma((2, 2)), dma((2,)), dma((2,)),
            dma((2, ndp)), dma((2, ndp)), dma((2, ndp)), dma((ndp,)),
        ],
        compiler_params=pltpu.CompilerParams(
            collective_id=0, has_side_effects=True, vmem_limit_bytes=24 * 1024 * 1024
        ),
    )(
        *(
            pltpu.with_memory_space_constraint(a, pltpu.HBM)
            for a in (
                arrivals[0], fresh[0], routes_t, gates_t, cotangent[0], norm_gain, w_gate[0], w_up[0], w_down[0]
            )
        )
    )
    return out[None], grad[None]


def solution(mesh):
    placed = (
        P("section", ("expert", "dp"), None),
        P(None, ("expert", "dp"), None),
        P("section", None, ("expert", "dp"), None),
        P("section", None, ("expert", "dp"), None),
        P("section", None, ("expert", "dp"), None),
        P("section", None),
        P("section", "expert", "dp"),
        P("section", "expert", "dp"),
        P("section", "expert", "dp"),
    )
    return jax.shard_map(
        functools.partial(local, mesh.shape["section"], mesh.shape["expert"], mesh.shape["dp"]),
        mesh=mesh,
        in_specs=placed,
        out_specs=(P("section", None, ("expert", "dp"), None), P("section", "expert", "dp")),
        check_vma=False,
    )
```

```python
import functools

import jax
import jax.numpy as jnp
from jax import lax
from jax.experimental import pallas as pl
from jax.experimental.pallas import tpu as pltpu
from jax.sharding import PartitionSpec as P

SPLIT = 4
CAP = 12
SLOTS = 16
NEAR = (3, 5, 2, 6, 1, 7)
ORDER = (0, 1, 3, 2)
MESH = pl.DeviceIdType.MESH
NT = (((1,), (1,)), ((), ()))
F32 = jnp.float32
BF16 = jnp.bfloat16


def kernel_body(
    nsec, nexp, ndp,
    arr, fresh, routes, gates, cot, gain, wg, wu, wd,
    out, grad_out,
    xin, cin, wbuf, tsend, trecv, xraw, acts, csend, crecv, cstage, cotx, hid, dsend, drecv, psum, rsend, mrecv, rrecv,
    rts, gts, gns, selb, selgb, mix, mixs, obuf, gacc,
    lsem, sends, wrs, wns, frs, trs, tdr, crs, cxr, cgr, cfr, cdr, hrs, hns, hfr, drs, mrs, rrs, zrs,
):
    s = lax.axis_index("section")
    i = lax.axis_index("expert")
    d = lax.axis_index("dp")
    ny = nexp // 2
    y = lax.div(i, 2)
    c = lax.rem(i, 2)
    tok, width = arr.shape
    hidn, cols = wg.shape
    half = hidn // 2
    rwide = rsend.shape[4]
    rstep = rwide // 3
    far = ny // 2
    near = [n for n in NEAR if 0 < n < ny and n != far]
    odd = lax.rem(y, 2)
    mate = y + 1 - 2 * odd
    mate_far = lax.rem(mate + far, ny)
    relay_n = far - 1 + 2 * odd
    mate_dev = (s, mate * 2 + c, d)
    flight = nexp // SPLIT
    rows = flight * SLOTS

    def at_x(k):
        return (s, i, lax.rem(d + k, ndp))

    def at_y(k):
        return (s, lax.rem(y + k, ny) * 2 + c, d)

    def ysrc(k):
        return lax.rem(y + ny - k, ny)

    partner = (s, y * 2 + 1 - c, d)

    def colsl(x):
        return pl.ds(pl.multiple_of(x * cols, cols), cols)

    def rc(src, dst, ss, rs, dev):
        return pltpu.make_async_remote_copy(
            src_ref=src, dst_ref=dst, send_sem=ss, recv_sem=rs, device_id=dev, device_id_type=MESH
        )

    s_w, s_t, s_c, s_x, s_h, s_d, s_m, s_r, s_z = (sends.at[n] for n in range(9))

    def drain(sem, ref):
        rc(ref, ref, sem, sem, partner).wait_send()

    def arrived(sem, ref):
        rc(ref, ref, sem, sem, partner).wait_recv()

    l_arr = pltpu.make_async_copy(arr, xin.at[0], lsem.at[0])
    l_cot = pltpu.make_async_copy(cot, cin, lsem.at[1])
    l_w = [
        pltpu.make_async_copy(w, wbuf.at[m, :, colsl(d)], lsem.at[2 + m])
        for m, w in enumerate((wg, wu, wd))
    ]
    l_fresh = pltpu.make_async_copy(fresh, xin.at[1], lsem.at[5])
    l_rt = pltpu.make_async_copy(routes, rts, lsem.at[9])
    l_gt = pltpu.make_async_copy(gates, gts, lsem.at[10])
    l_gn = pltpu.make_async_copy(gain, gns, lsem.at[11])
    for l in l_w:
        l.start()
    l_rt.start()
    l_gt.start()
    l_arr.start()
    l_gn.start()
    l_cot.start()

    @pl.when(s == 0)
    def _():
        l_fresh.start()

    bar = pltpu.get_barrier_semaphore()
    peers = [at_x(k) for k in range(1, ndp)] + [at_y(n) for n in range(1, ny)] + [partner]
    for p in peers:
        pl.semaphore_signal(bar, inc=1, device_id=p, device_id_type=MESH)

    @pl.when(s > 0)
    def _():
        pl.semaphore_signal(bar, inc=1, device_id=(s - 1, i, d), device_id_type=MESH)

    @pl.when(s < nsec - 1)
    def _():
        pl.semaphore_signal(bar, inc=1, device_id=(s + 1, i, d), device_id_type=MESH)

    with jax.named_scope("bar"):
        pl.semaphore_wait(
            bar,
            len(peers) + jnp.where(s > 0, 1, 0) + jnp.where(s < nsec - 1, 1, 0),
        )

    def part_of(w, j, own):
        return w.at[pl.ds(j * half, half), colsl(own)]

    def send_w(m):
        l_w[m].wait()
        for q in range(2):
            for j, k in enumerate((1, ndp - 1)):
                p = j if q == 0 else 1 - j
                rs = wrs.at[m, j] if q == 0 else wns.at[m]
                part = part_of(wbuf.at[m], p, d)
                rc(part, part, s_w, rs, at_x(k)).start()

    def forward_w(m):
        for j, k in enumerate((1, ndp - 1)):
            part = part_of(wbuf.at[m], j, lax.rem(d + ndp - k, ndp))
            arrived(wrs.at[m, j], part)
            rc(part, part, s_w, frs.at[m], at_x(k)).start()

    def wait_near(m):
        arrived(wns.at[m], wbuf.at[m, :, pl.ds(0, cols)])

    def wait_far(m):
        arrived(frs.at[m], wbuf.at[m, :, pl.ds(0, cols)])

    send_w(0)
    send_w(1)

    pos = lax.rem(lax.broadcasted_iota(jnp.int32, (rows, tok), 0), SLOTS)
    tail = SLOTS - CAP
    maps = [jnp.where(pos < CAP, pos, -5).astype(F32)]
    for q in range(3):
        maps.append(jnp.where(pos >= CAP, pos - CAP + tail * q, -5).astype(F32))
    ia = lax.broadcasted_iota(jnp.int32, (tok, tok), 0)
    ib = lax.broadcasted_iota(jnp.int32, (tok, tok), 1)
    before = (ia < ib).astype(F32).astype(BF16)
    eye = (ia == ib).astype(F32).astype(BF16)
    l_rt.wait()
    l_gt.wait()
    rt = rts[...]
    gt = gts[...].astype(F32)

    def select(k):
        r = rt[:, k, :]
        g = gt[:, k, :]
        names, shares = [], []
        for e in range(flight):
            m = r == e
            nm = jnp.max(jnp.where(m, 1.0, 0.0), axis=0, keepdims=True)
            sh = jnp.sum(jnp.where(m, g, 0.0), axis=0, keepdims=True)
            names.append(jnp.broadcast_to(nm, (SLOTS, tok)))
            shares.append(jnp.broadcast_to(sh, (SLOTS, tok)))
        naming = jnp.concatenate(names, axis=0)
        share = jnp.concatenate(shares, axis=0)
        places = jnp.dot(naming.astype(BF16), before, preferred_element_type=F32)
        picks, gated, mixes = [], [], []
        for slot in maps:
            chosen = (naming > 0.5) & (jnp.abs(places - slot) < 0.5)
            picks.append(jnp.where(chosen, 1.0, 0.0).astype(BF16))
            g3 = jnp.where(chosen, share, 0.0).astype(BF16)
            gated.append(g3)
            g3 = g3.reshape(flight, 1, SLOTS, tok)
            g3 = jnp.concatenate([g3, g3], axis=1).reshape(2 * rows, tok)
            mixes.append(lax.dot_general(eye, g3, NT, preferred_element_type=F32).astype(BF16))
        mix[k] = mixes[0]
        mixs[k] = jnp.concatenate(mixes[1:], axis=1)
        for q in range(3):
            selb[k, q] = jnp.concatenate([picks[0], picks[q + 1]], axis=1)
            selgb[k, q] = jnp.concatenate([gated[0], gated[q + 1]], axis=1)

    def view(ref, m, *at):
        return ref.at[(0,) + at] if m == 0 else ref.at[(1,) + at + (m - 1,)]

    def block(r):
        return colsl(lax.rem(d + ORDER[r], ndp))

    def pick(sel, k, x, put):
        last = x[:, rwide:]
        for q in range(3):
            both = jnp.concatenate([x[:, q * rstep : (q + 1) * rstep], last], axis=0)
            got = jnp.dot(sel[k, q], both, preferred_element_type=F32).astype(BF16)
            put(pl.ds(q * rstep, rstep), got.reshape(flight, SLOTS, rstep))

    def dispatch(m):
        k = 0 if m == 0 else 1
        for r in range(ndp) if m == 0 else (m - 1,):

            def put(cs, v, r=r):
                tsend[k, :, r, :, cs] = v

            pick(selb, k, xin[k, :, block(r)], put)
        for n in [far] * (m == ndp) + near:
            dest = lax.rem(y + n, ny)
            src = view(tsend, m, lax.div(dest, 2))
            rc(src, view(trecv, m, 0, y), s_t, trs.at[m, n - 1], at_y(n)).start()
        own = view(tsend, m, lax.div(y, 2))
        rc(own, view(trecv, m, 1, y), s_t, tdr.at[m], partner).start()
        if m == 0:
            trecv[0, 0, y] = tsend[0, lax.div(y, 2)]
        else:
            trecv[1, 0, y, m - 1] = tsend[1, lax.div(y, 2), m - 1]

    def onward(m, src, n):
        blk = view(trecv, m, 0, src)
        arrived(trs.at[m, n - 1], blk)
        rc(blk, view(trecv, m, 1, src), s_t, tdr.at[m], partner).start()

    def relay(m):
        onward(m, mate_far, relay_n)
        blk = view(trecv, m, 0, mate_far)
        rc(blk, blk, s_t, trs.at[m, far - 1], mate_dev).start()

    def spread(m):
        for n in near[::-1]:
            if n in (far - 1, far + 1) and m < ndp:

                @pl.when(relay_n != n)
                def _(n=n):
                    onward(m, ysrc(n), n)
            else:
                onward(m, ysrc(n), n)
    def spread_far(m):
        onward(m, ysrc(far), far)

    def wait_spread(m):
        arrived(tdr.at[m], trecv.at[0, 1] if m == 0 else trecv.at[1, 1, :, m - 1])

    count = nexp * SLOTS

    def turned(v):
        n, w = v.shape
        return pltpu.roll(v.reshape(n // 8, 8, w), 4, 1).reshape(n, w)

    low = lax.rem(lax.broadcasted_iota(jnp.int32, (count // 2, rstep), 0), 8) < 4

    def merge(get):
        tails = [
            get(pl.ds(8, 8), pl.ds(q * rstep, rstep)).astype(F32).reshape(count // 2, rstep) for q in range(3)
        ]
        first = jnp.where(low, turned(tails[0]), tails[1])
        second = turned(tails[2])
        return jnp.concatenate(
            [first.reshape(nexp, 1, 8, rstep), second.reshape(nexp, 1, 8, rstep)], axis=1
        ).reshape(count, rstep)

    def unpack(k, r):
        merged = merge(lambda rs, cs: trecv[k, :, :, r, rs, cs])
        mf = trecv[k, :, :, r, :, :].reshape(count, rwide).astype(F32)
        whole = jnp.concatenate([mf, merged], axis=1)
        xraw[r] = (whole * gns[:, block(r)]).astype(BF16)
        return sum(
            (mf[:, q * rstep : (q + 1) * rstep] * mf[:, q * rstep : (q + 1) * rstep] for q in range(3)),
            merged * merged,
        )

    def project(r):
        for m in range(2):
            part = lax.dot_general(wbuf[m, :, block(r)], xraw[r], NT, preferred_element_type=F32)
            if r == 0:
                acts[m] = part
            else:
                acts[m] += part

    def gate_up(k, squares):
        total = squares[0] + squares[1] + (squares[2] + squares[3])
        high = total.astype(BF16)
        parts = jnp.concatenate([high, (total - high.astype(F32)).astype(BF16)], axis=1)
        ones = jnp.ones((8, 2 * rstep), BF16)
        sums = lax.dot_general(ones, parts, NT, preferred_element_type=F32)[:1]
        scale = lax.rsqrt(sums * (1.0 / width) + 0.5)
        ga = acts[0] * scale
        ua = acts[1] * scale
        kept = lax.rem(lax.broadcasted_iota(jnp.int32, ga.shape, 1), SLOTS) < CAP
        h = jnp.where(kept, ga / (1.0 + jnp.exp(-ga)) * ua, 0.0)
        hid[k, d] = h.astype(BF16)
        return jnp.transpose(h).astype(BF16)

    def hid_half(k, x, p):
        return hid.at[k, x, pl.ds(p * half, half)]

    def share_hidden(k):
        for q in range(2):
            for j, n in enumerate((1, ndp - 1)):
                part = hid_half(k, d, j if q == 0 else 1 - j)
                rs = hrs.at[k, j] if q == 0 else hns.at[k]
                rc(part, part, s_h, rs, at_x(n)).start()

    def forward_hidden(k):
        for j, n in enumerate((1, ndp - 1)):
            part = hid_half(k, lax.rem(d + ndp - n, ndp), j)
            arrived(hrs.at[k, j], part)
            rc(part, part, s_h, hfr.at[k], at_x(n)).start()

    def wait_hidden(k):
        arrived(hns.at[k], hid.at[k, 0])
        arrived(hfr.at[k], hid.at[k, 0])

    hy = ny // 2

    def share_cot():
        across = lax.rem(d + 2, ndp)
        for j, n in enumerate((1, ndp - 1)):
            src = crecv.at[pl.ds(j * hy, hy), :, across]
            rc(src, cstage.at[j], s_x, cgr.at[j], at_x(n)).start()
        for j, n in enumerate((1, ndp - 1)):
            src = crecv.at[:, :, lax.rem(d + n, ndp)]
            rc(src, cotx.at[0, d], s_x, cxr.at[j], at_x(n)).start()
        cotx[0, d] = crecv[:, :, d]
        rc(cotx.at[0, d], cotx.at[1, d], s_x, cdr, partner).start()

    def forward_cot():
        for j, n in enumerate((1, ndp - 1)):
            arrived(cgr.at[j], cstage.at[j])
            dst = cotx.at[0, lax.rem(d + ndp - n, ndp), pl.ds(j * hy, hy)]
            rc(cstage.at[j], dst, s_x, cfr, at_x(n)).start()

    def spread_cot():
        for j, n in enumerate((1, ndp - 1)):
            x = lax.rem(d + ndp - n, ndp)
            arrived(cxr.at[j], cotx.at[0, x])
            rc(cotx.at[0, x], cotx.at[1, x], s_x, cdr, partner).start()
        x = lax.rem(d + 2, ndp)
        arrived(cfr, cotx.at[0, x])
        rc(cotx.at[0, x], cotx.at[1, x], s_x, cdr, partner).start()

    hrows = count // 2

    def direct(k, r, n, dest):
        return rc(rsend.at[k, r, dest], rrecv.at[k, r, y], s_r, rrs.at[k, r], at_y(n))

    def urgent(k, r):
        return k == 0 and r == ndp - 1

    def multiply(k, r, h):
        part = jnp.dot(h, wbuf[2, :, block(r)], preferred_element_type=F32)
        dsend[k, r] = part[hrows:].astype(BF16)
        rc(dsend.at[k, r], drecv.at[k, r], s_d, drs.at[k, r], partner).start()
        psum[r] = part[:hrows]

    def pack(k, r):
        with jax.named_scope(f"dw{k}{r}"):
            arrived(drs.at[k, r], drecv.at[k, r])
        total = psum[r] + drecv[k, r].astype(F32)
        t4 = total.reshape(ny, 2, 8, cols)
        lo, hi = t4[:, 0].reshape(ny * 8, cols), t4[:, 1].reshape(ny * 8, cols)
        lo3, hi3 = lo[:, rwide:], hi[:, rwide:]
        fill = jnp.concatenate([turned(lo3), lo3, turned(hi3)], axis=1)
        low = lax.rem(lax.broadcasted_iota(jnp.int32, (ny * 8, rwide), 0), 8) < 4
        hi = jnp.where(low, hi[:, :rwide], fill)
        packed = jnp.concatenate(
            [lo[:, :rwide].reshape(ny, 1, 8, rwide), hi.reshape(ny, 1, 8, rwide)], axis=1
        )
        rsend[k, r] = packed.reshape(ny, SLOTS, rwide).astype(BF16)
        if not urgent(k, r):
            rc(rsend.at[k, r, lax.rem(y + far, ny)], mrecv.at[k, r], s_m, mrs.at[k, r], mate_dev).start()

    def straight(k, r):
        for n in [far] * urgent(k, r) + near:
            if n in (far - 1, far + 1) and not urgent(k, r):

                @pl.when(2 * far - relay_n != n)
                def _(n=n):
                    direct(k, r, n, lax.rem(y + n, ny)).start()
            else:
                direct(k, r, n, lax.rem(y + n, ny)).start()
        rrecv[k, r, y] = rsend[k, r, y]

    def finish_far(k, r):
        with jax.named_scope(f"mw{k}{r}"):
            arrived(mrs.at[k, r], mrecv.at[k, r])
        both = rsend[k, r, mate_far].astype(F32) + mrecv[k, r].astype(F32)
        rsend[k, r, mate_far] = both.astype(BF16)
        dest = (s, mate_far * 2 + c, d)
        rc(rsend.at[k, r, mate_far], rrecv.at[k, r, y], s_r, rrs.at[k, r], dest).start()

    def zcopy(r, sec):
        cs = block(r)
        return rc(obuf.at[0, :, cs], xin.at[1, :, cs], s_z, zrs.at[r], (sec, i, d))

    def combine(k, r):
        cs = block(r)
        with jax.named_scope(f"rw{k}{r}"):
            arrived(rrs.at[k, r], rrecv.at[k, r, pl.ds(0, len(near) + urgent(k, r))])
        got = rrecv[k, r].reshape(ny * SLOTS, rwide)
        folded = jnp.concatenate([got[:, q * rstep : (q + 1) * rstep] for q in range(3)], axis=0)
        res = xin[k, :, cs].astype(F32) + jnp.concatenate(
            [
                jnp.dot(mix[k], got, preferred_element_type=F32),
                jnp.dot(mixs[k], folded, preferred_element_type=F32),
            ],
            axis=1,
        )
        obuf[k, :, cs] = res.astype(BF16)
        pltpu.make_async_copy(obuf.at[k, :, cs], out.at[k, :, cs], lsem.at[6 + k]).start()
        if k == 0:

            @pl.when(s < nsec - 1)
            def _():
                zcopy(r, s + 1).start()

    def zwait(r):
        with jax.named_scope(f"zw{r}"):

            @pl.when(s > 0)
            def _():
                zcopy(r, s - 1).wait_recv()

            if r == 0:

                @pl.when(s == 0)
                def _():
                    l_fresh.wait()

    def cot_arrive(n):
        arrived(crs.at[n - 1], crecv.at[ysrc(n)])

    select(0)
    l_arr.wait()
    with jax.named_scope("disp0"):
        dispatch(0)
    select(1)
    for k in range(2):
        for r in range(ndp):
            if not urgent(k, r):
                rrecv[k, r, lax.rem(y + far, ny)] = jnp.zeros((SLOTS, rwide), BF16)
    l_cot.wait()
    for k in range(2):
        for b in range(ndp):

            def put(cs, v, k=k, b=b):
                csend[:, k, b, :, cs] = v

            pick(selgb, k, cin[k, :, b * cols : (b + 1) * cols], put)
    with jax.named_scope("rel0"):
        relay(0)
    with jax.named_scope("spr0"):
        spread(0)
        spread_far(0)
    for n in near:
        dest = lax.rem(y + n, ny)
        rc(csend.at[lax.div(dest, 2)], crecv.at[y], s_c, crs.at[n - 1], at_y(n)).start()
    crecv[y] = csend[lax.div(y, 2)]
    with jax.named_scope("fw0"):
        forward_w(0)
    with jax.named_scope("fw1"):
        forward_w(1)
    send_w(2)
    with jax.named_scope("wspr0"):
        wait_spread(0)
    l_gn.wait()
    squares = [unpack(0, r) for r in range(ndp)]
    with jax.named_scope("cotm"):
        blk = crecv.at[mate_far]
        arrived(crs.at[relay_n - 1], blk)
        rc(blk, blk, s_c, crs.at[far - 1], mate_dev).start()
    with jax.named_scope("near01"):
        wait_near(0)
        wait_near(1)
    for r in range(ndp - 1):
        project(r)
    with jax.named_scope("far01"):
        wait_far(0)
        wait_far(1)
    project(ndp - 1)
    with jax.named_scope("gu0"):
        h = gate_up(0, squares)
    multiply(0, 0, h)
    with jax.named_scope("fw2"):
        forward_w(2)
    share_hidden(0)
    pack(0, 0)
    straight(0, 0)
    with jax.named_scope("cotw"):
        for n in near:
            if n in (far - 1, far + 1):

                @pl.when(relay_n != n)
                def _(n=n):
                    cot_arrive(n)
            else:
                cot_arrive(n)
        cot_arrive(far)
    share_cot()
    finish_far(0, 0)
    with jax.named_scope("near2"):
        wait_near(2)
    for r in (1, 2):
        multiply(0, r, h)
    for r in (1, 2):
        pack(0, r)
    for r in (1, 2):
        straight(0, r)
    combine(0, 0)
    finish_far(0, 1)
    finish_far(0, 2)
    with jax.named_scope("far2"):
        wait_far(2)
    multiply(0, 3, h)
    pack(0, 3)
    straight(0, 3)
    combine(0, 1)
    combine(0, 2)

    zwait(0)
    dispatch(1)
    combine(0, 3)
    with jax.named_scope("fh0"):
        forward_hidden(0)
    for r in (1, 2):
        zwait(r)
        dispatch(r + 1)
    with jax.named_scope("rel1"):
        relay(1)
    with jax.named_scope("fc"):
        forward_cot()
    zwait(3)
    dispatch(4)
    with jax.named_scope("rel23"):
        relay(2)
        relay(3)
    with jax.named_scope("spr123"):
        spread(1)
        spread(2)
        spread(3)
        spread_far(1)
        spread_far(2)
    squares = []
    for r in range(2):
        wait_spread(r + 1)
        squares.append(unpack(1, r))
        project(r)
    with jax.named_scope("spr4"):
        spread(4)
        spread_far(4)
    with jax.named_scope("spr3"):
        spread_far(3)
    with jax.named_scope("wspr3"):
        wait_spread(3)
    squares.append(unpack(1, 2))
    project(2)
    with jax.named_scope("wspr4"):
        wait_spread(4)
    squares.append(unpack(1, 3))
    project(3)
    with jax.named_scope("gu1"):
        h = gate_up(1, squares)
    share_hidden(1)
    multiply(1, 0, h)
    multiply(1, 1, h)
    pack(1, 0)
    straight(1, 0)
    multiply(1, 2, h)
    multiply(1, 3, h)
    for r in range(1, ndp):
        pack(1, r)
    for r in range(1, ndp):
        straight(1, r)
    finish_far(1, 0)
    with jax.named_scope("fh1"):
        forward_hidden(1)
    for r in range(1, ndp):
        finish_far(1, r)

    with jax.named_scope("sc"):
        spread_cot()
    with jax.named_scope("wsc"):
        arrived(cdr, cotx.at[1])
    for k in range(2):
        with jax.named_scope(f"wh{k}"):
            wait_hidden(k)
        with jax.named_scope(f"grad{k}"):
            for x in range(ndp):
                merged = merge(lambda rs, cs, x=x, k=k: cotx[:, x, :, k, rs, cs]).astype(BF16)
                main = cotx[:, x, :, k].reshape(count, rwide)
                cr = jnp.concatenate([main, merged], axis=1)
                add = jnp.dot(hid[k, x], cr, preferred_element_type=F32)
                if k == 0 and x == 0:
                    gacc[...] = add
                else:
                    gacc[...] += add
    gout = pltpu.make_async_copy(gacc, grad_out, lsem.at[8])
    gout.start()
    for r in range(ndp):
        combine(1, r)
    with jax.named_scope("tail"):
        drain(s_w, wbuf.at[:, :, pl.ds(0, 3 * cols)])
        drain(s_t, trecv.at[0])
        drain(s_t, trecv.at[1, :, pl.ds(0, ny - 1)])
        drain(s_c, crecv.at[pl.ds(0, ny - 1)])
        drain(s_x, cotx.at[1])
        drain(s_x, cotx.at[0, pl.ds(0, 3)])
        drain(s_x, cstage)
        drain(s_h, hid.at[:, pl.ds(0, 3)])
        drain(s_d, drecv)
        drain(s_m, mrecv.at[0, pl.ds(0, ndp - 1)])
        drain(s_m, mrecv.at[1])
        drain(s_r, rrecv.at[:, :, pl.ds(0, len(near))])
        drain(s_r, rrecv.at[0, 0, 0])
    with jax.named_scope("zs"):

        @pl.when(s < nsec - 1)
        def _():
            drain(s_z, obuf.at[0])

    with jax.named_scope("outw"):
        gout.wait()
        for k in range(2):
            pltpu.make_async_copy(obuf.at[k], out.at[k], lsem.at[6 + k]).wait()


def store_body(out, grad, out_hbm, grad_hbm, sem):
    a = pltpu.make_async_copy(out, out_hbm, sem.at[0])
    b = pltpu.make_async_copy(grad, grad_hbm, sem.at[1])
    a.start()
    b.start()
    a.wait()
    b.wait()


def local(nsec, nexp, ndp, arrivals, fresh, routes, gates, cotangent, norm_gain, w_gate, w_up, w_down):
    tok, width = arrivals.shape[1:]
    hidn, cols = w_gate.shape[1:]
    flight = nexp // SPLIT
    ny = nexp // 2
    steps = routes.shape[1]
    rows = nexp * SLOTS
    routes_t = jnp.transpose(routes[0], (2, 0, 1))
    gates_t = jnp.transpose(gates[0], (2, 0, 1))
    rwide = cols // 4 * 3
    any_spec = pl.BlockSpec(memory_space=pl.ANY)
    hbm_spec = pl.BlockSpec(memory_space=pltpu.HBM)
    dma = pltpu.SemaphoreType.DMA
    out, grad = pl.pallas_call(
        functools.partial(kernel_body, nsec, nexp, ndp),
        name="moe_relay",
        out_shape=(
            jax.ShapeDtypeStruct((steps, tok, width), BF16),
            jax.ShapeDtypeStruct((hidn, cols), F32),
        ),
        in_specs=[hbm_spec] * 9,
        out_specs=(any_spec, any_spec),
        scratch_shapes=[
            pltpu.VMEM((2, tok, width), BF16),
            pltpu.VMEM((2, tok, width), BF16),
            pltpu.VMEM((3, hidn, width), BF16),
            pltpu.VMEM((2, flight, ndp, SLOTS, rwide), BF16),
            pltpu.VMEM((2, 2, ny, ndp, SLOTS, rwide), BF16),
            pltpu.VMEM((ndp, rows, cols), BF16),
            pltpu.VMEM((2, hidn, rows), F32),
            pltpu.VMEM((flight, 2, ndp, SLOTS, rwide), BF16),
            pltpu.VMEM((ny, 2, ndp, SLOTS, rwide), BF16),
            pltpu.VMEM((2, ny // 2, 2, SLOTS, rwide), BF16),
            pltpu.VMEM((2, ndp, ny, 2, SLOTS, rwide), BF16),
            pltpu.VMEM((2, ndp, hidn, rows), BF16),
            pltpu.VMEM((2, ndp, rows // 2, cols), BF16),
            pltpu.VMEM((2, ndp, rows // 2, cols), BF16),
            pltpu.VMEM((ndp, rows // 2, cols), F32),
            pltpu.VMEM((2, ndp, ny, SLOTS, rwide), BF16),
            pltpu.VMEM((2, ndp, SLOTS, rwide), BF16),
            pltpu.VMEM((2, ndp, ny, SLOTS, rwide), BF16),
            pltpu.VMEM(routes_t.shape, jnp.int32),
            pltpu.VMEM(gates_t.shape, BF16),
            pltpu.VMEM((1, width), F32),
            pltpu.VMEM((2, 3, flight * SLOTS, 2 * tok), BF16),
            pltpu.VMEM((2, 3, flight * SLOTS, 2 * tok), BF16),
            pltpu.VMEM((2, tok, ny * SLOTS), BF16),
            pltpu.VMEM((2, tok, 3 * ny * SLOTS), BF16),
            pltpu.VMEM((2, tok, width), BF16),
            pltpu.VMEM((hidn, cols), F32),
            dma((12,)), dma((9,)),
            dma((3, 2)), dma((3,)), dma((3,)),
            dma((1 + ndp, ny - 1)), dma((1 + ndp,)),
            dma((ny - 1,)), dma((2,)), dma((2,)), dma(()), dma(()),
            dma((2, 2)), dma((2,)), dma((2,)),
            dma((2, ndp)), dma((2, ndp)), dma((2, ndp)), dma((ndp,)),
        ],
        compiler_params=pltpu.CompilerParams(
            collective_id=0, has_side_effects=True, vmem_limit_bytes=24 * 1024 * 1024
        ),
    )(
        *(
            pltpu.with_memory_space_constraint(a, pltpu.HBM)
            for a in (
                arrivals[0], fresh[0], routes_t, gates_t, cotangent[0], norm_gain, w_gate[0], w_up[0], w_down[0]
            )
        )
    )
    out, grad = pl.pallas_call(
        store_body,
        name="store",
        out_shape=(jax.ShapeDtypeStruct(out.shape, BF16), jax.ShapeDtypeStruct(grad.shape, F32)),
        in_specs=(any_spec, any_spec),
        out_specs=(any_spec, any_spec),
        scratch_shapes=[dma((2,))],
        compiler_params=pltpu.CompilerParams(vmem_limit_bytes=1024 * 1024),
    )(out, grad)
    return out[None], grad[None]


def solution(mesh):
    placed = (
        P("section", ("expert", "dp"), None),
        P(None, ("expert", "dp"), None),
        P("section", None, ("expert", "dp"), None),
        P("section", None, ("expert", "dp"), None),
        P("section", None, ("expert", "dp"), None),
        P("section", None),
        P("section", "expert", "dp"),
        P("section", "expert", "dp"),
        P("section", "expert", "dp"),
    )
    return jax.shard_map(
        functools.partial(local, mesh.shape["section"], mesh.shape["expert"], mesh.shape["dp"]),
        mesh=mesh,
        in_specs=placed,
        out_specs=(P("section", None, ("expert", "dp"), None), P("section", "expert", "dp")),
        check_vma=False,
    )
```

```python
import functools

import jax
import jax.numpy as jnp
from jax import lax
from jax.experimental import pallas as pl
from jax.experimental.pallas import tpu as pltpu
from jax.sharding import PartitionSpec as P

SPLIT = 4
CAP = 12
SLOTS = 16
DIRECT = 3
NEAR = (3, 5, 2, 6, 1, 7)
MESH = pl.DeviceIdType.MESH
NT = (((1,), (1,)), ((), ()))
F32 = jnp.float32
BF16 = jnp.bfloat16


def kernel_body(
    nsec, nexp, ndp,
    arr, fresh, routes, gates, cot, gain, wg, wu, wd,
    out, grad_out,
    xin, cin, wbuf, tsend, trecv, xraw, acts, csend, crecv, cstage, cotx, hid, dsend, drecv, psum, rsend, mrecv, rrecv,
    rts, gts, gns, selb, selgb, mix, mixs, obuf, gacc,
    lsem, sends, wrs, wns, frs, trs, tdr, crs, cxr, cgr, cfr, cdr, hrs, hns, hfr, drs, mrs, rrs, zrs,
):
    s = lax.axis_index("section")
    i = lax.axis_index("expert")
    d = lax.axis_index("dp")
    ny = nexp // 2
    y = lax.div(i, 2)
    c = lax.rem(i, 2)
    tok, width = arr.shape
    hidn, cols = wg.shape
    half = hidn // 2
    hc = cols // 2
    rwide = rsend.shape[4]
    rstep = rwide // 3
    far = ny // 2
    near = [n for n in NEAR if 0 < n < ny and n != far]
    odd = lax.rem(y, 2)
    mate = y + 1 - 2 * odd
    mate_far = lax.rem(mate + far, ny)
    relay_n = far - 1 + 2 * odd
    mate_dev = (s, mate * 2 + c, d)
    flight = nexp // SPLIT
    rows = flight * SLOTS

    def at_x(k):
        return (s, i, lax.rem(d + k, ndp))

    def at_y(k):
        return (s, lax.rem(y + k, ny) * 2 + c, d)

    def ysrc(k):
        return lax.rem(y + ny - k, ny)

    partner = (s, y * 2 + 1 - c, d)

    def colsl(x):
        return pl.ds(pl.multiple_of(x * cols, cols), cols)

    def rc(src, dst, ss, rs, dev):
        return pltpu.make_async_remote_copy(
            src_ref=src, dst_ref=dst, send_sem=ss, recv_sem=rs, device_id=dev, device_id_type=MESH
        )

    s_w, s_t, s_c, s_x, s_h, s_d, s_m, s_r, s_z = (sends.at[n] for n in range(9))

    def drain(sem, ref):
        rc(ref, ref, sem, sem, partner).wait_send()

    def arrived(sem, ref):
        rc(ref, ref, sem, sem, partner).wait_recv()

    near_dp, far_dp = (lax.rem(d + ndp - 1, ndp), lax.rem(d + 1, ndp)), lax.rem(d + 2, ndp)
    HALVES = (
        ((d, 0), (d, 1)),
        ((near_dp[0], 0), (near_dp[1], 1)),
        ((near_dp[0], 1), (near_dp[1], 0)),
        ((far_dp, 0), (far_dp, 1)),
    )

    def hs(owner, j):
        return pl.ds(pl.multiple_of(owner * cols + j * hc, hc), hc)

    def pieces(r):
        return [(hs(o, j), slice(q * hc, (q + 1) * hc)) for q, (o, j) in enumerate(HALVES[r])]

    def by_block(src, dst, sem, back=False):
        for r in range(ndp):
            for natural, local in pieces(r):
                a, b = src.at[:, natural], dst.at[r, :, local]
                pltpu.make_async_copy(a, b, sem).start()

    bar = pltpu.get_barrier_semaphore()
    peers = [at_x(k) for k in range(1, ndp)] + [at_y(n) for n in range(1, ny)] + [partner]
    for p in peers:
        pl.semaphore_signal(bar, inc=1, device_id=p, device_id_type=MESH)

    @pl.when(s > 0)
    def _():
        pl.semaphore_signal(bar, inc=1, device_id=(s - 1, i, d), device_id_type=MESH)

    @pl.when(s < nsec - 1)
    def _():
        pl.semaphore_signal(bar, inc=1, device_id=(s + 1, i, d), device_id_type=MESH)

    l_cot = pltpu.make_async_copy(cot, cin, lsem.at[1])
    l_w = [
        pltpu.make_async_copy(w, wbuf.at[m, :, colsl(d)], lsem.at[2 + m])
        for m, w in enumerate((wg, wu, wd))
    ]
    l_rt = pltpu.make_async_copy(routes, rts, lsem.at[9])
    l_gt = pltpu.make_async_copy(gates, gts, lsem.at[10])
    l_gn = pltpu.make_async_copy(gain, gns, lsem.at[11])
    for l in l_w:
        l.start()
    l_rt.start()
    l_gt.start()
    by_block(arr, xin.at[0], lsem.at[0])
    l_gn.start()
    l_cot.start()

    @pl.when(s == 0)
    def _():
        by_block(fresh, xin.at[1], lsem.at[5])

    with jax.named_scope("bar"):
        pl.semaphore_wait(
            bar,
            len(peers) + jnp.where(s > 0, 1, 0) + jnp.where(s < nsec - 1, 1, 0),
        )

    def part_of(m, j, owner):
        return wbuf.at[m, :, hs(owner, j)]

    def send_w(m):
        l_w[m].wait()
        for q in range(2):
            for j, k in enumerate((1, ndp - 1)):
                p = j if q == 0 else 1 - j
                rs = wrs.at[m, j] if q == 0 else wns.at[m]
                part = part_of(m, p, d)
                rc(part, part, s_w, rs, at_x(k)).start()

    def forward_w(m):
        for j, k in enumerate((1, ndp - 1)):
            part = part_of(m, j, lax.rem(d + ndp - k, ndp))
            arrived(wrs.at[m, j], part)
            rc(part, part, s_w, frs.at[m], at_x(k)).start()

    def wait_near(m):
        arrived(wns.at[m], wbuf.at[m, :, pl.ds(0, cols)])

    def wait_far(m):
        arrived(frs.at[m], wbuf.at[m, :, pl.ds(0, cols)])

    send_w(0)
    send_w(1)

    pos = lax.rem(lax.broadcasted_iota(jnp.int32, (rows, tok), 0), SLOTS)
    tail = SLOTS - CAP
    maps = [jnp.where(pos < CAP, pos, -5).astype(F32)]
    for q in range(3):
        maps.append(jnp.where(pos >= CAP, pos - CAP + tail * q, -5).astype(F32))
    ia = lax.broadcasted_iota(jnp.int32, (tok, tok), 0)
    ib = lax.broadcasted_iota(jnp.int32, (tok, tok), 1)
    before = (ia < ib).astype(F32).astype(BF16)
    eye = (ia == ib).astype(F32).astype(BF16)
    l_rt.wait()
    l_gt.wait()
    rt = rts[...]
    gt = gts[...].astype(F32)

    def select(k):
        r = rt[:, k, :]
        g = gt[:, k, :]
        names, shares = [], []
        for e in range(flight):
            m = r == e
            nm = jnp.max(jnp.where(m, 1.0, 0.0), axis=0, keepdims=True)
            sh = jnp.sum(jnp.where(m, g, 0.0), axis=0, keepdims=True)
            names.append(jnp.broadcast_to(nm, (SLOTS, tok)))
            shares.append(jnp.broadcast_to(sh, (SLOTS, tok)))
        naming = jnp.concatenate(names, axis=0)
        share = jnp.concatenate(shares, axis=0)
        places = jnp.dot(naming.astype(BF16), before, preferred_element_type=F32)
        picks, gated, mixes = [], [], []
        for slot in maps:
            chosen = (naming > 0.5) & (jnp.abs(places - slot) < 0.5)
            picks.append(jnp.where(chosen, 1.0, 0.0).astype(BF16))
            g3 = jnp.where(chosen, share, 0.0).astype(BF16)
            gated.append(g3)
            g3 = g3.reshape(flight, 1, SLOTS, tok)
            g3 = jnp.concatenate([g3, g3], axis=1).reshape(2 * rows, tok)
            mixes.append(lax.dot_general(eye, g3, NT, preferred_element_type=F32).astype(BF16))
        mix[k] = mixes[0]
        mixs[k] = jnp.concatenate(mixes[1:], axis=1)
        for q in range(3):
            selb[k, q] = jnp.concatenate([picks[0], picks[q + 1]], axis=1)
            selgb[k, q] = jnp.concatenate([gated[0], gated[q + 1]], axis=1)

    def view(ref, m, *at):
        return ref.at[(0,) + at] if m == 0 else ref.at[(1,) + at + (m - 1,)]

    def columns(ref, r, *at):
        return jnp.concatenate([ref[at + (natural,)] for natural, _ in pieces(r)], axis=-1)

    def pick(sel, k, x, put):
        last = x[:, rwide:]
        for q in range(3):
            both = jnp.concatenate([x[:, q * rstep : (q + 1) * rstep], last], axis=0)
            got = jnp.dot(sel[k, q], both, preferred_element_type=F32).astype(BF16)
            put(pl.ds(q * rstep, rstep), got.reshape(flight, SLOTS, rstep))

    def dispatch(m):
        k = 0 if m == 0 else 1
        for r in range(ndp) if m == 0 else (m - 1,):

            def put(cs, v, r=r):
                tsend[k, :, r, :, cs] = v

            pick(selb, k, xin[k, r], put)
        for n in [far] * (m >= DIRECT) + near:
            dest = lax.rem(y + n, ny)
            src = view(tsend, m, lax.div(dest, 2))
            rc(src, view(trecv, m, 0, y), s_t, trs.at[m, n - 1], at_y(n)).start()
        own = view(tsend, m, lax.div(y, 2))
        rc(own, view(trecv, m, 1, y), s_t, tdr.at[m], partner).start()
        if m == 0:
            trecv[0, 0, y] = tsend[0, lax.div(y, 2)]
        else:
            trecv[1, 0, y, m - 1] = tsend[1, lax.div(y, 2), m - 1]

    def onward(m, src, n):
        blk = view(trecv, m, 0, src)
        arrived(trs.at[m, n - 1], blk)
        rc(blk, view(trecv, m, 1, src), s_t, tdr.at[m], partner).start()

    def relay(m):
        onward(m, mate_far, relay_n)
        blk = view(trecv, m, 0, mate_far)
        rc(blk, blk, s_t, trs.at[m, far - 1], mate_dev).start()

    def spread(m):
        for n in near[::-1]:
            if n in (far - 1, far + 1) and m < DIRECT:

                @pl.when(relay_n != n)
                def _(n=n):
                    onward(m, ysrc(n), n)
            else:
                onward(m, ysrc(n), n)
    def spread_far(m):
        onward(m, ysrc(far), far)

    def wait_spread(m):
        arrived(tdr.at[m], trecv.at[0, 1] if m == 0 else trecv.at[1, 1, :, m - 1])

    count = nexp * SLOTS

    def turned(v):
        n, w = v.shape
        return pltpu.roll(v.reshape(n // 8, 8, w), 4, 1).reshape(n, w)

    low = lax.rem(lax.broadcasted_iota(jnp.int32, (count // 2, rstep), 0), 8) < 4

    def merge(get):
        tails = [
            get(pl.ds(8, 8), pl.ds(q * rstep, rstep)).astype(F32).reshape(count // 2, rstep) for q in range(3)
        ]
        first = jnp.where(low, turned(tails[0]), tails[1])
        second = turned(tails[2])
        return jnp.concatenate(
            [first.reshape(nexp, 1, 8, rstep), second.reshape(nexp, 1, 8, rstep)], axis=1
        ).reshape(count, rstep)

    def unpack(k, r):
        merged = merge(lambda rs, cs: trecv[k, :, :, r, rs, cs])
        mf = trecv[k, :, :, r, :, :].reshape(count, rwide).astype(F32)
        whole = jnp.concatenate([mf, merged], axis=1)
        xraw[r] = (whole * columns(gns, r, slice(None))).astype(BF16)
        return sum(
            (mf[:, q * rstep : (q + 1) * rstep] * mf[:, q * rstep : (q + 1) * rstep] for q in range(3)),
            merged * merged,
        )

    def project(r):
        for m in range(2):
            part = lax.dot_general(columns(wbuf, r, m, slice(None)), xraw[r], NT, preferred_element_type=F32)
            if r == 0:
                acts[m] = part
            else:
                acts[m] += part

    def gate_up(k, squares):
        total = squares[0] + squares[1] + (squares[2] + squares[3])
        high = total.astype(BF16)
        parts = jnp.concatenate([high, (total - high.astype(F32)).astype(BF16)], axis=1)
        ones = jnp.ones((8, 2 * rstep), BF16)
        sums = lax.dot_general(ones, parts, NT, preferred_element_type=F32)[:1]
        scale = lax.rsqrt(sums * (1.0 / width) + 0.5)
        ga = acts[0] * scale
        ua = acts[1] * scale
        kept = lax.rem(lax.broadcasted_iota(jnp.int32, ga.shape, 1), SLOTS) < CAP
        h = jnp.where(kept, ga / (1.0 + jnp.exp(-ga)) * ua, 0.0)
        hid[k, d] = h.astype(BF16)
        return jnp.transpose(h).astype(BF16)

    def hid_half(k, x, p):
        return hid.at[k, x, pl.ds(p * half, half)]

    def share_hidden(k):
        for q in range(2):
            for j, n in enumerate((1, ndp - 1)):
                part = hid_half(k, d, j if q == 0 else 1 - j)
                rs = hrs.at[k, j] if q == 0 else hns.at[k]
                rc(part, part, s_h, rs, at_x(n)).start()

    def forward_hidden(k):
        for j, n in enumerate((1, ndp - 1)):
            part = hid_half(k, lax.rem(d + ndp - n, ndp), j)
            arrived(hrs.at[k, j], part)
            rc(part, part, s_h, hfr.at[k], at_x(n)).start()

    def wait_hidden(k):
        arrived(hns.at[k], hid.at[k, 0])
        arrived(hfr.at[k], hid.at[k, 0])

    hy = ny // 2

    def share_cot():
        across = lax.rem(d + 2, ndp)
        for j, n in enumerate((1, ndp - 1)):
            src = crecv.at[pl.ds(j * hy, hy), :, across]
            rc(src, cstage.at[j], s_x, cgr.at[j], at_x(n)).start()
        for j, n in enumerate((1, ndp - 1)):
            src = crecv.at[:, :, lax.rem(d + n, ndp)]
            rc(src, cotx.at[0, d], s_x, cxr.at[j], at_x(n)).start()
        cotx[0, d] = crecv[:, :, d]
        rc(cotx.at[0, d], cotx.at[1, d], s_x, cdr, partner).start()

    def forward_cot():
        for j, n in enumerate((1, ndp - 1)):
            arrived(cgr.at[j], cstage.at[j])
            dst = cotx.at[0, lax.rem(d + ndp - n, ndp), pl.ds(j * hy, hy)]
            rc(cstage.at[j], dst, s_x, cfr, at_x(n)).start()

    def spread_cot():
        for j, n in enumerate((1, ndp - 1)):
            x = lax.rem(d + ndp - n, ndp)
            arrived(cxr.at[j], cotx.at[0, x])
            rc(cotx.at[0, x], cotx.at[1, x], s_x, cdr, partner).start()
        x = lax.rem(d + 2, ndp)
        arrived(cfr, cotx.at[0, x])
        rc(cotx.at[0, x], cotx.at[1, x], s_x, cdr, partner).start()

    hrows = count // 2

    def direct(k, r, n, dest):
        return rc(rsend.at[k, r, dest], rrecv.at[k, r, y], s_r, rrs.at[k, r], at_y(n))

    def urgent(k, r):
        return k == 0

    def multiply(k, r, h):
        part = jnp.dot(h, columns(wbuf, r, 2, slice(None)), preferred_element_type=F32)
        dsend[k, r] = part[hrows:].astype(BF16)
        rc(dsend.at[k, r], drecv.at[k, r], s_d, drs.at[k, r], partner).start()
        psum[r] = part[:hrows]

    def pack(k, r):
        with jax.named_scope(f"dw{k}{r}"):
            arrived(drs.at[k, r], drecv.at[k, r])
        total = psum[r] + drecv[k, r].astype(F32)
        t4 = total.reshape(ny, 2, 8, cols)
        lo, hi = t4[:, 0].reshape(ny * 8, cols), t4[:, 1].reshape(ny * 8, cols)
        lo3, hi3 = lo[:, rwide:], hi[:, rwide:]
        fill = jnp.concatenate([turned(lo3), lo3, turned(hi3)], axis=1)
        low = lax.rem(lax.broadcasted_iota(jnp.int32, (ny * 8, rwide), 0), 8) < 4
        hi = jnp.where(low, hi[:, :rwide], fill)
        packed = jnp.concatenate(
            [lo[:, :rwide].reshape(ny, 1, 8, rwide), hi.reshape(ny, 1, 8, rwide)], axis=1
        )
        rsend[k, r] = packed.reshape(ny, SLOTS, rwide).astype(BF16)
        if not urgent(k, r):
            rc(rsend.at[k, r, lax.rem(y + far, ny)], mrecv.at[r], s_m, mrs.at[r], mate_dev).start()

    def straight(k, r):
        for n in [far] * urgent(k, r) + near:
            if n in (far - 1, far + 1) and not urgent(k, r):

                @pl.when(2 * far - relay_n != n)
                def _(n=n):
                    direct(k, r, n, lax.rem(y + n, ny)).start()
            else:
                direct(k, r, n, lax.rem(y + n, ny)).start()
        rrecv[k, r, y] = rsend[k, r, y]

    def finish_far(k, r):
        with jax.named_scope(f"mw{k}{r}"):
            arrived(mrs.at[r], mrecv.at[r])
        both = rsend[k, r, mate_far].astype(F32) + mrecv[r].astype(F32)
        rsend[k, r, mate_far] = both.astype(BF16)
        dest = (s, mate_far * 2 + c, d)
        rc(rsend.at[k, r, mate_far], rrecv.at[k, r, y], s_r, rrs.at[k, r], dest).start()

    def zcopy(r, sec):
        return rc(obuf.at[0, r], xin.at[1, r], s_z, zrs.at[r], (sec, i, d))

    def combine(k, r):
        with jax.named_scope(f"rw{k}{r}"):
            arrived(rrs.at[k, r], rrecv.at[k, r, pl.ds(0, len(near) + urgent(k, r))])
        got = rrecv[k, r].reshape(ny * SLOTS, rwide)
        folded = jnp.concatenate([got[:, q * rstep : (q + 1) * rstep] for q in range(3)], axis=0)
        res = xin[k, r].astype(F32) + jnp.concatenate(
            [
                jnp.dot(mix[k], got, preferred_element_type=F32),
                jnp.dot(mixs[k], folded, preferred_element_type=F32),
            ],
            axis=1,
        )
        obuf[k, r] = res.astype(BF16)
        for natural, local in pieces(r):
            pltpu.make_async_copy(obuf.at[k, r, :, local], out.at[k, :, natural], lsem.at[6 + k]).start()
        if k == 0:

            @pl.when(s < nsec - 1)
            def _():
                zcopy(r, s + 1).start()

    def zwait(r):
        with jax.named_scope(f"zw{r}"):

            @pl.when(s > 0)
            def _():
                zcopy(r, s - 1).wait_recv()

            if r == 0:

                @pl.when(s == 0)
                def _():
                    pltpu.make_async_copy(xin.at[1], xin.at[1], lsem.at[5]).wait()

    def cot_arrive(n):
        arrived(crs.at[n - 1], crecv.at[ysrc(n)])

    select(0)
    pltpu.make_async_copy(xin.at[0], xin.at[0], lsem.at[0]).wait()
    with jax.named_scope("disp0"):
        dispatch(0)
    select(1)
    for k in range(2):
        for r in range(ndp):
            if not urgent(k, r):
                rrecv[k, r, lax.rem(y + far, ny)] = jnp.zeros((SLOTS, rwide), BF16)
    l_cot.wait()
    for k in range(2):
        for b in range(ndp):

            def put(cs, v, k=k, b=b):
                csend[:, k, b, :, cs] = v

            pick(selgb, k, cin[k, :, b * cols : (b + 1) * cols], put)
    with jax.named_scope("rel0"):
        relay(0)
    with jax.named_scope("spr0"):
        spread(0)
        spread_far(0)
    for n in near:
        dest = lax.rem(y + n, ny)
        rc(csend.at[lax.div(dest, 2)], crecv.at[y], s_c, crs.at[n - 1], at_y(n)).start()
    crecv[y] = csend[lax.div(y, 2)]
    with jax.named_scope("fw0"):
        forward_w(0)
    with jax.named_scope("fw1"):
        forward_w(1)
    send_w(2)
    with jax.named_scope("wspr0"):
        wait_spread(0)
    l_gn.wait()
    squares = [unpack(0, r) for r in range(ndp)]
    with jax.named_scope("cotm"):
        blk = crecv.at[mate_far]
        arrived(crs.at[relay_n - 1], blk)
        rc(blk, blk, s_c, crs.at[far - 1], mate_dev).start()
    with jax.named_scope("near01"):
        wait_near(0)
        wait_near(1)
    for r in range(ndp - 1):
        project(r)
    with jax.named_scope("far01"):
        wait_far(0)
        wait_far(1)
    project(ndp - 1)
    with jax.named_scope("gu0"):
        h = gate_up(0, squares)
    multiply(0, 0, h)
    pack(0, 0)
    straight(0, 0)
    with jax.named_scope("fw2"):
        forward_w(2)
    multiply(0, 1, h)
    share_hidden(0)
    with jax.named_scope("cotw"):
        for n in near:
            if n in (far - 1, far + 1):

                @pl.when(relay_n != n)
                def _(n=n):
                    cot_arrive(n)
            else:
                cot_arrive(n)
        cot_arrive(far)
    share_cot()
    pack(0, 1)
    straight(0, 1)
    combine(0, 0)
    with jax.named_scope("near2"):
        wait_near(2)
    multiply(0, 2, h)
    pack(0, 2)
    straight(0, 2)
    combine(0, 1)
    zwait(0)
    dispatch(1)
    with jax.named_scope("far2"):
        wait_far(2)
    multiply(0, 3, h)
    pack(0, 3)
    straight(0, 3)
    combine(0, 2)
    zwait(1)
    dispatch(2)

    with jax.named_scope("rel1"):
        relay(1)
    combine(0, 3)
    with jax.named_scope("fh0"):
        forward_hidden(0)
    with jax.named_scope("fc"):
        forward_cot()
    zwait(2)
    dispatch(3)
    with jax.named_scope("spr1"):
        spread(1)
        spread_far(1)
    with jax.named_scope("rel2"):
        relay(2)
    zwait(3)
    dispatch(4)
    with jax.named_scope("spr2"):
        spread(2)
    with jax.named_scope("sprf2"):
        spread_far(2)
    with jax.named_scope("spr3"):
        spread(3)
    squares = []
    for r in range(2):
        wait_spread(r + 1)
        squares.append(unpack(1, r))
        project(r)
    with jax.named_scope("sprf3"):
        spread_far(3)
    with jax.named_scope("spr4"):
        spread(4)
    with jax.named_scope("sprf4"):
        spread_far(4)
    with jax.named_scope("wspr3"):
        wait_spread(3)
    squares.append(unpack(1, 2))
    project(2)
    with jax.named_scope("wspr4"):
        wait_spread(4)
    squares.append(unpack(1, 3))
    project(3)
    with jax.named_scope("gu1"):
        h = gate_up(1, squares)
    share_hidden(1)
    multiply(1, 0, h)
    multiply(1, 1, h)
    pack(1, 0)
    straight(1, 0)
    multiply(1, 2, h)
    multiply(1, 3, h)
    for r in range(1, ndp):
        pack(1, r)
    for r in range(1, ndp):
        straight(1, r)
    with jax.named_scope("sc"):
        spread_cot()
    finish_far(1, 0)
    with jax.named_scope("fh1"):
        forward_hidden(1)
    for r in range(1, ndp):
        finish_far(1, r)
    with jax.named_scope("wsc"):
        arrived(cdr, cotx.at[1])

    def grad(k):
        with jax.named_scope(f"wh{k}"):
            wait_hidden(k)
        with jax.named_scope(f"grad{k}"):
            for x in range(ndp):
                merged = merge(lambda rs, cs, x=x, k=k: cotx[:, x, :, k, rs, cs]).astype(BF16)
                main = cotx[:, x, :, k].reshape(count, rwide)
                cr = jnp.concatenate([main, merged], axis=1)
                add = jnp.dot(hid[k, x], cr, preferred_element_type=F32)
                if k == 0 and x == 0:
                    gacc[...] = add
                else:
                    gacc[...] += add

    grad(0)
    combine(1, 0)
    combine(1, 1)
    grad(1)
    gout = pltpu.make_async_copy(gacc, grad_out, lsem.at[8])
    gout.start()
    combine(1, 2)
    combine(1, 3)
    with jax.named_scope("tail"):
        drain(s_w, wbuf.at[:, :, pl.ds(0, 3 * cols)])
        drain(s_t, trecv.at[0])
        drain(s_t, trecv.at[1, :, pl.ds(0, ny - 1)])
        drain(s_c, crecv.at[pl.ds(0, ny - 1)])
        drain(s_x, cotx.at[1])
        drain(s_x, cotx.at[0, pl.ds(0, 3)])
        drain(s_x, cstage)
        drain(s_h, hid.at[:, pl.ds(0, 3)])
        drain(s_d, drecv)
        drain(s_m, mrecv)
        drain(s_r, rrecv.at[0, :, pl.ds(0, len(near) + 1)])
        drain(s_r, rrecv.at[1, :, pl.ds(0, len(near))])
    with jax.named_scope("zs"):

        @pl.when(s < nsec - 1)
        def _():
            drain(s_z, obuf.at[0])

    with jax.named_scope("outw"):
        gout.wait()
        for k in range(2):
            pltpu.make_async_copy(obuf.at[k], obuf.at[k], lsem.at[6 + k]).wait()


def store_body(out, grad, out_hbm, grad_hbm, sem):
    a = pltpu.make_async_copy(out, out_hbm, sem.at[0])
    b = pltpu.make_async_copy(grad, grad_hbm, sem.at[1])
    a.start()
    b.start()
    a.wait()
    b.wait()


def local(nsec, nexp, ndp, arrivals, fresh, routes, gates, cotangent, norm_gain, w_gate, w_up, w_down):
    tok, width = arrivals.shape[1:]
    hidn, cols = w_gate.shape[1:]
    flight = nexp // SPLIT
    ny = nexp // 2
    steps = routes.shape[1]
    rows = nexp * SLOTS
    routes_t = jnp.transpose(routes[0], (2, 0, 1))
    gates_t = jnp.transpose(gates[0], (2, 0, 1))
    rwide = cols // 4 * 3
    any_spec = pl.BlockSpec(memory_space=pl.ANY)
    hbm_spec = pl.BlockSpec(memory_space=pltpu.HBM)
    dma = pltpu.SemaphoreType.DMA
    out, grad = pl.pallas_call(
        functools.partial(kernel_body, nsec, nexp, ndp),
        name="moe_relay",
        out_shape=(
            jax.ShapeDtypeStruct((steps, tok, width), BF16),
            jax.ShapeDtypeStruct((hidn, cols), F32),
        ),
        in_specs=[hbm_spec] * 9,
        out_specs=(any_spec, any_spec),
        scratch_shapes=[
            pltpu.VMEM((2, ndp, tok, cols), BF16),
            pltpu.VMEM((2, tok, width), BF16),
            pltpu.VMEM((3, hidn, width), BF16),
            pltpu.VMEM((2, flight, ndp, SLOTS, rwide), BF16),
            pltpu.VMEM((2, 2, ny, ndp, SLOTS, rwide), BF16),
            pltpu.VMEM((ndp, rows, cols), BF16),
            pltpu.VMEM((2, hidn, rows), F32),
            pltpu.VMEM((flight, 2, ndp, SLOTS, rwide), BF16),
            pltpu.VMEM((ny, 2, ndp, SLOTS, rwide), BF16),
            pltpu.VMEM((2, ny // 2, 2, SLOTS, rwide), BF16),
            pltpu.VMEM((2, ndp, ny, 2, SLOTS, rwide), BF16),
            pltpu.VMEM((2, ndp, hidn, rows), BF16),
            pltpu.VMEM((2, ndp, rows // 2, cols), BF16),
            pltpu.VMEM((2, ndp, rows // 2, cols), BF16),
            pltpu.VMEM((ndp, rows // 2, cols), F32),
            pltpu.VMEM((2, ndp, ny, SLOTS, rwide), BF16),
            pltpu.VMEM((ndp, SLOTS, rwide), BF16),
            pltpu.VMEM((2, ndp, ny, SLOTS, rwide), BF16),
            pltpu.VMEM(routes_t.shape, jnp.int32),
            pltpu.VMEM(gates_t.shape, BF16),
            pltpu.VMEM((1, width), F32),
            pltpu.VMEM((2, 3, flight * SLOTS, 2 * tok), BF16),
            pltpu.VMEM((2, 3, flight * SLOTS, 2 * tok), BF16),
            pltpu.VMEM((2, tok, ny * SLOTS), BF16),
            pltpu.VMEM((2, tok, 3 * ny * SLOTS), BF16),
            pltpu.VMEM((2, ndp, tok, cols), BF16),
            pltpu.VMEM((hidn, cols), F32),
            dma((12,)), dma((9,)),
            dma((3, 2)), dma((3,)), dma((3,)),
            dma((1 + ndp, ny - 1)), dma((1 + ndp,)),
            dma((ny - 1,)), dma((2,)), dma((2,)), dma(()), dma(()),
            dma((2, 2)), dma((2,)), dma((2,)),
            dma((2, ndp)), dma((ndp,)), dma((2, ndp)), dma((ndp,)),
        ],
        compiler_params=pltpu.CompilerParams(
            collective_id=0, has_side_effects=True, vmem_limit_bytes=24 * 1024 * 1024
        ),
    )(
        *(
            pltpu.with_memory_space_constraint(a, pltpu.HBM)
            for a in (
                arrivals[0], fresh[0], routes_t, gates_t, cotangent[0], norm_gain, w_gate[0], w_up[0], w_down[0]
            )
        )
    )
    out, grad = pl.pallas_call(
        store_body,
        name="store",
        out_shape=(jax.ShapeDtypeStruct(out.shape, BF16), jax.ShapeDtypeStruct(grad.shape, F32)),
        in_specs=(any_spec, any_spec),
        out_specs=(any_spec, any_spec),
        scratch_shapes=[dma((2,))],
        compiler_params=pltpu.CompilerParams(vmem_limit_bytes=1024 * 1024),
    )(out, grad)
    return out[None], grad[None]


def solution(mesh):
    placed = (
        P("section", ("expert", "dp"), None),
        P(None, ("expert", "dp"), None),
        P("section", None, ("expert", "dp"), None),
        P("section", None, ("expert", "dp"), None),
        P("section", None, ("expert", "dp"), None),
        P("section", None),
        P("section", "expert", "dp"),
        P("section", "expert", "dp"),
        P("section", "expert", "dp"),
    )
    return jax.shard_map(
        functools.partial(local, mesh.shape["section"], mesh.shape["expert"], mesh.shape["dp"]),
        mesh=mesh,
        in_specs=placed,
        out_specs=(P("section", None, ("expert", "dp"), None), P("section", "expert", "dp")),
        check_vma=False,
    )
```

```python
import functools

import jax
import jax.numpy as jnp
from jax import lax
from jax.experimental import pallas as pl
from jax.experimental.pallas import tpu as pltpu
from jax.sharding import PartitionSpec as P

SPLIT = 4
CAP = 12
SLOTS = 16
DIRECT = 2
NEAR = (3, 5, 2, 6, 1, 7)
MESH = pl.DeviceIdType.MESH
NT = (((1,), (1,)), ((), ()))
F32 = jnp.float32
BF16 = jnp.bfloat16


def kernel_body(
    nsec, nexp, ndp,
    arr, fresh, routes, gates, cot, gain, wg, wu, wd,
    out, grad_out,
    xin, cin, wbuf, tsend, trecv, xraw, acts, csend, crecv, cstage, cotx, hid, dsend, drecv, psum, rsend, mrecv, rrecv,
    rts, gts, gns, selb, selgb, mix, mixs, obuf, gacc,
    lsem, sends, wrs, wns, frs, trs, tdr, crs, cxr, cgr, cfr, cdr, hrs, hns, hfr, drs, mrs, rrs, zrs,
):
    s = lax.axis_index("section")
    i = lax.axis_index("expert")
    d = lax.axis_index("dp")
    ny = nexp // 2
    y = lax.div(i, 2)
    c = lax.rem(i, 2)
    tok, width = arr.shape
    hidn, cols = wg.shape
    half = hidn // 2
    hc = cols // 2
    rwide = rsend.shape[4]
    rstep = rwide // 3
    far = ny // 2
    near = [n for n in NEAR if 0 < n < ny and n != far]
    odd = lax.rem(y, 2)
    mate = y + 1 - 2 * odd
    mate_far = lax.rem(mate + far, ny)
    relay_n = far - 1 + 2 * odd
    mate_dev = (s, mate * 2 + c, d)
    flight = nexp // SPLIT
    rows = flight * SLOTS

    def at_x(k):
        return (s, i, lax.rem(d + k, ndp))

    def at_y(k):
        return (s, lax.rem(y + k, ny) * 2 + c, d)

    def ysrc(k):
        return lax.rem(y + ny - k, ny)

    partner = (s, y * 2 + 1 - c, d)

    def colsl(x):
        return pl.ds(pl.multiple_of(x * cols, cols), cols)

    def rc(src, dst, ss, rs, dev):
        return pltpu.make_async_remote_copy(
            src_ref=src, dst_ref=dst, send_sem=ss, recv_sem=rs, device_id=dev, device_id_type=MESH
        )

    s_w, s_t, s_c, s_x, s_h, s_d, s_m, s_r, s_z = (sends.at[n] for n in range(9))

    def drain(sem, ref):
        rc(ref, ref, sem, sem, partner).wait_send()

    def arrived(sem, ref):
        rc(ref, ref, sem, sem, partner).wait_recv()

    near_dp, far_dp = (lax.rem(d + ndp - 1, ndp), lax.rem(d + 1, ndp)), lax.rem(d + 2, ndp)
    HALVES = (
        ((d, 0), (d, 1)),
        ((near_dp[0], 0), (near_dp[1], 1)),
        ((near_dp[0], 1), (near_dp[1], 0)),
        ((far_dp, 0), (far_dp, 1)),
    )

    def hs(owner, j):
        return pl.ds(pl.multiple_of(owner * cols + j * hc, hc), hc)

    def pieces(r):
        return [(hs(o, j), slice(q * hc, (q + 1) * hc)) for q, (o, j) in enumerate(HALVES[r])]

    def by_block(src, dst, sem, back=False):
        for r in range(ndp):
            for natural, local in pieces(r):
                a, b = src.at[:, natural], dst.at[r, :, local]
                pltpu.make_async_copy(a, b, sem).start()

    bar = pltpu.get_barrier_semaphore()
    peers = [at_x(k) for k in range(1, ndp)] + [at_y(n) for n in range(1, ny)] + [partner]
    for p in peers:
        pl.semaphore_signal(bar, inc=1, device_id=p, device_id_type=MESH)

    @pl.when(s > 0)
    def _():
        pl.semaphore_signal(bar, inc=1, device_id=(s - 1, i, d), device_id_type=MESH)

    @pl.when(s < nsec - 1)
    def _():
        pl.semaphore_signal(bar, inc=1, device_id=(s + 1, i, d), device_id_type=MESH)

    l_cot = pltpu.make_async_copy(cot, cin, lsem.at[1])
    l_w = [
        pltpu.make_async_copy(w, wbuf.at[m, :, colsl(d)], lsem.at[2 + m])
        for m, w in enumerate((wg, wu, wd))
    ]
    l_rt = pltpu.make_async_copy(routes, rts, lsem.at[9])
    l_gt = pltpu.make_async_copy(gates, gts, lsem.at[10])
    l_gn = pltpu.make_async_copy(gain, gns, lsem.at[11])
    for l in l_w:
        l.start()
    l_rt.start()
    l_gt.start()
    by_block(arr, xin.at[0], lsem.at[0])
    l_gn.start()
    l_cot.start()

    @pl.when(s == 0)
    def _():
        by_block(fresh, xin.at[1], lsem.at[5])

    with jax.named_scope("bar"):
        pl.semaphore_wait(
            bar,
            len(peers) + jnp.where(s > 0, 1, 0) + jnp.where(s < nsec - 1, 1, 0),
        )

    def part_of(m, j, owner):
        return wbuf.at[m, :, hs(owner, j)]

    def send_w(m):
        l_w[m].wait()
        for q in range(2):
            for j, k in enumerate((1, ndp - 1)):
                p = j if q == 0 else 1 - j
                rs = wrs.at[m, j] if q == 0 else wns.at[m]
                part = part_of(m, p, d)
                rc(part, part, s_w, rs, at_x(k)).start()

    def forward_w(m):
        for j, k in enumerate((1, ndp - 1)):
            part = part_of(m, j, lax.rem(d + ndp - k, ndp))
            arrived(wrs.at[m, j], part)
            rc(part, part, s_w, frs.at[m], at_x(k)).start()

    def wait_near(m):
        arrived(wns.at[m], wbuf.at[m, :, pl.ds(0, cols)])

    def wait_far(m):
        arrived(frs.at[m], wbuf.at[m, :, pl.ds(0, cols)])

    send_w(0)
    send_w(1)

    pos = lax.rem(lax.broadcasted_iota(jnp.int32, (rows, tok), 0), SLOTS)
    tail = SLOTS - CAP
    maps = [jnp.where(pos < CAP, pos, -5).astype(F32)]
    for q in range(3):
        maps.append(jnp.where(pos >= CAP, pos - CAP + tail * q, -5).astype(F32))
    ia = lax.broadcasted_iota(jnp.int32, (tok, tok), 0)
    ib = lax.broadcasted_iota(jnp.int32, (tok, tok), 1)
    before = (ia < ib).astype(F32).astype(BF16)
    eye = (ia == ib).astype(F32).astype(BF16)
    l_rt.wait()
    l_gt.wait()
    rt = rts[...]
    gt = gts[...].astype(F32)

    def select(k):
        r = rt[:, k, :]
        g = gt[:, k, :]
        names, shares = [], []
        for e in range(flight):
            m = r == e
            nm = jnp.max(jnp.where(m, 1.0, 0.0), axis=0, keepdims=True)
            sh = jnp.sum(jnp.where(m, g, 0.0), axis=0, keepdims=True)
            names.append(jnp.broadcast_to(nm, (SLOTS, tok)))
            shares.append(jnp.broadcast_to(sh, (SLOTS, tok)))
        naming = jnp.concatenate(names, axis=0)
        share = jnp.concatenate(shares, axis=0)
        places = jnp.dot(naming.astype(BF16), before, preferred_element_type=F32)
        picks, gated, mixes = [], [], []
        for slot in maps:
            chosen = (naming > 0.5) & (jnp.abs(places - slot) < 0.5)
            picks.append(jnp.where(chosen, 1.0, 0.0).astype(BF16))
            g3 = jnp.where(chosen, share, 0.0).astype(BF16)
            gated.append(g3)
            g3 = g3.reshape(flight, 1, SLOTS, tok)
            g3 = jnp.concatenate([g3, g3], axis=1).reshape(2 * rows, tok)
            mixes.append(lax.dot_general(eye, g3, NT, preferred_element_type=F32).astype(BF16))
        mix[k] = mixes[0]
        mixs[k] = jnp.concatenate(mixes[1:], axis=1)
        for q in range(3):
            selb[k, q] = jnp.concatenate([picks[0], picks[q + 1]], axis=1)
            selgb[k, q] = jnp.concatenate([gated[0], gated[q + 1]], axis=1)

    def view(ref, m, *at):
        return ref.at[(0,) + at] if m == 0 else ref.at[(1,) + at + (m - 1,)]

    def columns(ref, r, *at):
        return jnp.concatenate([ref[at + (natural,)] for natural, _ in pieces(r)], axis=-1)

    def pick(sel, k, x, put):
        last = x[:, rwide:]
        for q in range(3):
            both = jnp.concatenate([x[:, q * rstep : (q + 1) * rstep], last], axis=0)
            got = jnp.dot(sel[k, q], both, preferred_element_type=F32).astype(BF16)
            put(pl.ds(q * rstep, rstep), got.reshape(flight, SLOTS, rstep))

    def dispatch(m):
        k = 0 if m == 0 else 1
        for r in range(ndp) if m == 0 else (m - 1,):

            def put(cs, v, r=r):
                tsend[k, :, r, :, cs] = v

            pick(selb, k, xin[k, r], put)
        for n in [far] * (m >= DIRECT) + near:
            dest = lax.rem(y + n, ny)
            src = view(tsend, m, lax.div(dest, 2))
            rc(src, view(trecv, m, 0, y), s_t, trs.at[m, n - 1], at_y(n)).start()
        own = view(tsend, m, lax.div(y, 2))
        rc(own, view(trecv, m, 1, y), s_t, tdr.at[m], partner).start()
        if m == 0:
            trecv[0, 0, y] = tsend[0, lax.div(y, 2)]
        else:
            trecv[1, 0, y, m - 1] = tsend[1, lax.div(y, 2), m - 1]

    def onward(m, src, n):
        blk = view(trecv, m, 0, src)
        arrived(trs.at[m, n - 1], blk)
        rc(blk, view(trecv, m, 1, src), s_t, tdr.at[m], partner).start()

    def relay(m):
        onward(m, mate_far, relay_n)
        blk = view(trecv, m, 0, mate_far)
        rc(blk, blk, s_t, trs.at[m, far - 1], mate_dev).start()

    def spread(m):
        for n in near[::-1]:
            if n in (far - 1, far + 1) and m < DIRECT:

                @pl.when(relay_n != n)
                def _(n=n):
                    onward(m, ysrc(n), n)
            else:
                onward(m, ysrc(n), n)
    def spread_far(m):
        onward(m, ysrc(far), far)

    def wait_spread(m):
        arrived(tdr.at[m], trecv.at[0, 1] if m == 0 else trecv.at[1, 1, :, m - 1])

    count = nexp * SLOTS

    def turned(v):
        n, w = v.shape
        return pltpu.roll(v.reshape(n // 8, 8, w), 4, 1).reshape(n, w)

    low = lax.rem(lax.broadcasted_iota(jnp.int32, (count // 2, rstep), 0), 8) < 4

    def merge(get):
        tails = [
            get(pl.ds(8, 8), pl.ds(q * rstep, rstep)).astype(F32).reshape(count // 2, rstep) for q in range(3)
        ]
        first = jnp.where(low, turned(tails[0]), tails[1])
        second = turned(tails[2])
        return jnp.concatenate(
            [first.reshape(nexp, 1, 8, rstep), second.reshape(nexp, 1, 8, rstep)], axis=1
        ).reshape(count, rstep)

    def unpack(k, r):
        merged = merge(lambda rs, cs: trecv[k, :, :, r, rs, cs])
        mf = trecv[k, :, :, r, :, :].reshape(count, rwide).astype(F32)
        whole = jnp.concatenate([mf, merged], axis=1)
        xraw[r] = (whole * columns(gns, r, slice(None))).astype(BF16)
        return sum(
            (mf[:, q * rstep : (q + 1) * rstep] * mf[:, q * rstep : (q + 1) * rstep] for q in range(3)),
            merged * merged,
        )

    def project(r):
        for m in range(2):
            part = lax.dot_general(columns(wbuf, r, m, slice(None)), xraw[r], NT, preferred_element_type=F32)
            if r == 0:
                acts[m] = part
            else:
                acts[m] += part

    def gate_up(k, squares):
        total = squares[0] + squares[1] + (squares[2] + squares[3])
        high = total.astype(BF16)
        parts = jnp.concatenate([high, (total - high.astype(F32)).astype(BF16)], axis=1)
        ones = jnp.ones((8, 2 * rstep), BF16)
        sums = lax.dot_general(ones, parts, NT, preferred_element_type=F32)[:1]
        scale = lax.rsqrt(sums * (1.0 / width) + 0.5)
        ga = acts[0] * scale
        ua = acts[1] * scale
        kept = lax.rem(lax.broadcasted_iota(jnp.int32, ga.shape, 1), SLOTS) < CAP
        h = jnp.where(kept, ga / (1.0 + jnp.exp(-ga)) * ua, 0.0)
        hid[k, d] = h.astype(BF16)
        return jnp.transpose(h).astype(BF16)

    def hid_half(k, x, p):
        return hid.at[k, x, pl.ds(p * half, half)]

    def share_hidden(k):
        for q in range(2):
            for j, n in enumerate((1, ndp - 1)):
                part = hid_half(k, d, j if q == 0 else 1 - j)
                rs = hrs.at[k, j] if q == 0 else hns.at[k]
                rc(part, part, s_h, rs, at_x(n)).start()

    def forward_hidden(k):
        for j, n in enumerate((1, ndp - 1)):
            part = hid_half(k, lax.rem(d + ndp - n, ndp), j)
            arrived(hrs.at[k, j], part)
            rc(part, part, s_h, hfr.at[k], at_x(n)).start()

    def wait_hidden(k):
        arrived(hns.at[k], hid.at[k, 0])
        arrived(hfr.at[k], hid.at[k, 0])

    hy = ny // 2

    def share_cot():
        across = lax.rem(d + 2, ndp)
        for j, n in enumerate((1, ndp - 1)):
            src = crecv.at[pl.ds(j * hy, hy), :, across]
            rc(src, cstage.at[j], s_x, cgr.at[j], at_x(n)).start()
        for j, n in enumerate((1, ndp - 1)):
            src = crecv.at[:, :, lax.rem(d + n, ndp)]
            rc(src, cotx.at[0, d], s_x, cxr.at[j], at_x(n)).start()
        cotx[0, d] = crecv[:, :, d]
        rc(cotx.at[0, d], cotx.at[1, d], s_x, cdr, partner).start()

    def forward_cot():
        for j, n in enumerate((1, ndp - 1)):
            arrived(cgr.at[j], cstage.at[j])
            dst = cotx.at[0, lax.rem(d + ndp - n, ndp), pl.ds(j * hy, hy)]
            rc(cstage.at[j], dst, s_x, cfr, at_x(n)).start()

    def spread_cot():
        for j, n in enumerate((1, ndp - 1)):
            x = lax.rem(d + ndp - n, ndp)
            arrived(cxr.at[j], cotx.at[0, x])
            rc(cotx.at[0, x], cotx.at[1, x], s_x, cdr, partner).start()
        x = lax.rem(d + 2, ndp)
        arrived(cfr, cotx.at[0, x])
        rc(cotx.at[0, x], cotx.at[1, x], s_x, cdr, partner).start()

    hrows = count // 2

    def direct(k, r, n, dest):
        return rc(rsend.at[k, r, dest], rrecv.at[k, r, y], s_r, rrs.at[k, r], at_y(n))

    def urgent(k, r):
        return k == 0

    def multiply(k, r, h):
        part = jnp.dot(h, columns(wbuf, r, 2, slice(None)), preferred_element_type=F32)
        dsend[k, r] = part[hrows:].astype(BF16)
        rc(dsend.at[k, r], drecv.at[k, r], s_d, drs.at[k, r], partner).start()
        psum[r] = part[:hrows]

    def pack(k, r):
        with jax.named_scope(f"dw{k}{r}"):
            arrived(drs.at[k, r], drecv.at[k, r])
        total = psum[r] + drecv[k, r].astype(F32)
        t4 = total.reshape(ny, 2, 8, cols)
        lo, hi = t4[:, 0].reshape(ny * 8, cols), t4[:, 1].reshape(ny * 8, cols)
        lo3, hi3 = lo[:, rwide:], hi[:, rwide:]
        fill = jnp.concatenate([turned(lo3), lo3, turned(hi3)], axis=1)
        low = lax.rem(lax.broadcasted_iota(jnp.int32, (ny * 8, rwide), 0), 8) < 4
        hi = jnp.where(low, hi[:, :rwide], fill)
        packed = jnp.concatenate(
            [lo[:, :rwide].reshape(ny, 1, 8, rwide), hi.reshape(ny, 1, 8, rwide)], axis=1
        )
        rsend[k, r] = packed.reshape(ny, SLOTS, rwide).astype(BF16)
        if not urgent(k, r):
            rc(rsend.at[k, r, lax.rem(y + far, ny)], mrecv.at[r], s_m, mrs.at[r], mate_dev).start()

    def straight(k, r):
        for n in [far] * urgent(k, r) + near:
            if n in (far - 1, far + 1) and not urgent(k, r):

                @pl.when(2 * far - relay_n != n)
                def _(n=n):
                    direct(k, r, n, lax.rem(y + n, ny)).start()
            else:
                direct(k, r, n, lax.rem(y + n, ny)).start()
        rrecv[k, r, y] = rsend[k, r, y]

    def finish_far(k, r):
        with jax.named_scope(f"mw{k}{r}"):
            arrived(mrs.at[r], mrecv.at[r])
        both = rsend[k, r, mate_far].astype(F32) + mrecv[r].astype(F32)
        rsend[k, r, mate_far] = both.astype(BF16)
        dest = (s, mate_far * 2 + c, d)
        rc(rsend.at[k, r, mate_far], rrecv.at[k, r, y], s_r, rrs.at[k, r], dest).start()

    def zcopy(r, sec):
        return rc(obuf.at[0, r], xin.at[1, r], s_z, zrs.at[r], (sec, i, d))

    def combine(k, r):
        with jax.named_scope(f"rw{k}{r}"):
            arrived(rrs.at[k, r], rrecv.at[k, r, pl.ds(0, len(near) + urgent(k, r))])
        got = rrecv[k, r].reshape(ny * SLOTS, rwide)
        folded = jnp.concatenate([got[:, q * rstep : (q + 1) * rstep] for q in range(3)], axis=0)
        res = xin[k, r].astype(F32) + jnp.concatenate(
            [
                jnp.dot(mix[k], got, preferred_element_type=F32),
                jnp.dot(mixs[k], folded, preferred_element_type=F32),
            ],
            axis=1,
        )
        obuf[k, r] = res.astype(BF16)
        for natural, local in pieces(r):
            pltpu.make_async_copy(obuf.at[k, r, :, local], out.at[k, :, natural], lsem.at[6 + k]).start()
        if k == 0:

            @pl.when(s < nsec - 1)
            def _():
                zcopy(r, s + 1).start()

    def zwait(r):
        with jax.named_scope(f"zw{r}"):

            @pl.when(s > 0)
            def _():
                zcopy(r, s - 1).wait_recv()

            if r == 0:

                @pl.when(s == 0)
                def _():
                    pltpu.make_async_copy(xin.at[1], xin.at[1], lsem.at[5]).wait()

    def cot_arrive(n):
        arrived(crs.at[n - 1], crecv.at[ysrc(n)])

    select(0)
    pltpu.make_async_copy(xin.at[0], xin.at[0], lsem.at[0]).wait()
    with jax.named_scope("disp0"):
        dispatch(0)
    select(1)
    for k in range(2):
        for r in range(ndp):
            if not urgent(k, r):
                rrecv[k, r, lax.rem(y + far, ny)] = jnp.zeros((SLOTS, rwide), BF16)
    l_cot.wait()
    for k in range(2):
        for b in range(ndp):

            def put(cs, v, k=k, b=b):
                csend[:, k, b, :, cs] = v

            pick(selgb, k, cin[k, :, b * cols : (b + 1) * cols], put)
    with jax.named_scope("rel0"):
        relay(0)
    with jax.named_scope("spr0"):
        spread(0)
        spread_far(0)
    for n in near:
        dest = lax.rem(y + n, ny)
        rc(csend.at[lax.div(dest, 2)], crecv.at[y], s_c, crs.at[n - 1], at_y(n)).start()
    crecv[y] = csend[lax.div(y, 2)]
    with jax.named_scope("fw0"):
        forward_w(0)
    with jax.named_scope("fw1"):
        forward_w(1)
    send_w(2)
    with jax.named_scope("wspr0"):
        wait_spread(0)
    l_gn.wait()
    squares = [unpack(0, r) for r in range(ndp)]
    with jax.named_scope("cotm"):
        blk = crecv.at[mate_far]
        arrived(crs.at[relay_n - 1], blk)
        rc(blk, blk, s_c, crs.at[far - 1], mate_dev).start()
    with jax.named_scope("near01"):
        wait_near(0)
        wait_near(1)
    for r in range(ndp - 1):
        project(r)
    with jax.named_scope("far01"):
        wait_far(0)
        wait_far(1)
    project(ndp - 1)
    with jax.named_scope("gu0"):
        h = gate_up(0, squares)
    multiply(0, 0, h)
    pack(0, 0)
    straight(0, 0)
    with jax.named_scope("fw2"):
        forward_w(2)
    multiply(0, 1, h)
    share_hidden(0)
    with jax.named_scope("cotw"):
        for n in near:
            if n in (far - 1, far + 1):

                @pl.when(relay_n != n)
                def _(n=n):
                    cot_arrive(n)
            else:
                cot_arrive(n)
        cot_arrive(far)
    share_cot()
    pack(0, 1)
    straight(0, 1)
    combine(0, 0)
    with jax.named_scope("near2"):
        wait_near(2)
    multiply(0, 2, h)
    pack(0, 2)
    straight(0, 2)
    combine(0, 1)
    zwait(0)
    dispatch(1)
    with jax.named_scope("far2"):
        wait_far(2)
    multiply(0, 3, h)
    pack(0, 3)
    straight(0, 3)
    combine(0, 2)
    zwait(1)
    dispatch(2)

    with jax.named_scope("rel1"):
        relay(1)
    combine(0, 3)
    with jax.named_scope("fh0"):
        forward_hidden(0)
    with jax.named_scope("fc"):
        forward_cot()
    zwait(2)
    dispatch(3)
    with jax.named_scope("spr1"):
        spread(1)
        spread_far(1)
    zwait(3)
    dispatch(4)
    with jax.named_scope("spr2"):
        spread(2)
    with jax.named_scope("sprf2"):
        spread_far(2)
    with jax.named_scope("spr3"):
        spread(3)
    squares = []
    for r in range(2):
        wait_spread(r + 1)
        squares.append(unpack(1, r))
        project(r)
    with jax.named_scope("sprf3"):
        spread_far(3)
    with jax.named_scope("spr4"):
        spread(4)
    with jax.named_scope("sprf4"):
        spread_far(4)
    with jax.named_scope("wspr3"):
        wait_spread(3)
    squares.append(unpack(1, 2))
    project(2)
    with jax.named_scope("wspr4"):
        wait_spread(4)
    squares.append(unpack(1, 3))
    project(3)
    with jax.named_scope("gu1"):
        h = gate_up(1, squares)
    share_hidden(1)
    multiply(1, 0, h)
    multiply(1, 1, h)
    pack(1, 0)
    straight(1, 0)
    multiply(1, 2, h)
    multiply(1, 3, h)
    for r in range(1, ndp):
        pack(1, r)
    straight(1, 1)
    finish_far(1, 0)
    with jax.named_scope("sc"):
        spread_cot()
    with jax.named_scope("fh1"):
        forward_hidden(1)
    finish_far(1, 1)
    finish_far(1, 2)
    straight(1, 2)
    finish_far(1, 3)
    straight(1, 3)
    with jax.named_scope("wsc"):
        arrived(cdr, cotx.at[1])

    def grad(k):
        with jax.named_scope(f"wh{k}"):
            wait_hidden(k)
        with jax.named_scope(f"grad{k}"):
            for x in range(ndp):
                merged = merge(lambda rs, cs, x=x, k=k: cotx[:, x, :, k, rs, cs]).astype(BF16)
                main = cotx[:, x, :, k].reshape(count, rwide)
                cr = jnp.concatenate([main, merged], axis=1)
                add = jnp.dot(hid[k, x], cr, preferred_element_type=F32)
                if k == 0 and x == 0:
                    gacc[...] = add
                else:
                    gacc[...] += add

    grad(0)
    combine(1, 0)
    combine(1, 1)
    grad(1)
    gout = pltpu.make_async_copy(gacc, grad_out, lsem.at[8])
    gout.start()
    combine(1, 2)
    combine(1, 3)
    with jax.named_scope("tail"):
        drain(s_w, wbuf.at[:, :, pl.ds(0, 3 * cols)])
        drain(s_t, trecv.at[0])
        drain(s_t, trecv.at[1, :, pl.ds(0, ny - 1)])
        drain(s_c, crecv.at[pl.ds(0, ny - 1)])
        drain(s_x, cotx.at[1])
        drain(s_x, cotx.at[0, pl.ds(0, 3)])
        drain(s_x, cstage)
        drain(s_h, hid.at[:, pl.ds(0, 3)])
        drain(s_d, drecv)
        drain(s_m, mrecv)
        drain(s_r, rrecv.at[0, :, pl.ds(0, len(near) + 1)])
        drain(s_r, rrecv.at[1, :, pl.ds(0, len(near))])
    with jax.named_scope("zs"):

        @pl.when(s < nsec - 1)
        def _():
            drain(s_z, obuf.at[0])

    with jax.named_scope("outw"):
        gout.wait()
        for k in range(2):
            pltpu.make_async_copy(obuf.at[k], obuf.at[k], lsem.at[6 + k]).wait()


def store_body(out, grad, out_hbm, grad_hbm, sem):
    a = pltpu.make_async_copy(out, out_hbm, sem.at[0])
    b = pltpu.make_async_copy(grad, grad_hbm, sem.at[1])
    a.start()
    b.start()
    a.wait()
    b.wait()


def local(nsec, nexp, ndp, arrivals, fresh, routes, gates, cotangent, norm_gain, w_gate, w_up, w_down):
    tok, width = arrivals.shape[1:]
    hidn, cols = w_gate.shape[1:]
    flight = nexp // SPLIT
    ny = nexp // 2
    steps = routes.shape[1]
    rows = nexp * SLOTS
    routes_t = jnp.transpose(routes[0], (2, 0, 1))
    gates_t = jnp.transpose(gates[0], (2, 0, 1))
    rwide = cols // 4 * 3
    any_spec = pl.BlockSpec(memory_space=pl.ANY)
    hbm_spec = pl.BlockSpec(memory_space=pltpu.HBM)
    dma = pltpu.SemaphoreType.DMA
    out, grad = pl.pallas_call(
        functools.partial(kernel_body, nsec, nexp, ndp),
        name="moe_relay",
        out_shape=(
            jax.ShapeDtypeStruct((steps, tok, width), BF16),
            jax.ShapeDtypeStruct((hidn, cols), F32),
        ),
        in_specs=[hbm_spec] * 9,
        out_specs=(any_spec, any_spec),
        scratch_shapes=[
            pltpu.VMEM((2, ndp, tok, cols), BF16),
            pltpu.VMEM((2, tok, width), BF16),
            pltpu.VMEM((3, hidn, width), BF16),
            pltpu.VMEM((2, flight, ndp, SLOTS, rwide), BF16),
            pltpu.VMEM((2, 2, ny, ndp, SLOTS, rwide), BF16),
            pltpu.VMEM((ndp, rows, cols), BF16),
            pltpu.VMEM((2, hidn, rows), F32),
            pltpu.VMEM((flight, 2, ndp, SLOTS, rwide), BF16),
            pltpu.VMEM((ny, 2, ndp, SLOTS, rwide), BF16),
            pltpu.VMEM((2, ny // 2, 2, SLOTS, rwide), BF16),
            pltpu.VMEM((2, ndp, ny, 2, SLOTS, rwide), BF16),
            pltpu.VMEM((2, ndp, hidn, rows), BF16),
            pltpu.VMEM((2, ndp, rows // 2, cols), BF16),
            pltpu.VMEM((2, ndp, rows // 2, cols), BF16),
            pltpu.VMEM((ndp, rows // 2, cols), F32),
            pltpu.VMEM((2, ndp, ny, SLOTS, rwide), BF16),
            pltpu.VMEM((ndp, SLOTS, rwide), BF16),
            pltpu.VMEM((2, ndp, ny, SLOTS, rwide), BF16),
            pltpu.VMEM(routes_t.shape, jnp.int32),
            pltpu.VMEM(gates_t.shape, BF16),
            pltpu.VMEM((1, width), F32),
            pltpu.VMEM((2, 3, flight * SLOTS, 2 * tok), BF16),
            pltpu.VMEM((2, 3, flight * SLOTS, 2 * tok), BF16),
            pltpu.VMEM((2, tok, ny * SLOTS), BF16),
            pltpu.VMEM((2, tok, 3 * ny * SLOTS), BF16),
            pltpu.VMEM((2, ndp, tok, cols), BF16),
            pltpu.VMEM((hidn, cols), F32),
            dma((12,)), dma((9,)),
            dma((3, 2)), dma((3,)), dma((3,)),
            dma((1 + ndp, ny - 1)), dma((1 + ndp,)),
            dma((ny - 1,)), dma((2,)), dma((2,)), dma(()), dma(()),
            dma((2, 2)), dma((2,)), dma((2,)),
            dma((2, ndp)), dma((ndp,)), dma((2, ndp)), dma((ndp,)),
        ],
        compiler_params=pltpu.CompilerParams(
            collective_id=0, has_side_effects=True, vmem_limit_bytes=24 * 1024 * 1024
        ),
    )(
        *(
            pltpu.with_memory_space_constraint(a, pltpu.HBM)
            for a in (
                arrivals[0], fresh[0], routes_t, gates_t, cotangent[0], norm_gain, w_gate[0], w_up[0], w_down[0]
            )
        )
    )
    out, grad = pl.pallas_call(
        store_body,
        name="store",
        out_shape=(jax.ShapeDtypeStruct(out.shape, BF16), jax.ShapeDtypeStruct(grad.shape, F32)),
        in_specs=(any_spec, any_spec),
        out_specs=(any_spec, any_spec),
        scratch_shapes=[dma((2,))],
        compiler_params=pltpu.CompilerParams(vmem_limit_bytes=1024 * 1024),
    )(out, grad)
    return out[None], grad[None]


def solution(mesh):
    placed = (
        P("section", ("expert", "dp"), None),
        P(None, ("expert", "dp"), None),
        P("section", None, ("expert", "dp"), None),
        P("section", None, ("expert", "dp"), None),
        P("section", None, ("expert", "dp"), None),
        P("section", None),
        P("section", "expert", "dp"),
        P("section", "expert", "dp"),
        P("section", "expert", "dp"),
    )
    return jax.shard_map(
        functools.partial(local, mesh.shape["section"], mesh.shape["expert"], mesh.shape["dp"]),
        mesh=mesh,
        in_specs=placed,
        out_specs=(P("section", None, ("expert", "dp"), None), P("section", "expert", "dp")),
        check_vma=False,
    )
```

```python
import functools

import jax
import jax.numpy as jnp
from jax import lax
from jax.experimental import pallas as pl
from jax.experimental.pallas import tpu as pltpu
from jax.sharding import PartitionSpec as P

SPLIT = 4
CAP = 12
SLOTS = 16
DIRECT = 2
NEAR = (3, 5, 2, 6, 1, 7)
MESH = pl.DeviceIdType.MESH
NT = (((1,), (1,)), ((), ()))
F32 = jnp.float32
BF16 = jnp.bfloat16


def kernel_body(
    nsec, nexp, ndp,
    arr, fresh, routes, gates, cot, gain, wg, wu, wd,
    out, grad_out,
    xin, cin, wbuf, tsend, trecv, xraw, acts, csend, crecv, cstage, cotx, hid, dsend, drecv, psum, rsend, mrecv, rrecv,
    rts, gts, gns, selb, selgb, mix, mixs, obuf, gacc,
    lsem, sends, wrs, wns, frs, trs, tdr, crs, cxr, cgr, cfr, cdr, hrs, hns, hfr, drs, mrs, rrs, zrs,
):
    s = lax.axis_index("section")
    i = lax.axis_index("expert")
    d = lax.axis_index("dp")
    ny = nexp // 2
    y = lax.div(i, 2)
    c = lax.rem(i, 2)
    tok, width = arr.shape
    hidn, cols = wg.shape
    half = hidn // 2
    hc = cols // 2
    rwide = rsend.shape[4]
    rstep = rwide // 3
    far = ny // 2
    near = [n for n in NEAR if 0 < n < ny and n != far]
    odd = lax.rem(y, 2)
    mate = y + 1 - 2 * odd
    mate_far = lax.rem(mate + far, ny)
    relay_n = far - 1 + 2 * odd
    mate_dev = (s, mate * 2 + c, d)
    flight = nexp // SPLIT
    rows = flight * SLOTS

    def at_x(k):
        return (s, i, lax.rem(d + k, ndp))

    def at_y(k):
        return (s, lax.rem(y + k, ny) * 2 + c, d)

    def ysrc(k):
        return lax.rem(y + ny - k, ny)

    partner = (s, y * 2 + 1 - c, d)

    def colsl(x):
        return pl.ds(pl.multiple_of(x * cols, cols), cols)

    def rc(src, dst, ss, rs, dev):
        return pltpu.make_async_remote_copy(
            src_ref=src, dst_ref=dst, send_sem=ss, recv_sem=rs, device_id=dev, device_id_type=MESH
        )

    s_w, s_t, s_c, s_x, s_h, s_d, s_m, s_r, s_z = (sends.at[n] for n in range(9))

    def drain(sem, ref):
        rc(ref, ref, sem, sem, partner).wait_send()

    def arrived(sem, ref):
        rc(ref, ref, sem, sem, partner).wait_recv()

    near_dp, far_dp = (lax.rem(d + ndp - 1, ndp), lax.rem(d + 1, ndp)), lax.rem(d + 2, ndp)
    HALVES = (
        ((d, 0), (d, 1)),
        ((near_dp[0], 0), (near_dp[1], 1)),
        ((near_dp[0], 1), (near_dp[1], 0)),
        ((far_dp, 0), (far_dp, 1)),
    )

    def hs(owner, j):
        return pl.ds(pl.multiple_of(owner * cols + j * hc, hc), hc)

    def pieces(r):
        return [(hs(o, j), slice(q * hc, (q + 1) * hc)) for q, (o, j) in enumerate(HALVES[r])]

    def by_block(src, dst, sem, back=False):
        for r in range(ndp):
            for natural, local in pieces(r):
                a, b = src.at[:, natural], dst.at[r, :, local]
                pltpu.make_async_copy(a, b, sem).start()

    bar = pltpu.get_barrier_semaphore()
    peers = [at_x(k) for k in range(1, ndp)] + [at_y(n) for n in range(1, ny)] + [partner]
    for p in peers:
        pl.semaphore_signal(bar, inc=1, device_id=p, device_id_type=MESH)

    @pl.when(s > 0)
    def _():
        pl.semaphore_signal(bar, inc=1, device_id=(s - 1, i, d), device_id_type=MESH)

    @pl.when(s < nsec - 1)
    def _():
        pl.semaphore_signal(bar, inc=1, device_id=(s + 1, i, d), device_id_type=MESH)

    l_cot = pltpu.make_async_copy(cot, cin, lsem.at[1])
    l_w = [
        pltpu.make_async_copy(w, wbuf.at[m, :, colsl(d)], lsem.at[2 + m])
        for m, w in enumerate((wg, wu, wd))
    ]
    l_rt = pltpu.make_async_copy(routes, rts, lsem.at[9])
    l_gt = pltpu.make_async_copy(gates, gts, lsem.at[10])
    l_gn = pltpu.make_async_copy(gain, gns, lsem.at[11])
    for l in l_w:
        l.start()
    l_rt.start()
    l_gt.start()
    by_block(arr, xin.at[0], lsem.at[0])
    l_gn.start()
    l_cot.start()

    @pl.when(s == 0)
    def _():
        by_block(fresh, xin.at[1], lsem.at[5])

    with jax.named_scope("bar"):
        pl.semaphore_wait(
            bar,
            len(peers) + jnp.where(s > 0, 1, 0) + jnp.where(s < nsec - 1, 1, 0),
        )

    def part_of(m, j, owner):
        return wbuf.at[m, :, hs(owner, j)]

    def send_w(m):
        l_w[m].wait()
        for q in range(2):
            for j, k in enumerate((1, ndp - 1)):
                p = j if q == 0 else 1 - j
                rs = wrs.at[m, j] if q == 0 else wns.at[m]
                part = part_of(m, p, d)
                rc(part, part, s_w, rs, at_x(k)).start()

    def forward_w(m):
        for j, k in enumerate((1, ndp - 1)):
            part = part_of(m, j, lax.rem(d + ndp - k, ndp))
            arrived(wrs.at[m, j], part)
            rc(part, part, s_w, frs.at[m], at_x(k)).start()

    def wait_near(m):
        arrived(wns.at[m], wbuf.at[m, :, pl.ds(0, cols)])

    def wait_far(m):
        arrived(frs.at[m], wbuf.at[m, :, pl.ds(0, cols)])

    send_w(0)
    send_w(1)

    pos = lax.rem(lax.broadcasted_iota(jnp.int32, (rows, tok), 0), SLOTS)
    tail = SLOTS - CAP
    maps = [jnp.where(pos < CAP, pos, -5).astype(F32)]
    for q in range(3):
        maps.append(jnp.where(pos >= CAP, pos - CAP + tail * q, -5).astype(F32))
    ia = lax.broadcasted_iota(jnp.int32, (tok, tok), 0)
    ib = lax.broadcasted_iota(jnp.int32, (tok, tok), 1)
    before = (ia < ib).astype(F32).astype(BF16)
    eye = (ia == ib).astype(F32).astype(BF16)
    l_rt.wait()
    l_gt.wait()
    rt = rts[...]
    gt = gts[...].astype(F32)

    def select(k):
        r = rt[:, k, :]
        g = gt[:, k, :]
        names, shares = [], []
        for e in range(flight):
            m = r == e
            nm = jnp.max(jnp.where(m, 1.0, 0.0), axis=0, keepdims=True)
            sh = jnp.sum(jnp.where(m, g, 0.0), axis=0, keepdims=True)
            names.append(jnp.broadcast_to(nm, (SLOTS, tok)))
            shares.append(jnp.broadcast_to(sh, (SLOTS, tok)))
        naming = jnp.concatenate(names, axis=0)
        share = jnp.concatenate(shares, axis=0)
        places = jnp.dot(naming.astype(BF16), before, preferred_element_type=F32)
        picks, gated, mixes = [], [], []
        for slot in maps:
            chosen = (naming > 0.5) & (jnp.abs(places - slot) < 0.5)
            picks.append(jnp.where(chosen, 1.0, 0.0).astype(BF16))
            g3 = jnp.where(chosen, share, 0.0).astype(BF16)
            gated.append(g3)
            g3 = g3.reshape(flight, 1, SLOTS, tok)
            g3 = jnp.concatenate([g3, g3], axis=1).reshape(2 * rows, tok)
            mixes.append(lax.dot_general(eye, g3, NT, preferred_element_type=F32).astype(BF16))
        mix[k] = mixes[0]
        mixs[k] = jnp.concatenate(mixes[1:], axis=1)
        for q in range(3):
            selb[k, q] = jnp.concatenate([picks[0], picks[q + 1]], axis=1)
            selgb[k, q] = jnp.concatenate([gated[0], gated[q + 1]], axis=1)

    def view(ref, m, *at):
        return ref.at[(0,) + at] if m == 0 else ref.at[(1,) + at + (m - 1,)]

    def columns(ref, r, *at):
        return jnp.concatenate([ref[at + (natural,)] for natural, _ in pieces(r)], axis=-1)

    def pick(sel, k, x, put):
        last = x[:, rwide:]
        for q in range(3):
            both = jnp.concatenate([x[:, q * rstep : (q + 1) * rstep], last], axis=0)
            got = jnp.dot(sel[k, q], both, preferred_element_type=F32).astype(BF16)
            put(pl.ds(q * rstep, rstep), got.reshape(flight, SLOTS, rstep))

    def dispatch(m):
        k = 0 if m == 0 else 1
        for r in range(ndp) if m == 0 else (m - 1,):

            def put(cs, v, r=r):
                tsend[k, :, r, :, cs] = v

            pick(selb, k, xin[k, r], put)
        for n in [far] * (m >= DIRECT) + near:
            dest = lax.rem(y + n, ny)
            src = view(tsend, m, lax.div(dest, 2))
            rc(src, view(trecv, m, 0, y), s_t, trs.at[m, n - 1], at_y(n)).start()
        own = view(tsend, m, lax.div(y, 2))
        rc(own, view(trecv, m, 1, y), s_t, tdr.at[m], partner).start()
        if m == 0:
            trecv[0, 0, y] = tsend[0, lax.div(y, 2)]
        else:
            trecv[1, 0, y, m - 1] = tsend[1, lax.div(y, 2), m - 1]

    def onward(m, src, n):
        blk = view(trecv, m, 0, src)
        arrived(trs.at[m, n - 1], blk)
        rc(blk, view(trecv, m, 1, src), s_t, tdr.at[m], partner).start()

    def relay(m):
        onward(m, mate_far, relay_n)
        blk = view(trecv, m, 0, mate_far)
        rc(blk, blk, s_t, trs.at[m, far - 1], mate_dev).start()

    def spread(m):
        for n in near[::-1]:
            if n in (far - 1, far + 1) and m < DIRECT:

                @pl.when(relay_n != n)
                def _(n=n):
                    onward(m, ysrc(n), n)
            else:
                onward(m, ysrc(n), n)
    def spread_far(m):
        onward(m, ysrc(far), far)

    def wait_spread(m):
        arrived(tdr.at[m], trecv.at[0, 1] if m == 0 else trecv.at[1, 1, :, m - 1])

    count = nexp * SLOTS

    def turned(v):
        n, w = v.shape
        return pltpu.roll(v.reshape(n // 8, 8, w), 4, 1).reshape(n, w)

    low = lax.rem(lax.broadcasted_iota(jnp.int32, (count // 2, rstep), 0), 8) < 4

    def merge(get):
        tails = [
            get(pl.ds(8, 8), pl.ds(q * rstep, rstep)).astype(F32).reshape(count // 2, rstep) for q in range(3)
        ]
        first = jnp.where(low, turned(tails[0]), tails[1])
        second = turned(tails[2])
        return jnp.concatenate(
            [first.reshape(nexp, 1, 8, rstep), second.reshape(nexp, 1, 8, rstep)], axis=1
        ).reshape(count, rstep)

    def unpack(k, r):
        merged = merge(lambda rs, cs: trecv[k, :, :, r, rs, cs])
        mf = trecv[k, :, :, r, :, :].reshape(count, rwide).astype(F32)
        whole = jnp.concatenate([mf, merged], axis=1)
        xraw[r] = (whole * columns(gns, r, slice(None))).astype(BF16)
        return sum(
            (mf[:, q * rstep : (q + 1) * rstep] * mf[:, q * rstep : (q + 1) * rstep] for q in range(3)),
            merged * merged,
        )

    def project(r):
        for m in range(2):
            part = lax.dot_general(columns(wbuf, r, m, slice(None)), xraw[r], NT, preferred_element_type=F32)
            if r == 0:
                acts[m] = part
            else:
                acts[m] += part

    def gate_up(k, squares):
        total = squares[0] + squares[1] + (squares[2] + squares[3])
        high = total.astype(BF16)
        parts = jnp.concatenate([high, (total - high.astype(F32)).astype(BF16)], axis=1)
        ones = jnp.ones((8, 2 * rstep), BF16)
        sums = lax.dot_general(ones, parts, NT, preferred_element_type=F32)[:1]
        scale = lax.rsqrt(sums * (1.0 / width) + 0.5)
        ga = acts[0] * scale
        ua = acts[1] * scale
        kept = lax.rem(lax.broadcasted_iota(jnp.int32, ga.shape, 1), SLOTS) < CAP
        h = jnp.where(kept, ga / (1.0 + jnp.exp(-ga)) * ua, 0.0)
        hid[k, d] = h.astype(BF16)
        return jnp.transpose(h).astype(BF16)

    def hid_half(k, x, p):
        return hid.at[k, x, pl.ds(p * half, half)]

    def share_hidden(k):
        for q in range(2):
            for j, n in enumerate((1, ndp - 1)):
                part = hid_half(k, d, j if q == 0 else 1 - j)
                rs = hrs.at[k, j] if q == 0 else hns.at[k]
                rc(part, part, s_h, rs, at_x(n)).start()

    def forward_hidden(k):
        for j, n in enumerate((1, ndp - 1)):
            part = hid_half(k, lax.rem(d + ndp - n, ndp), j)
            arrived(hrs.at[k, j], part)
            rc(part, part, s_h, hfr.at[k], at_x(n)).start()

    def wait_hidden(k):
        arrived(hns.at[k], hid.at[k, 0])
        arrived(hfr.at[k], hid.at[k, 0])

    hy = ny // 2

    def share_cot():
        across = lax.rem(d + 2, ndp)
        for j, n in enumerate((1, ndp - 1)):
            src = crecv.at[pl.ds(j * hy, hy), :, across]
            rc(src, cstage.at[j], s_x, cgr.at[j], at_x(n)).start()
        for j, n in enumerate((1, ndp - 1)):
            src = crecv.at[:, :, lax.rem(d + n, ndp)]
            rc(src, cotx.at[0, d], s_x, cxr.at[j], at_x(n)).start()
        cotx[0, d] = crecv[:, :, d]
        rc(cotx.at[0, d], cotx.at[1, d], s_x, cdr, partner).start()

    def forward_cot():
        for j, n in enumerate((1, ndp - 1)):
            arrived(cgr.at[j], cstage.at[j])
            dst = cotx.at[0, lax.rem(d + ndp - n, ndp), pl.ds(j * hy, hy)]
            rc(cstage.at[j], dst, s_x, cfr, at_x(n)).start()

    def spread_cot():
        for j, n in enumerate((1, ndp - 1)):
            x = lax.rem(d + ndp - n, ndp)
            arrived(cxr.at[j], cotx.at[0, x])
            rc(cotx.at[0, x], cotx.at[1, x], s_x, cdr, partner).start()
        x = lax.rem(d + 2, ndp)
        arrived(cfr, cotx.at[0, x])
        rc(cotx.at[0, x], cotx.at[1, x], s_x, cdr, partner).start()

    hrows = count // 2

    def direct(k, r, n, dest):
        return rc(rsend.at[k, r, dest], rrecv.at[k, r, y], s_r, rrs.at[k, r], at_y(n))

    def urgent(k, r):
        return k == 0

    def multiply(k, r, h):
        part = jnp.dot(h, columns(wbuf, r, 2, slice(None)), preferred_element_type=F32)
        dsend[k, r] = part[hrows:].astype(BF16)
        rc(dsend.at[k, r], drecv.at[k, r], s_d, drs.at[k, r], partner).start()
        psum[r] = part[:hrows]

    def pack(k, r):
        with jax.named_scope(f"dw{k}{r}"):
            arrived(drs.at[k, r], drecv.at[k, r])
        total = psum[r] + drecv[k, r].astype(F32)
        t4 = total.reshape(ny, 2, 8, cols)
        lo, hi = t4[:, 0].reshape(ny * 8, cols), t4[:, 1].reshape(ny * 8, cols)
        lo3, hi3 = lo[:, rwide:], hi[:, rwide:]
        fill = jnp.concatenate([turned(lo3), lo3, turned(hi3)], axis=1)
        low = lax.rem(lax.broadcasted_iota(jnp.int32, (ny * 8, rwide), 0), 8) < 4
        hi = jnp.where(low, hi[:, :rwide], fill)
        packed = jnp.concatenate(
            [lo[:, :rwide].reshape(ny, 1, 8, rwide), hi.reshape(ny, 1, 8, rwide)], axis=1
        )
        rsend[k, r] = packed.reshape(ny, SLOTS, rwide).astype(BF16)
        if not urgent(k, r):
            rc(rsend.at[k, r, lax.rem(y + far, ny)], mrecv.at[r], s_m, mrs.at[r], mate_dev).start()

    def straight(k, r):
        for n in [far] * urgent(k, r) + near:
            if n in (far - 1, far + 1) and not urgent(k, r):

                @pl.when(2 * far - relay_n != n)
                def _(n=n):
                    direct(k, r, n, lax.rem(y + n, ny)).start()
            else:
                direct(k, r, n, lax.rem(y + n, ny)).start()
        rrecv[k, r, y] = rsend[k, r, y]

    def finish_far(k, r):
        with jax.named_scope(f"mw{k}{r}"):
            arrived(mrs.at[r], mrecv.at[r])
        both = rsend[k, r, mate_far].astype(F32) + mrecv[r].astype(F32)
        rsend[k, r, mate_far] = both.astype(BF16)
        dest = (s, mate_far * 2 + c, d)
        rc(rsend.at[k, r, mate_far], rrecv.at[k, r, y], s_r, rrs.at[k, r], dest).start()

    def zcopy(r, sec):
        return rc(obuf.at[0, r], xin.at[1, r], s_z, zrs.at[r], (sec, i, d))

    def combine(k, r):
        with jax.named_scope(f"rw{k}{r}"):
            arrived(rrs.at[k, r], rrecv.at[k, r, pl.ds(0, len(near) + urgent(k, r))])
        got = rrecv[k, r].reshape(ny * SLOTS, rwide)
        folded = jnp.concatenate([got[:, q * rstep : (q + 1) * rstep] for q in range(3)], axis=0)
        res = xin[k, r].astype(F32) + jnp.concatenate(
            [
                jnp.dot(mix[k], got, preferred_element_type=F32),
                jnp.dot(mixs[k], folded, preferred_element_type=F32),
            ],
            axis=1,
        )
        obuf[k, r] = res.astype(BF16)
        for natural, local in pieces(r):
            pltpu.make_async_copy(obuf.at[k, r, :, local], out.at[k, :, natural], lsem.at[6 + k]).start()
        if k == 0:

            @pl.when(s < nsec - 1)
            def _():
                zcopy(r, s + 1).start()

    def zwait(r):
        with jax.named_scope(f"zw{r}"):

            @pl.when(s > 0)
            def _():
                zcopy(r, s - 1).wait_recv()

            if r == 0:

                @pl.when(s == 0)
                def _():
                    pltpu.make_async_copy(xin.at[1], xin.at[1], lsem.at[5]).wait()

    def cot_arrive(n):
        arrived(crs.at[n - 1], crecv.at[ysrc(n)])

    select(0)
    pltpu.make_async_copy(xin.at[0], xin.at[0], lsem.at[0]).wait()
    with jax.named_scope("disp0"):
        dispatch(0)
    select(1)
    for k in range(2):
        for r in range(ndp):
            if not urgent(k, r):
                rrecv[k, r, lax.rem(y + far, ny)] = jnp.zeros((SLOTS, rwide), BF16)
    l_cot.wait()
    for k in range(2):
        for b in range(ndp):

            def put(cs, v, k=k, b=b):
                csend[:, k, b, :, cs] = v

            pick(selgb, k, cin[k, :, b * cols : (b + 1) * cols], put)
    with jax.named_scope("rel0"):
        relay(0)
    with jax.named_scope("spr0"):
        spread(0)
        spread_far(0)
    for n in near:
        dest = lax.rem(y + n, ny)
        rc(csend.at[lax.div(dest, 2)], crecv.at[y], s_c, crs.at[n - 1], at_y(n)).start()
    crecv[y] = csend[lax.div(y, 2)]
    with jax.named_scope("fw0"):
        forward_w(0)
    with jax.named_scope("fw1"):
        forward_w(1)
    send_w(2)
    with jax.named_scope("wspr0"):
        wait_spread(0)
    l_gn.wait()
    squares = [unpack(0, r) for r in range(ndp)]
    with jax.named_scope("cotm"):
        blk = crecv.at[mate_far]
        arrived(crs.at[relay_n - 1], blk)
        rc(blk, blk, s_c, crs.at[far - 1], mate_dev).start()
    with jax.named_scope("near01"):
        wait_near(0)
        wait_near(1)
    for r in range(ndp - 1):
        project(r)
    with jax.named_scope("far01"):
        wait_far(0)
        wait_far(1)
    project(ndp - 1)
    with jax.named_scope("gu0"):
        h = gate_up(0, squares)
    multiply(0, 0, h)
    pack(0, 0)
    straight(0, 0)
    with jax.named_scope("fw2"):
        forward_w(2)
    multiply(0, 1, h)
    share_hidden(0)
    with jax.named_scope("cotw"):
        for n in near:
            if n in (far - 1, far + 1):

                @pl.when(relay_n != n)
                def _(n=n):
                    cot_arrive(n)
            else:
                cot_arrive(n)
        cot_arrive(far)
    share_cot()
    pack(0, 1)
    straight(0, 1)
    combine(0, 0)
    with jax.named_scope("near2"):
        wait_near(2)
    multiply(0, 2, h)
    pack(0, 2)
    straight(0, 2)
    combine(0, 1)
    zwait(0)
    dispatch(1)
    with jax.named_scope("far2"):
        wait_far(2)
    multiply(0, 3, h)
    pack(0, 3)
    straight(0, 3)
    combine(0, 2)
    zwait(1)
    dispatch(2)

    with jax.named_scope("rel1"):
        relay(1)
    combine(0, 3)
    with jax.named_scope("fh0"):
        forward_hidden(0)
    with jax.named_scope("fc"):
        forward_cot()
    zwait(2)
    dispatch(3)
    with jax.named_scope("spr1"):
        spread(1)
        spread_far(1)
    zwait(3)
    dispatch(4)
    with jax.named_scope("spr2"):
        spread(2)
    with jax.named_scope("sprf2"):
        spread_far(2)
    with jax.named_scope("spr3"):
        spread(3)
    squares = []
    for r in range(2):
        wait_spread(r + 1)
        squares.append(unpack(1, r))
        project(r)
    with jax.named_scope("sprf3"):
        spread_far(3)
    with jax.named_scope("spr4"):
        spread(4)
    with jax.named_scope("sprf4"):
        spread_far(4)
    with jax.named_scope("wspr3"):
        wait_spread(3)
    squares.append(unpack(1, 2))
    project(2)
    with jax.named_scope("wspr4"):
        wait_spread(4)
    squares.append(unpack(1, 3))
    project(3)
    with jax.named_scope("gu1"):
        h = gate_up(1, squares)
    share_hidden(1)
    multiply(1, 0, h)
    multiply(1, 1, h)
    pack(1, 0)
    straight(1, 0)
    multiply(1, 2, h)
    multiply(1, 3, h)
    for r in range(1, ndp):
        pack(1, r)
    straight(1, 1)
    finish_far(1, 0)
    with jax.named_scope("sc"):
        spread_cot()
    with jax.named_scope("fh1"):
        forward_hidden(1)
    finish_far(1, 1)
    finish_far(1, 2)
    straight(1, 2)
    finish_far(1, 3)
    straight(1, 3)
    with jax.named_scope("wsc"):
        arrived(cdr, cotx.at[1])

    def grad(k):
        with jax.named_scope(f"wh{k}"):
            wait_hidden(k)
        with jax.named_scope(f"grad{k}"):
            for x in range(ndp):
                merged = merge(lambda rs, cs, x=x, k=k: cotx[:, x, :, k, rs, cs]).astype(BF16)
                main = cotx[:, x, :, k].reshape(count, rwide)
                cr = jnp.concatenate([main, merged], axis=1)
                add = jnp.dot(hid[k, x], cr, preferred_element_type=F32)
                if k == 0 and x == 0:
                    gacc[...] = add
                else:
                    gacc[...] += add

    grad(0)
    combine(1, 0)
    combine(1, 1)
    grad(1)
    gout = pltpu.make_async_copy(gacc, grad_out, lsem.at[8])
    gout.start()
    with jax.named_scope("tail"):
        drain(s_w, wbuf.at[:, :, pl.ds(0, 3 * cols)])
        drain(s_t, trecv.at[0])
        drain(s_t, trecv.at[1, :, pl.ds(0, ny - 1)])
        drain(s_c, crecv.at[pl.ds(0, ny - 1)])
        drain(s_x, cotx.at[1])
        drain(s_x, cotx.at[0, pl.ds(0, 3)])
        drain(s_x, cstage)
        drain(s_h, hid.at[:, pl.ds(0, 3)])
        drain(s_d, drecv)
        drain(s_m, mrecv)
    with jax.named_scope("zs"):

        @pl.when(s < nsec - 1)
        def _():
            drain(s_z, obuf.at[0])
    pltpu.make_async_copy(obuf.at[0], obuf.at[0], lsem.at[6]).wait()
    combine(1, 2)
    combine(1, 3)
    drain(s_r, rrecv.at[0, :, pl.ds(0, len(near) + 1)])
    drain(s_r, rrecv.at[1, :, pl.ds(0, len(near))])

    with jax.named_scope("outw"):
        gout.wait()
        pltpu.make_async_copy(obuf.at[1], obuf.at[1], lsem.at[7]).wait()


def store_body(out, grad, out_hbm, grad_hbm, sem):
    a = pltpu.make_async_copy(out, out_hbm, sem.at[0])
    b = pltpu.make_async_copy(grad, grad_hbm, sem.at[1])
    a.start()
    b.start()
    a.wait()
    b.wait()


def local(nsec, nexp, ndp, arrivals, fresh, routes, gates, cotangent, norm_gain, w_gate, w_up, w_down):
    tok, width = arrivals.shape[1:]
    hidn, cols = w_gate.shape[1:]
    flight = nexp // SPLIT
    ny = nexp // 2
    steps = routes.shape[1]
    rows = nexp * SLOTS
    routes_t = jnp.transpose(routes[0], (2, 0, 1))
    gates_t = jnp.transpose(gates[0], (2, 0, 1))
    rwide = cols // 4 * 3
    any_spec = pl.BlockSpec(memory_space=pl.ANY)
    hbm_spec = pl.BlockSpec(memory_space=pltpu.HBM)
    dma = pltpu.SemaphoreType.DMA
    out, grad = pl.pallas_call(
        functools.partial(kernel_body, nsec, nexp, ndp),
        name="moe_relay",
        out_shape=(
            jax.ShapeDtypeStruct((steps, tok, width), BF16),
            jax.ShapeDtypeStruct((hidn, cols), F32),
        ),
        in_specs=[hbm_spec] * 9,
        out_specs=(any_spec, any_spec),
        scratch_shapes=[
            pltpu.VMEM((2, ndp, tok, cols), BF16),
            pltpu.VMEM((2, tok, width), BF16),
            pltpu.VMEM((3, hidn, width), BF16),
            pltpu.VMEM((2, flight, ndp, SLOTS, rwide), BF16),
            pltpu.VMEM((2, 2, ny, ndp, SLOTS, rwide), BF16),
            pltpu.VMEM((ndp, rows, cols), BF16),
            pltpu.VMEM((2, hidn, rows), F32),
            pltpu.VMEM((flight, 2, ndp, SLOTS, rwide), BF16),
            pltpu.VMEM((ny, 2, ndp, SLOTS, rwide), BF16),
            pltpu.VMEM((2, ny // 2, 2, SLOTS, rwide), BF16),
            pltpu.VMEM((2, ndp, ny, 2, SLOTS, rwide), BF16),
            pltpu.VMEM((2, ndp, hidn, rows), BF16),
            pltpu.VMEM((2, ndp, rows // 2, cols), BF16),
            pltpu.VMEM((2, ndp, rows // 2, cols), BF16),
            pltpu.VMEM((ndp, rows // 2, cols), F32),
            pltpu.VMEM((2, ndp, ny, SLOTS, rwide), BF16),
            pltpu.VMEM((ndp, SLOTS, rwide), BF16),
            pltpu.VMEM((2, ndp, ny, SLOTS, rwide), BF16),
            pltpu.VMEM(routes_t.shape, jnp.int32),
            pltpu.VMEM(gates_t.shape, BF16),
            pltpu.VMEM((1, width), F32),
            pltpu.VMEM((2, 3, flight * SLOTS, 2 * tok), BF16),
            pltpu.VMEM((2, 3, flight * SLOTS, 2 * tok), BF16),
            pltpu.VMEM((2, tok, ny * SLOTS), BF16),
            pltpu.VMEM((2, tok, 3 * ny * SLOTS), BF16),
            pltpu.VMEM((2, ndp, tok, cols), BF16),
            pltpu.VMEM((hidn, cols), F32),
            dma((12,)), dma((9,)),
            dma((3, 2)), dma((3,)), dma((3,)),
            dma((1 + ndp, ny - 1)), dma((1 + ndp,)),
            dma((ny - 1,)), dma((2,)), dma((2,)), dma(()), dma(()),
            dma((2, 2)), dma((2,)), dma((2,)),
            dma((2, ndp)), dma((ndp,)), dma((2, ndp)), dma((ndp,)),
        ],
        compiler_params=pltpu.CompilerParams(
            collective_id=0, has_side_effects=True, vmem_limit_bytes=24 * 1024 * 1024
        ),
    )(
        *(
            pltpu.with_memory_space_constraint(a, pltpu.HBM)
            for a in (
                arrivals[0], fresh[0], routes_t, gates_t, cotangent[0], norm_gain, w_gate[0], w_up[0], w_down[0]
            )
        )
    )
    out, grad = pl.pallas_call(
        store_body,
        name="store",
        out_shape=(jax.ShapeDtypeStruct(out.shape, BF16), jax.ShapeDtypeStruct(grad.shape, F32)),
        in_specs=(any_spec, any_spec),
        out_specs=(any_spec, any_spec),
        scratch_shapes=[dma((2,))],
        compiler_params=pltpu.CompilerParams(vmem_limit_bytes=1024 * 1024),
    )(out, grad)
    return out[None], grad[None]


def solution(mesh):
    placed = (
        P("section", ("expert", "dp"), None),
        P(None, ("expert", "dp"), None),
        P("section", None, ("expert", "dp"), None),
        P("section", None, ("expert", "dp"), None),
        P("section", None, ("expert", "dp"), None),
        P("section", None),
        P("section", "expert", "dp"),
        P("section", "expert", "dp"),
        P("section", "expert", "dp"),
    )
    return jax.shard_map(
        functools.partial(local, mesh.shape["section"], mesh.shape["expert"], mesh.shape["dp"]),
        mesh=mesh,
        in_specs=placed,
        out_specs=(P("section", None, ("expert", "dp"), None), P("section", "expert", "dp")),
        check_vma=False,
    )
```
